32 devices in a mesh: dp: 1 (over z), tp: 4 (over y), cp: 8 (over x, core).
Axes of the slice: x: 4, y: 4, z: 1, core: 2. Of those that a mesh axis runs over, the one named last changes fastest.
The devices are a block of a 4x4x8 slice.
Arguments:
- hidden: bfloat16 [6, 2048, 6144], P('dp', 'cp')
- positions: int32 [6, 2048], P('dp', 'cp')
- w_dq: bfloat16 [6144, 1536], replicated
- g_q: float32 [1536], replicated
- w_uq: bfloat16 [1536, 12288], P(None, 'tp')
- w_dkv: bfloat16 [6144, 576], replicated
- g_kv: float32 [512], replicated
- w_uk: bfloat16 [512, 8192], P(None, 'tp')
- w_uv: bfloat16 [512, 8192], P(None, 'tp')
- w_o: bfloat16 [8192, 6144], P('tp')
Outputs:
- output 1: bfloat16 [6, 2048, 6144], P('dp', 'cp')
- output 2: bfloat16 [6, 2048, 512], P('dp', 'cp')
- output 3: bfloat16 [6, 2048, 64], P('dp', 'cp')
All inputs are finite; a program needn't handle non-finite values.
Results may differ from the reference program's by a relative error of at most 0.00745629.
Values are sent between devices in bfloat16 or wider.
A program may use at most 768 MiB of HBM per device.

```python
import jax
import jax.numpy as jnp
from jax import lax

N_SEQ = 6
SEQ_LEN = 2048
CP_SIZE = 8
D_MODEL = 6144
N_HEADS = 64
Q_RANK = 1536
KV_RANK = 512
NOPE_DIM = 128
ROPE_DIM = 64
V_DIM = 128

QK_DIM = NOPE_DIM + ROPE_DIM
BLOCK_LEN = SEQ_LEN // (2 * CP_SIZE)
SOFT_SCALE = QK_DIM ** -0.5
ROPE_BASE = 10000.0
NORM_EPS = 1e-6
Q_GAIN = 3.0


def draw_positions(rng_key):
    base_ids = jnp.tile(jnp.arange(CP_SIZE, dtype=jnp.int32)[None, :], (N_SEQ, 1))
    pair_ids = jax.random.permutation(rng_key, base_ids, axis=1, independent=True)
    offsets = jnp.arange(BLOCK_LEN, dtype=jnp.int32)
    first_blocks = pair_ids[:, :, None] * BLOCK_LEN + offsets
    second_blocks = (2 * CP_SIZE - 1 - pair_ids)[:, :, None] * BLOCK_LEN + offsets
    return jnp.stack([first_blocks, second_blocks], axis=2).reshape(N_SEQ, SEQ_LEN)


def draw_normal(rng_key, tensor_shape, std_dev):
    return (jax.random.normal(rng_key, tensor_shape, jnp.float32) * std_dev).astype(jnp.bfloat16)


def setup_inputs(seed: int = 0, part: int = 0) -> dict:
    root_key = jax.random.key(seed)
    part_key = jax.random.fold_in(root_key, part)
    weight_keys = jax.random.split(jax.random.key(seed + 1), 8)
    hidden = draw_normal(jax.random.fold_in(part_key, 0), (N_SEQ, SEQ_LEN, D_MODEL), 1.0)
    positions = draw_positions(jax.random.fold_in(part_key, 1))
    w_dq = draw_normal(weight_keys[0], (D_MODEL, Q_RANK), D_MODEL ** -0.5)
    g_q = jax.random.uniform(weight_keys[1], (Q_RANK,), jnp.float32, 0.5, 1.5)
    w_uq = draw_normal(weight_keys[2], (Q_RANK, N_HEADS * QK_DIM), Q_GAIN * Q_RANK ** -0.5)
    w_dkv = draw_normal(weight_keys[3], (D_MODEL, KV_RANK + ROPE_DIM), D_MODEL ** -0.5)
    g_kv = jax.random.uniform(weight_keys[4], (KV_RANK,), jnp.float32, 0.5, 1.5)
    w_uk = draw_normal(weight_keys[5], (KV_RANK, N_HEADS * NOPE_DIM), KV_RANK ** -0.5)
    w_uv = draw_normal(weight_keys[6], (KV_RANK, N_HEADS * V_DIM), KV_RANK ** -0.5)
    w_o = draw_normal(weight_keys[7], (N_HEADS * V_DIM, D_MODEL), (N_HEADS * V_DIM) ** -0.5)
    return {'hidden': hidden, 'positions': positions, 'w_dq': w_dq, 'g_q': g_q, 'w_uq': w_uq,
            'w_dkv': w_dkv, 'g_kv': g_kv, 'w_uk': w_uk, 'w_uv': w_uv, 'w_o': w_o}


def rms_norm(tensor, norm_gain):
    tensor_f32 = tensor.astype(jnp.float32)
    inv_rms = lax.rsqrt(jnp.mean(tensor_f32 * tensor_f32, axis=-1, keepdims=True) + NORM_EPS)
    return (tensor_f32 * inv_rms * norm_gain).astype(jnp.bfloat16)


def rotate(tensor, cos_t, sin_t):
    tensor_f32 = tensor.astype(jnp.float32)
    half_dim = tensor_f32.shape[-1] // 2
    lower_half = tensor_f32[..., :half_dim]
    upper_half = tensor_f32[..., half_dim:]
    return jnp.concatenate([lower_half * cos_t - upper_half * sin_t,
                            lower_half * sin_t + upper_half * cos_t], axis=-1).astype(jnp.bfloat16)


def reference(hidden, positions, w_dq, g_q, w_uq, w_dkv, g_kv, w_uk, w_uv, w_o):
    inv_freq = ROPE_BASE ** (-2.0 * jnp.arange(ROPE_DIM // 2, dtype=jnp.float32) / ROPE_DIM)

    def one_sequence(seq_args):
        x_seq, pos_seq = seq_args
        angles = pos_seq.astype(jnp.float32)[:, None] * inv_freq[None, :]
        cos_t = jnp.cos(angles)
        sin_t = jnp.sin(angles)
        q_latent = jnp.dot(x_seq, w_dq, preferred_element_type=jnp.float32).astype(jnp.bfloat16)
        q_normed = rms_norm(q_latent, g_q)
        q_full = jnp.dot(q_normed, w_uq, preferred_element_type=jnp.float32).astype(jnp.bfloat16)
        q_full = q_full.reshape(SEQ_LEN, N_HEADS, QK_DIM)
        q_nope = q_full[:, :, :NOPE_DIM]
        q_rope = rotate(q_full[:, :, NOPE_DIM:], cos_t[:, None, :], sin_t[:, None, :])
        kv_joint = jnp.dot(x_seq, w_dkv, preferred_element_type=jnp.float32).astype(jnp.bfloat16)
        latent = rms_norm(kv_joint[:, :KV_RANK], g_kv)
        k_rope = rotate(kv_joint[:, KV_RANK:], cos_t, sin_t)
        k_nope = jnp.dot(latent, w_uk, preferred_element_type=jnp.float32).astype(jnp.bfloat16)
        k_nope = k_nope.reshape(SEQ_LEN, N_HEADS, NOPE_DIM)
        values = jnp.dot(latent, w_uv, preferred_element_type=jnp.float32).astype(jnp.bfloat16)
        values = values.reshape(SEQ_LEN, N_HEADS, V_DIM)
        allowed = pos_seq[None, :] <= pos_seq[:, None]

        def one_head(head_args):
            qn_head, qr_head, kn_head, v_head = head_args
            scores = (jnp.dot(qn_head, kn_head.T, preferred_element_type=jnp.float32)
                      + jnp.dot(qr_head, k_rope.T, preferred_element_type=jnp.float32)) * SOFT_SCALE
            scores = jnp.where(allowed, scores, -jnp.inf)
            probs_bf = jax.nn.softmax(scores, axis=-1).astype(jnp.bfloat16)
            return jnp.dot(probs_bf, v_head, preferred_element_type=jnp.float32).astype(jnp.bfloat16)

        heads_out = lax.map(one_head, (jnp.swapaxes(q_nope, 0, 1), jnp.swapaxes(q_rope, 0, 1),
                                       jnp.swapaxes(k_nope, 0, 1), jnp.swapaxes(values, 0, 1)))
        attn_out = jnp.swapaxes(heads_out, 0, 1).reshape(SEQ_LEN, N_HEADS * V_DIM)
        y_seq = (x_seq.astype(jnp.float32)
                 + jnp.dot(attn_out, w_o, preferred_element_type=jnp.float32)).astype(jnp.bfloat16)
        return y_seq, latent, k_rope

    out_hidden, latent, k_rope = lax.map(one_sequence, (hidden, positions))
    return out_hidden, latent, k_rope
```

```python
import functools
import jax, jax.numpy as jnp
from jax import lax
from jax.experimental import pallas as pl
from jax.experimental.pallas import tpu as pltpu
from jax.sharding import PartitionSpec as P

F32, BF16 = jnp.float32, jnp.bfloat16
NEG = float("-inf")
LOG2E = 1.4426950408889634
LANES, HALF, MXU, TRIG = 128, 64, 256, 384
HALVES = 2
SOURCES = 4


MESH = pl.DeviceIdType.MESH
NORM_EPS = 1e-6


class Place:
    def __init__(self, n_tp, n_cp):
        self.dp, self.y, self.c = (lax.axis_index(a) for a in ("dp", "tp", "cp"))
        y, c = self.y, self.c
        self.n_tp = n_tp
        self.core = lax.rem(c, HALVES)
        self.partner = c + 1 - HALVES * self.core
        self.right, self.left, self.far = (lax.rem(c + k, n_cp) for k in (2, n_cp - 2, n_cp // HALVES))
        self.up, self.dn, self.dg = (lax.rem(y + k, n_tp) for k in (1, n_tp - 1, n_tp // HALVES))
        self.flip = lax.rem(y + self.core, HALVES)
        self.mate = lax.rem(y + 1 + HALVES * self.flip, n_tp)
        self.other = lax.rem(y + 3 - HALVES * self.flip, n_tp)

    def block(self, row, core):
        return lax.div(lax.rem(row + (self.n_tp - 1) * core, self.n_tp), HALVES)

    def greet(self, peers):
        barrier = pltpu.get_barrier_semaphore()
        for yy, cc in peers:
            pl.semaphore_signal(barrier, inc=1, device_id=(self.dp, yy, cc), device_id_type=MESH)
        pl.semaphore_wait(barrier, len(peers))

    def copy(self, src, dst, ss, rs, yy, cc):
        return pltpu.make_async_remote_copy(src_ref=src, dst_ref=dst, send_sem=ss, recv_sem=rs,
                                            device_id=(self.dp, yy, cc), device_id_type=MESH)

    def o_sends(self, own, par, dst, ss, rs):
        tb, tp = self.block(self.y, self.core), self.block(self.y, 1 - self.core)
        ways = [(own, tb, 1, 0, self.mate, self.c), (own, 1 - tb, 2, 0, self.other, self.c), (par, tp, 0, 1, self.y, self.partner),
                (par, tp, 1, 1, self.other, self.partner), (par, 1 - tp, 2, 1, self.mate, self.partner)]
        return [self.copy(a.at[blk], dst(src, part), ss.at[k], rs.at[k], yy, cc)
                for k, (a, blk, src, part, yy, cc) in enumerate(ways)]

    def o_forwards(self, src, dst, ss, rs):
        return [self.copy(src(2, part), dst(3, part), ss.at[5 + part], rs.at[5 + part], self.mate, self.c) for part in range(HALVES)]


def attn_kernel(dims, tab, *refs):
    G, NB, BL, HP, scale2, n_tp, n_cp = dims
    CK = HALVES * BL
    H = HALVES * HP
    q_own, q_par, cs_own, cs_par, wkT, wv, lat, wf = refs[:8]
    ost_own, ost_par, obuf, wx = refs[8:12]
    latbuf, KT, V, Q, sF, sS, mx, lsum, acc, ob, sem, osem, oss, ors, wss, wrs = refs[12:]
    n = pl.program_id(0)
    me = Place(n_tp, n_cp)
    rows_ = ((me.up, me.c), (me.dn, me.c), (me.up, me.partner), (me.dn, me.partner))
    w_to = ((me.y, me.partner), (me.y, me.right), (me.y, me.left))

    def w_send(k, slot):
        return me.copy(wf, wx.at[slot], wss.at[k], wrs.at[k], *w_to[k])

    def copies(i):
        return [pltpu.make_async_copy(lat.at[p, i], latbuf.at[pl.ds(HALVES * p, HALVES)], sem.at[p]) for p in range(n_cp)]

    def o_store(i):
        return [pltpu.make_async_copy(ob.at[k], dst.at[i], osem.at[k]) for k, dst in enumerate((ost_own, ost_par))]

    def o_sends(i):
        return me.o_sends(ost_own.at[i], ost_par.at[i], lambda s, p: obuf.at[s, p, i], oss.at[i], ors.at[i])

    def o_forwards(i):
        at = lambda s, p: obuf.at[s, p, i]
        return me.o_forwards(at, at, oss.at[i], ors.at[i])

    @pl.when(n == 0)
    def _():
        for c in copies(0):
            c.start()
        me.greet(rows_ + w_to)
        for k in range(3):
            w_send(k, me.c).start()

    @pl.when(n > 0)
    def _():
        for c in o_store(n - 1):
            c.wait()
        for s in o_sends(n - 1):
            s.start()

    lane = lax.broadcasted_iota(jnp.int32, (BL, LANES), 1)
    low64 = lane < HALF
    low32 = lax.rem(lane, HALF) < 32
    for src_i, (q, cs) in enumerate(((q_own, cs_own), (q_par, cs_par))):
        for half in range(HALVES):
            r0 = (half * 2 + src_i) * BL
            rows = pl.ds(half * BL, BL)
            ct = cs[rows, :LANES]
            st = cs[rows, LANES:MXU]
            for p in range(HP):
                a = q[0, rows, p * TRIG:p * TRIG + LANES]
                b = q[0, rows, p * TRIG + LANES:p * TRIG + MXU].astype(F32)
                c = q[0, rows, p * TRIG + MXU:p * TRIG + TRIG].astype(F32)
                u = jnp.where(low64, b, c)
                no = jnp.where(low64, c, b).astype(BF16)
                w = jnp.where(low32, pltpu.roll(u, 96, 1), pltpu.roll(u, 32, 1))
                rot = (u * ct + w * st).astype(BF16)
                Q[HALVES * p, r0:r0 + BL, :LANES] = a
                Q[HALVES * p, r0:r0 + BL, LANES:MXU] = rot
                Q[HALVES * p + 1, r0:r0 + BL, :LANES] = no
                Q[HALVES * p + 1, r0:r0 + BL, LANES:MXU] = rot

    for c in copies(n):
        c.wait()

    WB = 4 * BL
    lane_k = lax.broadcasted_iota(jnp.int32, (WB, LANES), 1)
    KR = wkT.shape[1]

    b0, b1 = tab[n, NB], tab[n, NB + 1]

    @pl.loop(0, NB // 4)
    def _(kc):
        rows = pl.ds(pl.multiple_of(kc * WB, WB), WB)
        blocks = jnp.concatenate([latbuf[tab[n, kc * 4 + j]] for j in range(SOURCES)], axis=0)
        lt = blocks[:, :KR]
        kr = jnp.where(lane_k < HALF, blocks[:, KR:].astype(F32), 0.0)
        krT = kr.T.astype(BF16)
        krO = jnp.concatenate([krT[HALF:], krT[:HALF]], axis=0)
        kt = lax.dot_general(wkT[...], lt, (((1,), (1,)), ((), ())), preferred_element_type=F32).astype(BF16)
        V[rows, :] = jnp.dot(lt, wv[...], preferred_element_type=F32).astype(BF16)
        for h in range(H):
            k = kt[h * LANES:h * LANES + LANES]
            KT[h, :LANES, rows] = k if h % HALVES == 0 else jnp.concatenate([k[HALF:], k[:HALF]], axis=0)
            KT[h, LANES:, rows] = krT if h % HALVES == 0 else krO

    @pl.when(n + 1 < G)
    def _():
        for c in copies(n + 1):
            c.start()

    HR = HALVES * BL
    R = HALVES * HR
    WK = 4 * BL
    row = lax.broadcasted_iota(jnp.int32, (HR, WK), 0)
    col = lax.broadcasted_iota(jnp.int32, (HR, WK), 1)
    dF = jnp.where(row < BL, b0 * BL + row, (b1 - 1) * BL + row) - col
    dS = jnp.where(row < BL, (NB - 1 - b0) * BL + row, (NB - 2 - b1) * BL + row) - col

    nF, nS = NB // 8, NB // 4

    def fold(t):
        w = t.shape[1] // HALVES
        t = jnp.maximum(t[:, :w], t[:, w:])
        return t if w == LANES else fold(t)

    def track(h, part, t, c, count):
        m = fold(t)
        if c > 0:
            m = jnp.maximum(mx[h, part], m)
        if c == count - 1:
            m = jnp.broadcast_to(jnp.max(m, axis=1, keepdims=True), (HR, LANES))
        mx[h, part] = m

    rF, rS = slice(0, HR), slice(HR, R)

    def p1(c, with_f):
        cols = slice(c * WK, c * WK + WK)
        for h in range(H):
            s = jnp.dot(Q[h, 0 if with_f else HR:R, :], KT[h, :, cols], preferred_element_type=F32) * scale2
            if with_f:
                f = jnp.where(dF >= c * WK, s[:HR], NEG)
                sF[h, c] = f
                track(h, rF, f, c, nF)
                s = s[HR:]
            else:
                s = jnp.where(dS >= c * WK, s, NEG)
            sS[h, c] = s
            track(h, rS, s, c, nS)

    def finish(h, part, k, total, l):
        o = (total * (1.0 / jnp.sum(l, axis=1, keepdims=True))).astype(BF16)
        for i in range(HALVES):
            ob[i, k, :, h * LANES:h * LANES + LANES] = o[i * BL:i * BL + BL]

    def p2(c, with_f):
        cols = slice(c * WK, c * WK + WK)
        for h in range(H):
            r0 = 0 if with_f else HR
            es, ls = [], None
            for j in range(WK // LANES):
                js = slice(j * LANES, j * LANES + LANES)
                e = jnp.exp2(sS[h, c, :, js] - mx[h, rS])
                if with_f:
                    e = jnp.concatenate([jnp.exp2(sF[h, c, :, js] - mx[h, rF]), e], axis=0)
                ls = e if ls is None else ls + e
                es.append(e.astype(BF16))
            pv = jnp.dot(jnp.concatenate(es, axis=1), V[cols, h * LANES:h * LANES + LANES], preferred_element_type=F32)
            if c > 0:
                ls, pv = lsum[h, r0:R] + ls, acc[h, r0:R] + pv
            if c == nF - 1:
                finish(h, rF, 0, pv[:HR], ls[:HR])
            if c == nS - 1:
                finish(h, rS, 1, pv, ls)
            else:
                lsum[h, r0:R] = ls
                acc[h, r0:R] = pv

    for k, stage in enumerate((p1, p2)):
        for c in range(nS):
            pl.when(n + c >= -k)(functools.partial(stage, c, c < nF))

    @pl.when(jnp.logical_and(n > 0, n + 1 < G))
    def _():
        for k, f in zip((1, 4), o_forwards(n - 1)):
            o_sends(n - 1)[k].wait_recv()
            f.start()

    for c in o_store(n):
        c.start()

    @pl.when(n == G - 1)
    def _():
        for c in o_store(n):
            c.wait()

        def drain_forward(i, _):
            for f in o_forwards(i):
                f.wait()
            return 0

        @pl.loop(0, G - 1)
        def _(i):
            for k, s in enumerate(o_sends(i)):
                s.wait_send()
                if k in (0, 2, 3):
                    s.wait_recv()

        lax.fori_loop(0, G - 2, drain_forward, 0)
        for k in (1, 4):
            o_sends(G - 2)[k].wait_recv()
        for k, slot in enumerate((me.partner, me.left, me.right)):
            w_send(k, me.c).wait_send()
            w_send(k, slot).wait_recv()


def attention(mesh, tab, q_own, q_par, cs_own, cs_par, wkT, wv, lat, wf, soft_scale):
    G, T = tab.shape[0], q_own.shape[1] * mesh.shape["cp"]
    BL = q_own.shape[1] // HALVES
    NB = T // BL
    VD = wv.shape[1]
    H = VD // LANES
    R = 4 * BL
    dims = (G, NB, BL, H // HALVES, float(soft_scale * LOG2E), mesh.shape["tp"], mesh.shape["cp"])
    blk = lambda a: pl.BlockSpec((1,) + a.shape[1:], lambda n, t: (n, 0, 0))
    full = lambda a: pl.BlockSpec(a.shape, lambda n, t: (0, 0))
    hbm = pl.BlockSpec(memory_space=pltpu.HBM)
    dma = pltpu.SemaphoreType.DMA
    sds = jax.ShapeDtypeStruct
    ost = sds((G, 2, BL, VD), BF16)
    stat = pltpu.VMEM((H, R, LANES), F32)
    return pl.pallas_call(
        functools.partial(attn_kernel, dims),
        grid_spec=pltpu.PrefetchScalarGridSpec(
            num_scalar_prefetch=1, grid=(G,),
            in_specs=[blk(q_own), blk(q_par)] + [pl.BlockSpec((HALVES * BL, cs_own.shape[1]), lambda n, t: (n, 0))] * 2 + [full(wkT), full(wv), hbm, hbm],
            out_specs=[hbm] * 4,
            scratch_shapes=[
                pltpu.VMEM((NB, BL, lat.shape[-1]), BF16), pltpu.VMEM((H, MXU, T), BF16), pltpu.VMEM((T, VD), BF16),
                pltpu.VMEM((H, R, MXU), BF16), pltpu.VMEM((H, NB // 8, R // HALVES, R), F32),
                pltpu.VMEM((H, NB // 4, R // HALVES, R), F32), stat, stat, stat, pltpu.VMEM((2, 2, BL, VD), BF16),
                dma((NB // HALVES,)), dma((HALVES,)), dma((G, 7)), dma((G, 7)), dma((3,)), dma((3,))],
        ),
        out_shape=[ost, ost, sds((4, 2, G, BL, VD), BF16), sds((mesh.shape["cp"],) + wf.shape, BF16)],
        compiler_params=pltpu.CompilerParams(collective_id=1, has_side_effects=True, vmem_limit_bytes=63 * 2**20),
        cost_estimate=pl.CostEstimate(flops=G * H * T * R * 800, bytes_accessed=G * T * 640 * 2, transcendentals=0),
        name="attn",
    )(tab, q_own, q_par, cs_own, cs_par, wkT, wv, lat, wf)


def proj_kernel(dims, x, w_dq, w_dkv, w_uq, g_q, g_kv, cs, w_o,
                lat_all, latent, k_rope, q_own, q_par, wf, cs_par, qn_o, qn_p,
                xbuf, wdq, wdkv, wuq, csb, pay, krb, kvb, qlat, qn, qst, gq, gkv,
                xsem, wsem, csem, osem, wss, wrs, lss, lrs, qss, qrs, css, crs, lsem):
    n_tp, n_cp, n_t, half_cols, wc = dims
    dp, y, c = lax.axis_index("dp"), lax.axis_index("tp"), lax.axis_index("cp")
    core = lax.rem(c, HALVES)
    partner = c + 1 - HALVES * core
    right, left, far = lax.rem(c + 2, n_cp), lax.rem(c + n_cp - 2, n_cp), lax.rem(c + 4, n_cp)
    up, dn, dg = lax.rem(y + 1, n_tp), lax.rem(y + n_tp - 1, n_tp), lax.rem(y + 2, n_tp)
    peers = [(up, c), (dn, c), (dg, c), (y, partner), (y, right), (y, left)]

    barrier = pltpu.get_barrier_semaphore()
    for yy, cc in peers:
        pl.semaphore_signal(barrier, inc=1, device_id=(dp, yy, cc), device_id_type=MESH)
    pl.semaphore_wait(barrier, len(peers))

    def rdma(src, dst, ss, rs, yy, cc):
        return pltpu.make_async_remote_copy(src_ref=src, dst_ref=dst, send_sem=ss, recv_sem=rs,
                                            device_id=(dp, yy, cc), device_id_type=MESH)

    half = lax.rem(y, HALVES)
    col_opp = pl.multiple_of((1 - half) * half_cols + c * wc, LANES)
    col_same = pl.multiple_of(half * half_cols + c * wc, LANES)
    w_sends = [rdma(w_o.at[:, pl.ds(col_opp, wc)], wf.at[0], wss.at[0], wrs.at[0], dn, c),
               rdma(w_o.at[:, pl.ds(col_opp, wc)], wf.at[1], wss.at[1], wrs.at[1], up, c),
               rdma(w_o.at[:, pl.ds(col_same, wc)], wf.at[2], wss.at[2], wrs.at[2], dg, c)]
    for s in w_sends:
        s.start()
    cs_send = rdma(cs, cs_par, css, crs, y, partner)
    cs_send.start()

    rows = xbuf.shape[1]
    bl = pay.shape[3]

    def load_x(i):
        return pltpu.make_async_copy(x.at[pl.ds((i % n_t) * rows, rows), :], xbuf.at[i % HALVES], xsem.at[i % HALVES])

    kr_rank = gkv.shape[1]
    nj = MXU
    loads = [pltpu.make_async_copy(w_dkv, wdkv, wsem.at[0]), pltpu.make_async_copy(g_kv, gkv, wsem.at[1]),
             pltpu.make_async_copy(cs, csb, csem)]
    late = [pltpu.make_async_copy(w_dq, wdq, wsem.at[2]), pltpu.make_async_copy(g_q, gq, wsem.at[3]),
            pltpu.make_async_copy(w_uq.at[:, pl.ds(pl.multiple_of(core * wuq.shape[1], LANES), wuq.shape[1])], wuq, wsem.at[4])]
    loads[0].start()
    load_x(0).start()
    loads[1].start()
    loads[2].start()
    for d in loads:
        d.wait()

    lane = lax.broadcasted_iota(jnp.int32, (rows, LANES), 1)
    low32 = lax.rem(lane, HALF) < 32
    tile = lambda t: pl.ds(t * 2, HALVES)
    stores = {}
    lat_sends = []

    def norm(t32, gain):
        return (t32 * lax.rsqrt(jnp.mean(t32 * t32, axis=-1, keepdims=True) + NORM_EPS) * gain).astype(BF16)

    def send_own(t):
        own = lat_all.at[c, tile(t)]
        for k, cc in ((0, partner), (1, left), (2, right)):
            s = rdma(own, own, lss.at[t, k], lrs.at[t, k], y, cc)
            s.start()
            lat_sends.append(s)

    for t in range(n_t):
        load_x(t).wait()
        if t == 0:
            for d in [load_x(1)] + late:
                d.start()

        def kv_dot(wrows):
            d = lax.dot_general(xbuf[t % HALVES], wdkv[wrows, :], (((1,), (1,)), ((), ())), preferred_element_type=F32)
            return d.astype(BF16)

        @pl.loop(0, kr_rank // nj)
        def _(j):
            kvb[:, pl.ds(pl.multiple_of(j * nj, nj), nj)] = kv_dot(pl.ds(pl.multiple_of(j * nj, nj), nj))

        u = kv_dot(pl.ds(kr_rank, wdkv.shape[0] - kr_rank)).astype(F32)
        load_x(t + 2).start()
        lat = norm(kvb[...].astype(F32), gkv[...])
        u = jnp.concatenate([u, u], axis=1)
        r = pl.ds(t * rows, rows)
        w = jnp.where(low32, pltpu.roll(u, 96, 1), pltpu.roll(u, 32, 1))
        rot = u * csb[r, :LANES] + w * csb[r, LANES:MXU]
        if t >= 2:
            for s in stores.pop(t - 2):
                s.wait()
        sl = t % HALVES
        krb[sl] = rot[:, :HALF].astype(BF16)
        pay[sl, :, :, :, :kr_rank] = lat.reshape(2, 2, bl, kr_rank)
        pay[sl, :, :, :, kr_rank:] = jnp.where(lane < HALF, rot, csb[r, MXU:TRIG]).astype(BF16).reshape(2, 2, bl, LANES)
        st = [pltpu.make_async_copy(pay.at[sl], lat_all.at[c, tile(t)], lsem.at[t]),
              pltpu.make_async_copy(pay.at[sl, :, :, :, :kr_rank], latent.at[tile(t)], osem.at[0, sl]),
              pltpu.make_async_copy(krb.at[sl], k_rope.at[r], osem.at[1, sl])]
        for s in st:
            s.start()
        stores[t] = st[1:]
        if t > 0:
            pltpu.make_async_copy(pay.at[1 - sl], lat_all.at[c, tile(t - 1)], lsem.at[t - 1]).wait()
            send_own(t - 1)

    last = n_t - 1
    for d in late:
        d.wait()

    def stage1(t):
        rp, lp = lat_all.at[right, tile(t)], lat_all.at[left, tile(t)]
        rdma(rp, rp, lss.at[t, 3], lrs.at[t, 1], y, partner).wait_recv()
        rdma(lp, lp, lss.at[t, 3], lrs.at[t, 2], y, partner).wait_recv()
        l0, r1 = lat_all.at[left, tile(t), 0], lat_all.at[right, tile(t), 1]
        for k, src, i, cc in ((5, l0, 5, right), (6, r1, 6, left), (3, rp, 3, partner), (4, lp, 4, partner)):
            s = rdma(src, src, lss.at[t, k], lrs.at[t, i], y, cc)
            s.start()
            lat_sends.append(s)

    def stage2(t):
        f0, f1 = lat_all.at[far, tile(t), 0], lat_all.at[far, tile(t), 1]
        for k, ref in ((5, f0), (6, f1)):
            rdma(ref, ref, lss.at[t, 7], lrs.at[t, k], y, partner).wait_recv()
            s = rdma(ref, ref, lss.at[t, k + 2], lrs.at[t, k + 2], y, partner)
            s.start()
            lat_sends.append(s)

    def project(src, wref, dst, width):
        @pl.loop(0, wref.shape[1] // width)
        def _(j):
            cols = pl.ds(pl.multiple_of(j * width, width), width)
            dst[:, cols] = jnp.dot(src[...], wref[:, cols], preferred_element_type=F32).astype(BF16)

    q_sends, q_stores = [], {}
    for t in range(n_t):
        i = n_t + t
        load_x(i).wait()
        project(xbuf.at[i % HALVES], wdq, qlat, nj)
        if i + 2 < HALVES * n_t:
            load_x(i + 2).start()
        if t == 0:
            sl = last % HALVES
            pltpu.make_async_copy(pay.at[sl], lat_all.at[c, tile(last)], lsem.at[last]).wait()
            send_own(last)
            for k in list(stores):
                for s in stores.pop(k):
                    s.wait()
        stage1(t)
        sl = t % HALVES
        qn[sl] = norm(qlat[...].astype(F32), gq[...])
        r = pl.ds(t * rows, rows)
        cp = pltpu.make_async_copy(qn.at[sl], qn_o.at[r], osem.at[2, sl])
        cp.start()
        if t >= 2:
            q_stores.pop(t - 2).wait()
        project(qn.at[sl], wuq, qst.at[sl], HALVES * nj)
        cp.wait()
        s = rdma(qn_o.at[r], qn_p.at[r], qss.at[t], qrs.at[t], y, partner)
        s.start()
        q_sends.append((cp, s))
        so = pltpu.make_async_copy(qst.at[sl], q_own.at[r], osem.at[3, sl])
        so.start()
        q_stores[t] = so

    def load_qp(t):
        r = pl.ds(t * rows, rows)
        return pltpu.make_async_copy(qn_p.at[r], qn.at[t % HALVES], osem.at[2, t % HALVES])

    def take_qp(t):
        r = pl.ds(t * rows, rows)
        rdma(qn_o.at[r], qn_p.at[r], qss.at[t], qrs.at[t], y, partner).wait_recv()
        load_qp(t).start()

    take_qp(0)
    for t in range(n_t):
        sl = (n_t + t) % HALVES
        for k in [k for k in q_stores if (k % HALVES) == sl]:
            q_stores.pop(k).wait()
        load_qp(t).wait()
        if t + 1 < n_t:
            take_qp(t + 1)
        project(qn.at[t % HALVES], wuq, qst.at[sl], HALVES * nj)
        so = pltpu.make_async_copy(qst.at[sl], q_par.at[pl.ds(t * rows, rows)], osem.at[3, sl])
        so.start()
        q_stores[n_t + t] = so
        stage2(t)
    for k in list(q_stores):
        q_stores.pop(k).wait()

    pp, rp, lp = lax.rem(partner, n_cp), lax.rem(partner + 2, n_cp), lax.rem(partner + n_cp - 2, n_cp)
    fp = lax.rem(partner + 4, n_cp)
    for t in range(n_t):
        for i, ref in ((0, lat_all.at[pp, tile(t)]), (3, lat_all.at[rp, tile(t)]), (4, lat_all.at[lp, tile(t)]),
                       (7, lat_all.at[fp, tile(t), 0]), (8, lat_all.at[fp, tile(t), 1])):
            rdma(ref, ref, lss.at[t, 7], lrs.at[t, i], y, partner).wait_recv()
    for s in lat_sends:
        s.wait_send()
    for _, s in q_sends:
        s.wait_send()
    for s in w_sends:
        s.wait()
    cs_send.wait()


def project_all(mesh, x, w_dq, w_dkv, w_uq, g_q, g_kv, cs, w_o, bl):
    n_tp, n_cp = mesh.shape["tp"], mesh.shape["cp"]
    n_seq, seq, width = x.shape
    rows = HALVES * seq
    n_t = n_seq // HALVES
    rank, kvw = w_dq.shape[1], w_dkv.shape[1]
    kr = g_kv.shape[0]
    qw = w_uq.shape[1] // HALVES
    half_cols = width // HALVES
    wc = half_cols // n_cp
    total = n_seq * seq
    hbm = pl.BlockSpec(memory_space=pltpu.HBM)
    sds = jax.ShapeDtypeStruct
    dma = pltpu.SemaphoreType.DMA
    return pl.pallas_call(
        functools.partial(proj_kernel, (n_tp, n_cp, n_t, half_cols, wc)),
        in_specs=[hbm] * 8,
        out_specs=[hbm] * 9,
        out_shape=[sds((n_cp, n_seq, 2, bl, kr + LANES), BF16), sds((n_seq, 2, bl, kr), BF16), sds((total, kvw - kr), BF16),
                   sds((total, qw), BF16), sds((total, qw), BF16), sds((3, w_o.shape[0], wc), BF16),
                   sds(cs.shape, F32), sds((total, rank), BF16), sds((total, rank), BF16)],
        scratch_shapes=[
            pltpu.VMEM((2, rows, width), BF16), pltpu.VMEM((width, rank), BF16), pltpu.VMEM((kvw, width), BF16),
            pltpu.VMEM((rank, qw), BF16), pltpu.VMEM(cs.shape, F32), pltpu.VMEM((2, 2, 2, bl, kr + LANES), BF16),
            pltpu.VMEM((2, rows, kvw - kr), BF16), pltpu.VMEM((rows, kr), BF16), pltpu.VMEM((rows, rank), BF16), pltpu.VMEM((2, rows, rank), BF16),
            pltpu.VMEM((2, rows, qw), BF16), pltpu.VMEM((1, rank), F32), pltpu.VMEM((1, kr), F32),
            dma((HALVES,)), dma((5,)), dma, dma((4, HALVES)), dma((3,)), dma((3,)), dma((n_t, 9)), dma((n_t, 9)),
            dma((n_t,)), dma((n_t,)), dma, dma, dma((n_t,))],
        compiler_params=pltpu.CompilerParams(collective_id=0, has_side_effects=True, vmem_limit_bytes=63 * 1024 * 1024),
        cost_estimate=pl.CostEstimate(flops=HALVES * total * (width * (rank + kvw) + HALVES * rank * qw), bytes_accessed=10**8,
                                      transcendentals=0),
        name="proj",
    )(x.reshape(total, width), w_dq, w_dkv.T, w_uq, g_q.reshape(1, -1), g_kv.reshape(1, -1), cs, w_o)


def out_kernel(dims, x, w_o, wf, wx, ost_own, ost_par, obuf, out, wy, oy,
               wbuf, ov, xb, stage, wsem, osem, xsem, ssem, oss, ors, wss, wrs, ass, ars):
    n_tp, n_cp, n_seq, bl, half_cols = dims
    me = Place(n_tp, n_cp)
    me.greet(((me.up, me.c), (me.dn, me.c), (me.up, me.partner), (me.dn, me.partner),
              (me.y, me.partner), (me.y, me.right), (me.y, me.left)))
    cols, kb = xb.shape[-1], obuf.shape[-1]
    w, krows = cols // HALVES, w_o.shape[0]
    hk = krows // HALVES
    last = n_seq - 1
    half_of = lambda row: lax.rem(row, HALVES)
    tb = me.block(me.y, me.core)

    to_last = lambda s, p: oy.at[s, p, 1]
    to_prev = lambda s, p: oy.at[s, p, 0]
    prev_fwd = me.o_forwards(lambda s, p: obuf.at[s, p, last - 1], to_prev, oss.at[0], ors.at[0])
    last_sends = me.o_sends(ost_own.at[last], ost_par.at[last], to_last, oss.at[1], ors.at[1])
    last_fwd = me.o_forwards(to_last, to_last, oss.at[1], ors.at[1])
    for s in last_sends + prev_fwd:
        s.start()

    def w_copy(k, src, dst, yy, cc):
        return me.copy(src, dst, wss.at[k], wrs.at[k], yy, cc)

    lo_rows, hi_rows = pl.ds(0, hk), pl.ds(hk, hk)
    p_right, p_left, p_far = (lax.rem(me.partner + k, n_cp) for k in (2, n_cp - 2, n_cp // HALVES))
    w_sends = [w_copy(0, wx.at[me.right], wy.at[me.right], me.y, me.partner), w_copy(1, wx.at[me.left], wy.at[me.left], me.y, me.partner),
               w_copy(2, wx.at[me.left, :, lo_rows], wy.at[me.left, :, lo_rows], me.y, me.right),
               w_copy(3, wx.at[me.right, :, hi_rows], wy.at[me.right, :, hi_rows], me.y, me.left)]
    for s in w_sends:
        s.start()
    far_fwd = []
    for k, part in ((4, lo_rows), (5, hi_rows)):
        ref = wy.at[me.far, :, part]
        far_fwd.append(w_copy(k, ref, ref, me.y, me.partner))

    def w_recv(k, ref):
        w_copy(k, ref, ref, me.y, me.partner).wait_recv()

    n_m = n_seq // HALVES
    rows = HALVES * bl
    k_of = (None, me.flip, 1 - me.flip, HALVES)
    pieces = ((wf, wx.at[me.partner]), (wx.at[me.right], wy.at[p_right]), (wx.at[me.left], wy.at[p_left]), (wy.at[me.far], wy.at[p_far]))
    offs = [pl.multiple_of(v * w, LANES) for v in (me.core, 1 - me.core)]

    def col_of(j, row):
        dx = j + (j // HALVES) * (1 - HALVES * (j % HALVES))
        xq = lax.rem(lax.div(me.c, HALVES) + dx, n_cp // HALVES)
        return pl.multiple_of(half_of(row) * half_cols + xq * cols, LANES)

    def w_loads(j):
        b = j % HALVES
        out_ = [pltpu.make_async_copy(w_o.at[:, pl.ds(col_of(j, me.y), cols)], wbuf.at[b, 0], wsem.at[b, 0])]
        for r in range(1, 4):
            for part in range(HALVES):
                out_.append(pltpu.make_async_copy(pieces[j][part].at[k_of[r]], wbuf.at[b, r, :, pl.ds(offs[part], w)],
                                                  wsem.at[b, HALVES * r + part]))
        return out_

    def x_load(j):
        return pltpu.make_async_copy(x.at[:, pl.ds(pl.multiple_of(tb * bl, bl), bl), pl.ds(col_of(j, me.y), cols)], xb.at[j % HALVES], xsem.at[j % HALVES])

    o_offs = [pl.multiple_of(v * kb, LANES) for v in (me.core, 1 - me.core)]

    def o_loads(n0, cnt, refs):
        out_ = []
        for i in range(cnt):
            for r in range(SOURCES):
                for part in range(HALVES):
                    src = ost_own.at[n0 + i, tb] if (r, part) == (0, 0) else refs(r, part, n0 + i)
                    out_.append(pltpu.make_async_copy(src, ov.at[n0 + i, :, pl.ds(pl.multiple_of(r * krows + o_offs[part], LANES), kb)],
                                                      osem.at[n0 + i, HALVES * r + part]))
        return out_

    early = o_loads(0, last - 1, lambda r, p, i: obuf.at[r, p, i])
    late = o_loads(last - 1, 2, lambda r, p, i: oy.at[r, p, i - last + 1] if (i == last or r == 3) else obuf.at[r, p, i])
    for d in w_loads(0) + early + [x_load(0)]:
        d.start()

    def region(row, j, m, n0=0, cnt=2):
        return out.at[pl.ds(HALVES * m + n0, cnt), pl.ds(pl.multiple_of(me.block(row, me.core) * bl, bl), bl), pl.ds(col_of(j, row), cols)]

    def ring(k, ref, j, m, yy):
        i = j * n_m + m
        return me.copy(ref, ref, ass.at[i, k], ars.at[i, k], yy, me.c)

    def tile_sends(j, m):
        ref = region(me.y, j, m)
        return ring(0, ref, j, m, me.up), ring(1, ref, j, m, me.dn)

    def forward(j, m):
        ring(0, region(me.dn, j, m), j, m, me.up).wait_recv()
        ring(2, region(me.dn, j, m, 0, 1), j, m, me.up).start()
        ring(1, region(me.up, j, m), j, m, me.up).wait_recv()
        ring(3, region(me.up, j, m, 1, 1), j, m, me.dn).start()

    nt = MXU

    def tile(j, m):
        b = j % HALVES

        @pl.loop(0, cols // nt)
        def _(t):
            cs_ = pl.ds(pl.multiple_of(t * nt, nt), nt)
            a = ov[pl.ds(HALVES * m, HALVES)].reshape(rows, 4 * krows)
            s = None
            for r in range(SOURCES):
                d = jnp.dot(a[:, r * krows:(r + 1) * krows], wbuf[b, r, :, cs_], preferred_element_type=F32)
                s = d if s is None else s + d
            xr = xb[b, pl.ds(HALVES * m, HALVES), :, cs_].reshape(rows, nt).astype(F32)
            stage[:, :, cs_] = (xr + s).astype(BF16).reshape(2, bl, nt)

        c = pltpu.make_async_copy(stage, region(me.y, j, m), ssem)
        c.start()
        c.wait()
        for s in tile_sends(j, m):
            s.start()

    def need(j):
        if j == 0:
            w_recv(0, wy.at[p_right])
        elif j == 1:
            w_recv(1, wy.at[p_left])
        else:
            for k, part in ((2, lo_rows), (3, hi_rows)):
                w_recv(k, wy.at[me.far, :, part])
            for f in far_fwd:
                f.start()
            for k, part in ((4, lo_rows), (5, hi_rows)):
                w_recv(k, wy.at[p_far, :, part])
        for d in w_loads(j + 1) + [x_load(j + 1)]:
            d.start()

    def late_o():
        for k, f in zip((1, 4), last_fwd):
            last_sends[k].wait_recv()
            f.start()
        for k in (0, 2, 3):
            last_sends[k].wait_recv()
        for f in prev_fwd + last_fwd:
            f.wait_recv()
        for d in late:
            d.start()
        for d in late:
            d.wait()

    for d in early:
        d.wait()

    @pl.loop(0, 4 * n_m)
    def _(i):
        j, m = lax.div(i, n_m), lax.rem(i, n_m)
        for jj in range(SOURCES):
            @pl.when(i == jj * n_m)
            def _(jj=jj):
                for d in w_loads(jj) + [x_load(jj)]:
                    d.wait()
                if jj < 2:
                    need(jj)
        pl.when(i == n_m - 1)(late_o)
        tile(j, m)

        @pl.when(j > 0)
        def _():
            forward(j - 1, m)

        pl.when(i == 3 * n_m - 1)(lambda: need(2))

    @pl.loop(0, n_m)
    def _(m):
        forward(3, m)

    @pl.loop(0, 4 * n_m)
    def _(i):
        j, m = lax.div(i, n_m), lax.rem(i, n_m)
        for k, row, n0, cnt in ((0, me.y, 0, HALVES), (1, me.y, 0, HALVES), (2, me.dn, 0, 1), (3, me.up, 1, 1)):
            r = region(row, j, m, n0, cnt)
            me.copy(r, r, ass.at[i, k], ars.at[i, k], me.up, me.c).wait_send()
        for k, n0 in ((2, 0), (3, 1)):
            r = region(me.dg, j, m, n0, 1)
            me.copy(r, r, ass.at[i, k], ars.at[i, k], me.up, me.c).wait_recv()

    for s in last_sends + prev_fwd + last_fwd + w_sends + far_fwd:
        s.wait_send()


def out_product(mesh, x, w_o, wf, wx, ost_own, ost_par, obuf):
    n_tp, n_cp = mesh.shape["tp"], mesh.shape["cp"]
    n_seq, seq, width = x.shape
    bl = seq // HALVES
    cols = HALVES * wf.shape[-1]
    krows = w_o.shape[0]
    hbm = pl.BlockSpec(memory_space=pltpu.HBM)
    dma = pltpu.SemaphoreType.DMA
    sds = jax.ShapeDtypeStruct
    tiles = HALVES * n_seq
    return pl.pallas_call(
        functools.partial(out_kernel, (n_tp, n_cp, n_seq, bl, width // HALVES)),
        in_specs=[hbm] * 7, out_specs=[hbm] * 3,
        out_shape=[sds(x.shape, BF16), sds(wx.shape, BF16), sds((4, 2, HALVES) + obuf.shape[3:], BF16)],
        scratch_shapes=[
            pltpu.VMEM((2, 4, krows, cols), BF16), pltpu.VMEM((n_seq, bl, 4 * krows), BF16), pltpu.VMEM((2, n_seq, bl, cols), BF16),
            pltpu.VMEM((2, bl, cols), BF16), dma((2, 8)), dma((n_seq, 8)), dma((HALVES,)), dma, dma((2, 7)), dma((2, 7)),
            dma((6,)), dma((6,)), dma((tiles, 4)), dma((tiles, 4))],
        compiler_params=pltpu.CompilerParams(collective_id=2, has_side_effects=True, vmem_limit_bytes=63 * 2**20),
        cost_estimate=pl.CostEstimate(flops=n_seq * seq * cols * 16 * krows, bytes_accessed=10**8, transcendentals=0),
        name="outp",
    )(x, w_o, wf, wx, ost_own, ost_par, obuf)[0]


def settle_kernel(src, dst, buf, rsem, wsem):
    n = buf.shape[0]
    ins = [pltpu.make_async_copy(src.at[i], buf.at[i], rsem.at[i]) for i in range(n)]
    outs = [pltpu.make_async_copy(buf.at[i], dst.at[i], wsem.at[i]) for i in range(n)]
    for d in ins:
        d.start()
    for a, b in zip(ins, outs):
        a.wait()
        b.start()
    for b in outs:
        b.wait()


def settle(a):
    parts = HALVES * a.shape[0]
    shape = (parts, a.shape[1] // HALVES, a.shape[2])
    hbm = pl.BlockSpec(memory_space=pltpu.HBM)
    sem = pltpu.SemaphoreType.DMA((parts,))
    return pl.pallas_call(
        settle_kernel, in_specs=[hbm], out_specs=hbm, out_shape=jax.ShapeDtypeStruct(shape, a.dtype),
        scratch_shapes=[pltpu.VMEM(shape, a.dtype), sem, sem],
        compiler_params=pltpu.CompilerParams(vmem_limit_bytes=32 * 2**20), name="settle",
    )(a.reshape(shape)).reshape(a.shape)


ROPE_BASE = 10000.0


def solution(mesh):
    def local_step(x, pos, w_dq, g_q, w_uq, w_dkv, g_kv, w_uk, w_uv, w_o):
        n_seq, seq, _ = x.shape
        n_cp = mesh.shape["cp"]
        bl = seq // HALVES
        nb = HALVES * n_cp
        kv_rank = g_kv.shape[0]
        rope = w_dkv.shape[1] - kv_rank
        heads = (w_uq.shape[1] - w_uk.shape[1]) // rope
        nope = w_uk.shape[1] // heads
        c = lax.axis_index("cp")
        core = c % HALVES

        inv_freq = ROPE_BASE ** (-2.0 * jnp.arange(rope // HALVES, dtype=F32) / rope)
        lanes = jnp.arange(LANES)
        ang = pos.astype(F32)[..., None] * jnp.tile(inv_freq, LANES // (rope // HALVES))
        sign = jnp.where(lanes % rope < rope // HALVES, -1.0, 1.0)
        bid = jnp.broadcast_to((pos[:, :1] // bl).astype(F32)[..., None], ang.shape)
        cs_own = jnp.concatenate([jnp.cos(ang), jnp.sin(ang) * sign, bid], axis=-1).reshape(n_seq * seq, TRIG)
        lat_all, latent, k_rope, q_own, q_par, wf, cs_par, _, _ = project_all(
            mesh, x, w_dq, w_dkv, w_uq, g_q, g_kv, cs_own, w_o, bl)
        latent, k_rope = latent.reshape(n_seq, seq, kv_rank), k_rope.reshape(n_seq, seq, rope)
        q_own, q_par = (a.reshape(n_seq, seq, -1) for a in (q_own, q_par))
        hw = w_uk.shape[1] // HALVES
        wkT = lax.dynamic_slice(w_uk, (0, core * hw), (kv_rank, hw)).T
        wv = lax.dynamic_slice(w_uv, (0, core * hw), (kv_rank, hw))

        ids = lat_all[:, :, 0, 0, kv_rank + rope].astype(jnp.int32)
        blocks = jnp.arange(nb)
        first = ids[:, :, None] == blocks
        second = nb - 1 - ids[:, :, None] == blocks
        dev = jnp.arange(n_cp)[:, None, None]
        slots = jnp.sum(jnp.where(first, HALVES * dev, 0) + jnp.where(second, HALVES * dev + 1, 0), axis=0)
        mine = [jnp.sum(jnp.where(jnp.arange(n_cp)[:, None] == k, ids, 0), axis=0)[:, None] for k in (c, c ^ 1)]
        tab = jnp.concatenate([slots] + mine, axis=1).astype(jnp.int32)

        ost_own, ost_par, obuf, wx = attention(mesh, tab, q_own, q_par, cs_own, cs_par, wkT, wv, lat_all, wf, (nope + rope) ** -0.5)
        return settle(out_product(mesh, x, w_o, wf, wx, ost_own, ost_par, obuf)), latent, k_rope

    seq_spec = P("dp", "cp", None)
    whole = P(None, None)
    in_specs = (seq_spec, P("dp", "cp"), whole, P(None), P(None, "tp"), whole, P(None), P(None, "tp"), P(None, "tp"), P("tp", None))
    return jax.shard_map(local_step, mesh=mesh, in_specs=in_specs, out_specs=(seq_spec,) * 3, check_vma=False)
```

```python
import functools
import numpy as np
import jax, jax.numpy as jnp
from jax import lax
from jax.experimental import pallas as pl
from jax.experimental.pallas import tpu as pltpu
from jax.sharding import PartitionSpec as P

F32, BF16 = jnp.float32, jnp.bfloat16
NEG = float("-inf")
LOG2E = 1.4426950408889634
LANES, HALF, QUARTER, MXU, WIDE, PAIR = 128, 64, 32, 256, 512, 384
HALVES = 2
SOURCES = 4
MIB = 2**20
SPARE = 7


MESH = pl.DeviceIdType.MESH
NORM_EPS = 1e-6


class Place:
    def __init__(self, n_tp, n_cp):
        self.dp, self.y, self.c = (lax.axis_index(a) for a in ("dp", "tp", "cp"))
        y, c = self.y, self.c
        self.n_tp = n_tp
        self.core = lax.rem(c, HALVES)
        self.partner = c + 1 - HALVES * self.core
        self.right, self.left, self.far = (lax.rem(c + k, n_cp) for k in (HALVES, n_cp - 2, n_cp // HALVES))
        self.up, self.dn, self.dg = (lax.rem(y + k, n_tp) for k in (1, n_tp - 1, n_tp // HALVES))
        self.flip = lax.rem(y + self.core, HALVES)
        self.mate = lax.rem(y + 1 + HALVES * self.flip, n_tp)
        self.other = lax.rem(y + 3 - HALVES * self.flip, n_tp)

    def block(self, row, core):
        return lax.div(lax.rem(row + (self.n_tp - 1) * core, self.n_tp), HALVES)

    def greet(self, peers):
        barrier = pltpu.get_barrier_semaphore()
        for yy, cc in peers:
            pl.semaphore_signal(barrier, inc=1, device_id=(self.dp, yy, cc), device_id_type=MESH)
        pl.semaphore_wait(barrier, len(peers))

    def copy(self, src, dst, ss, rs, yy, cc):
        return pltpu.make_async_remote_copy(src_ref=src, dst_ref=dst, send_sem=ss, recv_sem=rs,
                                            device_id=(self.dp, yy, cc), device_id_type=MESH)

    def o_sends(self, own, par, dst, ss, rs):
        tb, tp = self.block(self.y, self.core), self.block(self.y, 1 - self.core)
        ways = [(own, tb, 1, 0, self.mate, self.c), (own, 1 - tb, 2, 0, self.other, self.c), (par, tp, 0, 1, self.y, self.partner),
                (par, tp, 1, 1, self.other, self.partner), (par, 1 - tp, 2, 1, self.mate, self.partner)]
        return [self.copy(a.at[blk], dst(src, part), ss.at[k], rs.at[k], yy, cc)
                for k, (a, blk, src, part, yy, cc) in enumerate(ways)]

    def o_forwards(self, src, dst, ss, rs):
        return [self.copy(src(2, part), dst(3, part), ss.at[5 + part], rs.at[5 + part], self.mate, self.c) for part in range(HALVES)]


def w_parts(rows):
    cut = rows // 8
    return (pl.ds(0, rows - cut), pl.ds(cut, rows - cut)), (pl.ds(rows - cut, cut), pl.ds(0, cut))


def attn_kernel(dims, tab, *refs):
    G, NB, BL, HP, scale2, n_tp, n_cp = dims
    CK = HALVES * BL
    H = HALVES * HP
    q_own, q_par, cs_own, cs_par, w_uk, w_uv, lat, wf = refs[:8]
    ost_own, ost_par, obuf, wx = refs[8:12]
    latbuf, KT, V, Q, sF, sS, sX, mx, lsum, acc, ob, wk, wkT, wv, sem, ksem, osem, oss, ors, wss, wrs = refs[12:]
    n = pl.program_id(0)
    me = Place(n_tp, n_cp)
    rows_ = ((me.up, me.c), (me.dn, me.c), (me.up, me.partner), (me.dn, me.partner))
    w_to = ((me.y, me.partner), (me.y, me.right), (me.y, me.left))

    krows = wf.shape[1]
    w_rows = (pl.ds(0, krows),) + w_parts(krows)[0]

    def w_send(k, slot):
        return me.copy(wf.at[:, w_rows[k]], wx.at[slot, :, w_rows[k]], wss.at[k], wrs.at[k], *w_to[k])

    def copies(i):
        return [pltpu.make_async_copy(lat.at[p, i], latbuf.at[pl.ds(HALVES * p, HALVES)], sem.at[p]) for p in range(n_cp)]

    def o_store(i):
        return [pltpu.make_async_copy(ob.at[k], dst.at[i], osem.at[k]) for k, dst in enumerate((ost_own, ost_par))]

    def o_sends(i):
        return me.o_sends(ost_own.at[i], ost_par.at[i], lambda s, p: obuf.at[s, p, i], oss.at[i], ors.at[i])

    def o_forwards(i):
        at = lambda s, p: obuf.at[s, p, i]
        return me.o_forwards(at, at, oss.at[i], ors.at[i])

    hw = wv.shape[1]
    kv_loads = [pltpu.make_async_copy(a.at[:, pl.ds(pl.multiple_of(me.core * hw, LANES), hw)], b, ksem.at[k])
                for k, (a, b) in enumerate(((w_uk, wk), (w_uv, wv)))]

    @pl.when(n == 0)
    def _():
        for c in copies(0) + kv_loads:
            c.start()
        me.greet(rows_ + w_to)
        for k in range(3):
            w_send(k, me.c).start()
        for c in kv_loads:
            c.wait()
        wkT[...] = wk[...].T

    lane = lax.broadcasted_iota(jnp.int32, (BL, LANES), 1)
    low64 = lane < HALF
    low32 = lax.rem(lane, HALF) < QUARTER
    for src_i, (q, cs) in enumerate(((q_own, cs_own), (q_par, cs_par))):
        @pl.loop(0, HALVES)
        def _(half, src_i=src_i, q=q, cs=cs):
            r0 = half * 2 + src_i
            rows = pl.ds(pl.multiple_of(half * BL, BL), BL)
            ct = cs[rows, :LANES]
            st = cs[rows, LANES:]
            for p in range(HP):
                a = q[0, rows, p * PAIR:p * PAIR + LANES]
                b = q[0, rows, p * PAIR + LANES:p * PAIR + MXU].astype(F32)
                c = q[0, rows, p * PAIR + MXU:p * PAIR + PAIR].astype(F32)
                u = jnp.where(low64, b, c)
                no = jnp.where(low64, c, b).astype(BF16)
                w = jnp.where(low32, pltpu.roll(u, 96, 1), pltpu.roll(u, QUARTER, 1))
                rot = (u * ct + w * st).astype(BF16)
                Q[HALVES * p, r0, :, :LANES] = a
                Q[HALVES * p, r0, :, LANES:MXU] = rot
                Q[HALVES * p + 1, r0, :, :LANES] = no
                Q[HALVES * p + 1, r0, :, LANES:MXU] = rot

    @pl.when(n > 0)
    def _():
        for c in o_store(n - 1):
            c.wait()
        for s in o_sends(n - 1):
            s.start()

    for c in copies(n):
        c.wait()

    WB = 4 * BL
    lane_k = lax.broadcasted_iota(jnp.int32, (WB, LANES), 1)
    KR = wkT.shape[1]

    b0, b1 = tab[n, NB], tab[n, NB + 1]

    @pl.loop(0, NB // 4)
    def _(kc):
        blocks = jnp.concatenate([latbuf[tab[n, kc * 4 + j]] for j in range(SOURCES)], axis=0)
        lt = blocks[:, :KR]
        kr = jnp.where(lane_k < HALF, blocks[:, KR:].astype(F32), 0.0)
        krT = kr.T.astype(BF16)
        krO = jnp.concatenate([krT[HALF:], krT[:HALF]], axis=0)
        kt = lax.dot_general(wkT[...], lt, (((1,), (1,)), ((), ())), preferred_element_type=F32).astype(BF16)
        V[kc] = jnp.dot(lt, wv[...], preferred_element_type=F32).astype(BF16)
        for h in range(H):
            k = kt[h * LANES:h * LANES + LANES]
            KT[kc, h, :LANES] = k if h % HALVES == 0 else jnp.concatenate([k[HALF:], k[:HALF]], axis=0)
            KT[kc, h, LANES:] = krT if h % HALVES == 0 else krO

    @pl.when(n + 1 < G)
    def _():
        for c in copies(n + 1):
            c.start()

    HR = HALVES * BL
    R = HALVES * HR
    WK = 4 * BL
    nS = NB // 4 - 1
    row = lax.broadcasted_iota(jnp.int32, (HR, WK), 0)
    col = lax.broadcasted_iota(jnp.int32, (HR, WK), 1)
    dF = jnp.where(row < BL, b0 * BL + row, (b1 - 1) * BL + row) - col
    dS = jnp.where(row < BL, (NB - 1 - b0) * BL + row, (NB - 2 - b1) * BL + row) - col
    rF, rS = slice(0, HR), slice(HR, R)
    extra = []
    for i in range(HALVES):
        at = [tab[n, NB + 2 + 4 * i + k] for k in range(SOURCES)]
        is_first = row[:BL, :LANES] * 0 + at[3] > 0
        extra.append((at[0], at[1], row[:BL] + at[2] - col[:BL], is_first, pl.ds(i * BL, BL), pl.ds((2 + i) * BL, BL)))

    def fold(t):
        w = t.shape[1] // HALVES
        t = jnp.maximum(t[:, :w], t[:, w:])
        return t if w == LANES else fold(t)

    def p1(c):
        for h in range(H):
            q = Q[h, 2:].reshape(HR, MXU) if c else Q[h].reshape(R, MXU)
            s = jnp.dot(q, KT[c, h], preferred_element_type=F32) * scale2
            if c == 0:
                f = jnp.where(dF >= 0, s[:HR], NEG)
                sF[h] = f
                mx[h, rF] = fold(f)
                s = s[HR:]
            elif c == nS - 1:
                s = jnp.where(dS >= c * WK, s, NEG)
            sS[h, c] = s
            mx[h, rS] = jnp.maximum(mx[h, rS], fold(s)) if c else fold(s)

    def p1x():
        for h in range(H):
            for i, (block, chunk, d, is_first, r_f, r_s) in enumerate(extra):
                s = jnp.dot(Q[h, block], KT[chunk, h], preferred_element_type=F32) * scale2
                s = jnp.where(d >= 0, s, NEG)
                sX[h, i] = s
                m = fold(s)
                for r, t in ((r_f, jnp.where(is_first, m, NEG)), (r_s, jnp.where(is_first, NEG, m))):
                    t = jnp.maximum(mx[h, r], t)
                    mx[h, r] = jnp.broadcast_to(jnp.max(t, axis=1, keepdims=True), (BL, LANES))

    def weigh(load, chunk, h):
        es, ls = [], None
        for j in range(WK // LANES):
            e = jnp.exp2(load(slice(j * LANES, j * LANES + LANES)))
            ls = e if ls is None else ls + e
            es.append(e.astype(BF16))
        return ls, jnp.dot(jnp.concatenate(es, axis=1), V[chunk, :, h * LANES:h * LANES + LANES], preferred_element_type=F32)

    def p2(c):
        for h in range(H):
            def load(js):
                t = sS[h, c, :, js] - mx[h, rS]
                return t if c else jnp.concatenate([sF[h, :, js] - mx[h, rF], t], axis=0)
            ls, pv = weigh(load, c, h)
            r = rS if c else slice(0, R)
            lsum[h, r] = lsum[h, r] + ls if c else ls
            acc[h, r] = acc[h, r] + pv if c else pv

    def p2x():
        for h in range(H):
            for i, (_, chunk, _, is_first, r_f, r_s) in enumerate(extra):
                m = jnp.where(is_first, mx[h, r_f], mx[h, r_s])
                ls, pv = weigh(lambda js: sX[h, i, :, js] - m, chunk, h)
                for k, r in enumerate((r_f, r_s)):
                    pick = (lambda t: jnp.where(is_first, t, 0.0)) if k == 0 else (lambda t: jnp.where(is_first, 0.0, t))
                    l = lsum[h, r] + pick(ls)
                    total = acc[h, r] + pick(pv)
                    ob[i, k, :, h * LANES:h * LANES + LANES] = (total * (1.0 / jnp.sum(l, axis=1, keepdims=True))).astype(BF16)

    stages = [functools.partial(f, c) for f in (p1, p2) for c in range(nS)]
    stages.insert(nS, p1x)
    for k, stage in enumerate(stages + [p2x]):
        pl.when(n + k >= 0)(stage)

    @pl.when(jnp.logical_and(n > 0, n + 1 < G))
    def _():
        for k, f in zip((1, 4), o_forwards(n - 1)):
            o_sends(n - 1)[k].wait_recv()
            f.start()

    for c in o_store(n):
        c.start()

    @pl.when(n == G - 1)
    def _():
        for c in o_store(n):
            c.wait()

        def drain_forward(i, _):
            for f in o_forwards(i):
                f.wait()
            return 0

        @pl.loop(0, G - 1)
        def _(i):
            for k, s in enumerate(o_sends(i)):
                s.wait_send()
                if k in (0, 2, 3):
                    s.wait_recv()

        lax.fori_loop(0, G - 2, drain_forward, 0)
        for k in (1, 4):
            o_sends(G - 2)[k].wait_recv()
        for k, slot in enumerate((me.partner, me.left, me.right)):
            w_send(k, me.c).wait_send()
            w_send(k, slot).wait_recv()


def attention(mesh, tab, q_own, q_par, cs_own, cs_par, w_uk, w_uv, lat, wf, soft_scale):
    G, T = tab.shape[0], q_own.shape[1] * mesh.shape["cp"]
    BL = q_own.shape[1] // HALVES
    NB = T // BL
    KR, VD = w_uv.shape[0], w_uv.shape[1] // HALVES
    H = VD // LANES
    R = 4 * BL
    dims = (G, NB, BL, H // HALVES, float(soft_scale * LOG2E), mesh.shape["tp"], mesh.shape["cp"])
    blk = lambda a: pl.BlockSpec((1,) + a.shape[1:], lambda n, t: (n, 0, 0))
    hbm = pl.BlockSpec(memory_space=pltpu.HBM)
    dma = pltpu.SemaphoreType.DMA
    sds = jax.ShapeDtypeStruct
    ost = sds((G, 2, BL, VD), BF16)
    stat = pltpu.VMEM((H, R, LANES), F32)
    return pl.pallas_call(
        functools.partial(attn_kernel, dims),
        grid_spec=pltpu.PrefetchScalarGridSpec(
            num_scalar_prefetch=1, grid=(G,),
            in_specs=[blk(q_own), blk(q_par)] + [pl.BlockSpec((HALVES * BL, cs_own.shape[1]), lambda n, t: (n, 0))] * 2 + [hbm] * 4,
            out_specs=[hbm] * 4,
            scratch_shapes=[
                pltpu.VMEM((NB, BL, lat.shape[-1]), BF16), pltpu.VMEM((NB // 4, H, MXU, R), BF16), pltpu.VMEM((NB // 4, R, VD), BF16),
                pltpu.VMEM((H, 4, BL, MXU), BF16), pltpu.VMEM((H, R // HALVES, R), F32),
                pltpu.VMEM((H, NB // 4 - 1, R // HALVES, R), F32), pltpu.VMEM((H, 2, BL, R), F32), stat, stat, stat, pltpu.VMEM((HALVES, HALVES, BL, VD), BF16),
                pltpu.VMEM((KR, VD), BF16), pltpu.VMEM((VD, KR), BF16), pltpu.VMEM((KR, VD), BF16),
                dma((NB // HALVES,)), dma((HALVES,)), dma((HALVES,)), dma((G, 7)), dma((G, 7)), dma((3,)), dma((3,))],
        ),
        out_shape=[ost, ost, sds((4, 2, G, BL, VD), BF16), sds((mesh.shape["cp"],) + wf.shape, BF16)],
        compiler_params=pltpu.CompilerParams(collective_id=1, has_side_effects=True, vmem_limit_bytes=63 * MIB),
        cost_estimate=pl.CostEstimate(flops=G * H * T * R * 800, bytes_accessed=G * T * 640 * 2, transcendentals=0),
        name="attn",
    )(tab, q_own, q_par, cs_own, cs_par, w_uk, w_uv, lat, wf)


def proj_kernel(dims, pos, x, w_dq, w_dkv, w_uq, gq, gkv, fr, w_o,
                lat_all, latent, k_rope, q_own, q_par, wf, cs_own, cs_par, qn_o, qn_p,
                xbuf, wdq, wdkv, wuq, csb, pay, krb, kvb, qlat, qn, qst,
                xsem, wsem, dsem, csem, osem, wss, wrs, lss, lrs, qss, qrs, css, crs, lsem):
    n_tp, n_cp, n_t, half_cols, wc = dims
    me = Place(n_tp, n_cp)
    y, c, partner, right, left, far = me.y, me.c, me.partner, me.right, me.left, me.far

    rows = xbuf.shape[1]
    bl = pay.shape[3]
    kr_rank = gkv.shape[0]
    nj = WIDE
    last = n_t - 1
    every = HALVES * n_t

    def load_x(i):
        return pltpu.make_async_copy(x.at[pl.ds(pl.multiple_of(lax.rem(i, n_t) * rows, rows), rows), :], xbuf.at[lax.rem(i, HALVES)],
                                     xsem.at[lax.rem(i, HALVES)])

    kv_load = pltpu.make_async_copy(w_dkv, wdkv, wsem.at[0])
    kv_load.start()
    load_x(0).start()
    me.greet([(me.up, c), (me.dn, c), (me.dg, c), (y, partner), (y, right), (y, left)])
    half = lax.rem(y, HALVES)
    col_opp = pl.multiple_of((1 - half) * half_cols + c * wc, LANES)
    col_same = pl.multiple_of(half * half_cols + c * wc, LANES)
    w_sends = [me.copy(w_o.at[:, pl.ds(col, wc)], wf.at[k], wss.at[k], wrs.at[k], yy, c)
               for k, (col, yy) in enumerate(((col_opp, me.dn), (col_opp, me.up), (col_same, me.dg)))]
    for s in w_sends:
        s.start()

    def dq_load(j):
        cols = pl.ds(pl.multiple_of(j * nj, nj), nj)
        return pltpu.make_async_copy(w_dq.at[:, cols], wdq.at[:, cols], dsem.at[j])

    late = [pltpu.make_async_copy(w_uq.at[:, pl.ds(pl.multiple_of(me.core * wuq.shape[1], LANES), wuq.shape[1])], wuq, wsem.at[1])]

    def bid(n):
        return lax.div(pos[n, 0], bl)

    lane_b = lax.broadcasted_iota(jnp.int32, (bl, LANES), 1)
    row_b = lax.broadcasted_iota(jnp.int32, (bl, LANES), 0)
    sign = jnp.where(lax.rem(lane_b, HALF) < QUARTER, -1.0, 1.0)

    @pl.loop(0, every)
    def _(n):
        for k in range(HALVES):
            b = bid(n) if k == 0 else HALVES * n_cp - 1 - bid(n)
            ang = (b * bl + row_b).astype(F32) * fr[...]
            r = pl.ds(pl.multiple_of((HALVES * n + k) * bl, bl), bl)
            csb[r, :LANES] = jnp.cos(ang)
            csb[r, LANES:] = jnp.sin(ang) * sign

    cs_store = pltpu.make_async_copy(csb, cs_own, csem)
    cs_store.start()
    kv_load.wait()
    cs_store.wait()
    cs_send = me.copy(cs_own, cs_par, css, crs, y, partner)
    cs_send.start()

    lane = lax.broadcasted_iota(jnp.int32, (rows, LANES), 1)
    low32 = lax.rem(lane, HALF) < QUARTER
    upper = lax.broadcasted_iota(jnp.int32, (rows, LANES), 0) < rows // HALVES
    tile = lambda t: pl.ds(t * 2, HALVES)
    block = lambda t: pl.ds(pl.multiple_of(t * rows, rows), rows)

    def norm(t32, gain):
        return (t32 * lax.rsqrt(jnp.mean(t32 * t32, axis=-1, keepdims=True) + NORM_EPS) * gain).astype(BF16)

    def lat_copy(k, i, t, ref, yy, cc):
        return me.copy(ref, ref, lss.at[t, k], lrs.at[t, i], yy, cc)

    def own_store(t):
        return pltpu.make_async_copy(pay.at[lax.rem(t, HALVES)], lat_all.at[c, tile(t)], lsem.at[t])

    def out_stores(t):
        sl = lax.rem(t, HALVES)
        return [pltpu.make_async_copy(pay.at[sl, :, :, :, :kr_rank], latent.at[tile(t)], osem.at[0, sl]),
                pltpu.make_async_copy(krb.at[sl], k_rope.at[block(t)], osem.at[1, sl])]

    def send_own(t):
        own_store(t).wait()
        for k, cc in ((0, partner), (1, left), (2, right)):
            lat_copy(k, k, t, lat_all.at[c, tile(t)], y, cc).start()

    def settle_stores(t):
        for s in out_stores(t):
            s.wait()

    @pl.loop(0, n_t)
    def _(t):
        load_x(t).wait()

        pl.when(t == 0)(lambda: load_x(1).start())

        @pl.when(t == 1)
        def _():
            for j in range(wdq.shape[1] // nj):
                dq_load(j).start()
            for d in late:
                d.start()

        pl.when(t > 0)(lambda: send_own(t - 1))

        sl = lax.rem(t, HALVES)

        def kv_dot(wrows):
            d = lax.dot_general(xbuf[sl], wdkv[wrows, :], (((1,), (1,)), ((), ())), preferred_element_type=F32)
            return d.astype(BF16)

        @pl.loop(0, kr_rank // nj)
        def _(j):
            js = pl.ds(pl.multiple_of(j * nj, nj), nj)
            kvb[:, js] = kv_dot(js)

        u = kv_dot(pl.ds(kr_rank, wdkv.shape[0] - kr_rank)).astype(F32)
        pl.when(t + HALVES < n_t)(lambda: load_x(t + 2).start())
        lat = norm(kvb[...].astype(F32), gkv[...])
        u = jnp.concatenate([u, u], axis=1)
        w = jnp.where(low32, pltpu.roll(u, 96, 1), pltpu.roll(u, QUARTER, 1))
        rot = u * csb[block(t), :LANES] + w * csb[block(t), LANES:]
        pl.when(t >= HALVES)(lambda: settle_stores(t - 2))
        krb[sl] = rot[:, :HALF].astype(BF16)
        pay[sl, :, :, :, :kr_rank] = lat.reshape(HALVES, HALVES, bl, kr_rank)
        ids = jnp.where(upper, bid(HALVES * t), bid(HALVES * t + 1)).astype(F32)
        pay[sl, :, :, :, kr_rank:] = jnp.where(lane < HALF, rot, ids).astype(BF16).reshape(HALVES, HALVES, bl, LANES)
        for s in [own_store(t)] + out_stores(t):
            s.start()

    send_own(last)
    for d in late:
        d.wait()

    def stage1(t):
        rp, lp = lat_all.at[right, tile(t)], lat_all.at[left, tile(t)]
        lat_copy(3, 1, t, rp, y, partner).wait_recv()
        lat_copy(3, 2, t, lp, y, partner).wait_recv()
        for k, ref, cc in ((5, lat_all.at[left, tile(t), 0], right), (6, lat_all.at[right, tile(t), 1], left), (3, rp, partner), (4, lp, partner)):
            lat_copy(k, k, t, ref, y, cc).start()

    def stage2(t):
        for k in range(HALVES):
            ref = lat_all.at[far, tile(t), k]
            lat_copy(SPARE, 5 + k, t, ref, y, partner).wait_recv()
            lat_copy(7 + k, 7 + k, t, ref, y, partner).start()

    def project(src, wref, dst, width, before=None):
        @pl.loop(0, wref.shape[1] // width)
        def _(j):
            if before is not None:
                before(j)
            cols = pl.ds(pl.multiple_of(j * width, width), width)
            dst[:, cols] = jnp.dot(src[...], wref[:, cols], preferred_element_type=F32).astype(BF16)

    def q_store(u, dst, t):
        return pltpu.make_async_copy(qst.at[lax.rem(u, HALVES)], dst.at[block(t)], osem.at[3, lax.rem(u, HALVES)])

    def q_send(t):
        return me.copy(qn_o.at[block(t)], qn_p.at[block(t)], qss.at[t], qrs.at[t], y, partner)

    @pl.loop(0, n_t)
    def _(t):
        v = last - t
        pl.when(t >= HALVES)(lambda: load_x(v).wait())
        project(xbuf.at[lax.rem(v, HALVES)], wdq, qlat, nj, lambda j: pl.when(t == 0)(lambda: dq_load(j).wait()))
        pl.when(v >= HALVES)(lambda: load_x(v - 2).start())

        @pl.when(t == 0)
        def _():
            for k in (last - 1, last):
                settle_stores(k)

        stage1(t)
        sl = lax.rem(t, HALVES)
        qn[sl] = norm(qlat[...].astype(F32), gq[...])
        cp = pltpu.make_async_copy(qn.at[sl], qn_o.at[block(v)], osem.at[2, sl])
        cp.start()
        pl.when(t >= HALVES)(lambda: q_store(t, q_own, t - 2).wait())
        project(qn.at[sl], wuq, qst.at[sl], wuq.shape[1] // HALVES)
        cp.wait()
        q_send(v).start()
        q_store(t, q_own, v).start()

    def load_qp(t):
        return pltpu.make_async_copy(qn_p.at[block(last - t)], qn.at[lax.rem(t, HALVES)], osem.at[2, lax.rem(t, HALVES)])

    def take_qp(t):
        q_send(last - t).wait_recv()
        load_qp(t).start()

    take_qp(0)

    @pl.loop(0, n_t)
    def _(t):
        load_qp(t).wait()
        pl.when(t + 1 < n_t)(lambda: take_qp(t + 1))
        q_store(n_t + t, q_own, t).wait()
        project(qn.at[lax.rem(t, HALVES)], wuq, qst.at[lax.rem(n_t + t, HALVES)], wuq.shape[1] // HALVES)
        q_store(n_t + t, q_par, last - t).start()
        stage2(t)

    for k in range(HALVES):
        q_store(k, q_par, 0).wait()

    pr, pl_, pf = (lax.rem(partner + k, n_cp) for k in (HALVES, n_cp - 2, n_cp // HALVES))

    @pl.loop(0, n_t)
    def _(t):
        whole, part = lat_all.at[c, tile(t)], lat_all.at[c, tile(t), 0]
        for i, ref in ((0, lat_all.at[partner, tile(t)]), (3, lat_all.at[pr, tile(t)]), (4, lat_all.at[pl_, tile(t)]),
                       (7, lat_all.at[pf, tile(t), 0]), (8, lat_all.at[pf, tile(t), 1])):
            lat_copy(SPARE, i, t, ref, y, partner).wait_recv()
        for k in range(9):
            lat_copy(k, k, t, whole if k < 5 else part, y, partner).wait_send()
        q_send(t).wait_send()

    for s in w_sends + [cs_send]:
        s.wait()


def project_all(mesh, pos, x, w_dq, w_dkv, w_uq, g_q, g_kv, freq, w_o, bl):
    n_tp, n_cp = mesh.shape["tp"], mesh.shape["cp"]
    n_seq, seq, width = x.shape
    rows = HALVES * seq
    n_t = n_seq // HALVES
    rank, kvw = w_dq.shape[1], w_dkv.shape[1]
    kr = g_kv.shape[0]
    qw = w_uq.shape[1] // HALVES
    half_cols = width // HALVES
    wc = half_cols // n_cp
    total = n_seq * seq
    hbm = pl.BlockSpec(memory_space=pltpu.HBM)
    sds = jax.ShapeDtypeStruct
    dma = pltpu.SemaphoreType.DMA
    trig = sds((total, MXU), F32)
    return pl.pallas_call(
        functools.partial(proj_kernel, (n_tp, n_cp, n_t, half_cols, wc)),
        in_specs=[pl.BlockSpec(memory_space=pltpu.SMEM)] + [hbm] * 4 + [pl.BlockSpec(memory_space=pltpu.VMEM)] * 3 + [hbm],
        out_specs=[hbm] * 10,
        out_shape=[sds((n_cp, n_seq, 2, bl, kr + LANES), BF16), sds((n_seq, 2, bl, kr), BF16), sds((total, kvw - kr), BF16),
                   sds((total, qw), BF16), sds((total, qw), BF16), sds((3, w_o.shape[0], wc), BF16),
                   trig, trig, sds((total, rank), BF16), sds((total, rank), BF16)],
        scratch_shapes=[
            pltpu.VMEM((HALVES, rows, width), BF16), pltpu.VMEM((width, rank), BF16), pltpu.VMEM((kvw, width), BF16),
            pltpu.VMEM((rank, qw), BF16), pltpu.VMEM(trig.shape, F32), pltpu.VMEM((HALVES, HALVES, 2, bl, kr + LANES), BF16),
            pltpu.VMEM((HALVES, rows, kvw - kr), BF16), pltpu.VMEM((rows, kr), BF16), pltpu.VMEM((rows, rank), BF16),
            pltpu.VMEM((HALVES, rows, rank), BF16), pltpu.VMEM((HALVES, rows, qw), BF16),
            dma((HALVES,)), dma((HALVES,)), dma((rank // WIDE,)), dma, dma((4, HALVES)), dma((3,)), dma((3,)), dma((n_t, 9)), dma((n_t, 9)),
            dma((n_t,)), dma((n_t,)), dma, dma, dma((n_t,))],
        compiler_params=pltpu.CompilerParams(collective_id=0, has_side_effects=True, vmem_limit_bytes=63 * MIB),
        cost_estimate=pl.CostEstimate(flops=HALVES * total * (width * (rank + kvw) + HALVES * rank * qw), bytes_accessed=10**8,
                                      transcendentals=0),
        name="proj",
    )(pos, x.reshape(total, width), w_dq, w_dkv.T, w_uq, g_q, g_kv, freq, w_o)


def out_kernel(dims, x, w_o, wf, wx, ost_own, ost_par, obuf, out, wy, oy,
               wbuf, ov, xb, stage, wsem, osem, xsem, ssem, oss, ors, wss, wrs, ass, ars):
    n_tp, n_cp, n_seq, bl, half_cols = dims
    me = Place(n_tp, n_cp)
    cols, kb = xb.shape[-1], obuf.shape[-1]
    w, krows = cols // HALVES, w_o.shape[0]
    hk = krows // HALVES
    last = n_seq - 1
    half_of = lambda row: lax.rem(row, HALVES)
    tb = me.block(me.y, me.core)

    to_last = lambda s, p: oy.at[s, p, 1]
    to_prev = lambda s, p: oy.at[s, p, 0]
    prev_fwd = me.o_forwards(lambda s, p: obuf.at[s, p, last - 1], to_prev, oss.at[0], ors.at[0])
    last_sends = me.o_sends(ost_own.at[last], ost_par.at[last], to_last, oss.at[1], ors.at[1])
    last_fwd = me.o_forwards(to_last, to_last, oss.at[1], ors.at[1])
    def w_copy(k, src, dst, yy, cc):
        return me.copy(src, dst, wss.at[k], wrs.at[k], yy, cc)

    far_rows = pl.ds(0, hk), pl.ds(hk, hk)
    (to_r, to_l), (rest_r, rest_l) = w_parts(krows)
    p_right, p_left, p_far = (lax.rem(me.partner + k, n_cp) for k in (HALVES, n_cp - 2, n_cp // HALVES))
    mine, side = (me.y, me.partner), ((me.y, me.right), (me.y, me.left))

    def w_move(k, buf, dev, part, to):
        return w_copy(k, buf.at[dev, :, part], wy.at[dev, :, part], *to)

    w_sends = [w_copy(0, wf.at[:, rest_r], wy.at[me.c, :, rest_r], *side[0]), w_copy(1, wf.at[:, rest_l], wy.at[me.c, :, rest_l], *side[1]),
               w_move(2, wx, me.left, to_r, mine), w_move(3, wx, me.right, to_l, mine),
               w_move(4, wx, me.left, far_rows[0], side[0]), w_move(5, wx, me.right, far_rows[1], side[1])]
    rest_fwd = [w_move(6, wy, me.left, rest_r, mine), w_move(7, wy, me.right, rest_l, mine)]
    far_fwd = [w_move(8 + k, wy, me.far, far_rows[k], mine) for k in range(HALVES)]

    def w_recv(k, dev, part):
        w_move(k, wy, dev, part, mine).wait_recv()

    n_m = n_seq // HALVES
    rows = HALVES * bl
    k_of = (None, me.flip, 1 - me.flip, HALVES)
    every = pl.ds(0, krows)
    own = ((wx, to_l), (wy, rest_l)), ((wx, to_r), (wy, rest_r))
    pieces = ((((wf, every),), ((wx.at[me.partner], every),)),) + tuple(
        (tuple((buf.at[dev], part) for buf, part in own[i]), ((wy.at[dev_p], every),))
        for i, (dev, dev_p) in enumerate(((me.right, p_right), (me.left, p_left)))) + ((((wy.at[me.far], every),), ((wy.at[p_far], every),)),)
    offs = [pl.multiple_of(v * w, LANES) for v in (me.core, 1 - me.core)]

    def col_of(j, row):
        dx = j + (j // HALVES) * (1 - HALVES * (j % HALVES))
        xq = lax.rem(lax.div(me.c, HALVES) + dx, n_cp // HALVES)
        return pl.multiple_of(half_of(row) * half_cols + xq * cols, LANES)

    def w_loads(j):
        b = j % HALVES
        out_ = [pltpu.make_async_copy(w_o.at[:, pl.ds(col_of(j, me.y), cols)], wbuf.at[b, 0], wsem.at[b, 0])]
        for r in range(1, 4):
            for part in range(HALVES):
                for i, (buf, part_rows) in enumerate(pieces[j][part]):
                    out_.append(pltpu.make_async_copy(buf.at[k_of[r], part_rows], wbuf.at[b, r, part_rows, pl.ds(offs[part], w)],
                                                      wsem.at[b, HALVES * r + part + 8 * i]))
        return out_

    def x_load(j):
        return pltpu.make_async_copy(x.at[:, pl.ds(pl.multiple_of(tb * bl, bl), bl), pl.ds(col_of(j, me.y), cols)], xb.at[j % HALVES], xsem.at[j % HALVES])

    o_offs = [pl.multiple_of(v * kb, LANES) for v in (me.core, 1 - me.core)]

    def o_loads(n0, cnt, refs):
        out_ = []
        for i in range(cnt):
            for r in range(SOURCES):
                for part in range(HALVES):
                    src = ost_own.at[n0 + i, tb] if (r, part) == (0, 0) else refs(r, part, n0 + i)
                    out_.append(pltpu.make_async_copy(src, ov.at[n0 + i, :, pl.ds(pl.multiple_of(r * krows + o_offs[part], LANES), kb)],
                                                      osem.at[n0 + i, HALVES * r + part]))
        return out_

    early = o_loads(0, last - 1, lambda r, p, i: obuf.at[r, p, i])
    late = o_loads(last - 1, 2, lambda r, p, i: oy.at[r, p, i - last + 1] if (i == last or r == 3) else obuf.at[r, p, i])
    for d in w_loads(0) + early + [x_load(0)]:
        d.start()
    me.greet(((me.up, me.c), (me.dn, me.c), (me.up, me.partner), (me.dn, me.partner),
              (me.y, me.partner), (me.y, me.right), (me.y, me.left)))
    for s in last_sends + prev_fwd + w_sends:
        s.start()

    def region(row, j, m, n0=0, cnt=2):
        return out.at[pl.ds(HALVES * m + n0, cnt), pl.ds(pl.multiple_of(me.block(row, me.core) * bl, bl), bl), pl.ds(col_of(j, row), cols)]

    def ring(k, ref, j, m, yy):
        i = j * n_m + m
        return me.copy(ref, ref, ass.at[i, k], ars.at[i, k], yy, me.c)

    def tile_sends(j, m):
        ref = region(me.y, j, m)
        return ring(0, ref, j, m, me.up), ring(1, ref, j, m, me.dn)

    def forward(j, m):
        ring(0, region(me.dn, j, m), j, m, me.up).wait_recv()
        ring(2, region(me.dn, j, m, 0, 1), j, m, me.up).start()
        ring(1, region(me.up, j, m), j, m, me.up).wait_recv()
        ring(3, region(me.up, j, m, 1, 1), j, m, me.dn).start()

    nt = MXU

    def tile(j, m):
        b = j % HALVES

        @pl.loop(0, cols // nt)
        def _(t):
            cs_ = pl.ds(pl.multiple_of(t * nt, nt), nt)
            a = ov[pl.ds(HALVES * m, HALVES)].reshape(rows, 4 * krows)
            s = None
            for r in range(SOURCES):
                d = jnp.dot(a[:, r * krows:(r + 1) * krows], wbuf[b, r, :, cs_], preferred_element_type=F32)
                s = d if s is None else s + d
            xr = xb[b, pl.ds(HALVES * m, HALVES), :, cs_].reshape(rows, nt).astype(F32)
            stage[:, :, cs_] = (xr + s).astype(BF16).reshape(2, bl, nt)

        c = pltpu.make_async_copy(stage, region(me.y, j, m), ssem)
        c.start()
        c.wait()
        for s in tile_sends(j, m):
            s.start()

    def need(j):
        if j == 0:
            w_recv(1, me.right, rest_l)
            rest_fwd[1].start()
            w_recv(3, p_right, to_l)
            w_recv(7, p_right, rest_l)
        elif j == 1:
            w_recv(0, me.left, rest_r)
            rest_fwd[0].start()
            w_recv(2, p_left, to_r)
            w_recv(6, p_left, rest_r)
        else:
            for k in range(HALVES):
                w_recv(4 + k, me.far, far_rows[k])
                far_fwd[k].start()
            for k in range(HALVES):
                w_recv(8 + k, p_far, far_rows[k])
        for d in w_loads(j + 1) + [x_load(j + 1)]:
            d.start()

    def late_o():
        for k in (0, 2, 3):
            last_sends[k].wait_recv()
        for f in prev_fwd + last_fwd:
            f.wait_recv()
        for d in late:
            d.start()
        for d in late:
            d.wait()

    for k, f in zip((1, 4), last_fwd):
        last_sends[k].wait_recv()
        f.start()
    for d in early:
        d.wait()

    @pl.loop(0, 4 * n_m)
    def _(i):
        j, m = lax.div(i, n_m), lax.rem(i, n_m)
        for jj in range(SOURCES):
            @pl.when(i == jj * n_m)
            def _(jj=jj):
                for d in w_loads(jj) + [x_load(jj)]:
                    d.wait()
                if jj == 1:
                    need(jj)
        pl.when(i == n_m - 1)(late_o)
        tile(j, m)
        pl.when(i == 0)(lambda: need(0))

        @pl.when(j > 0)
        def _():
            forward(j - 1, m)

        pl.when(i == 3 * n_m - 1)(lambda: need(2))

    @pl.loop(0, n_m)
    def _(m):
        forward(3, m)

    @pl.loop(0, 4 * n_m)
    def _(i):
        j, m = lax.div(i, n_m), lax.rem(i, n_m)
        for k, row, n0, cnt in ((0, me.y, 0, HALVES), (1, me.y, 0, HALVES), (2, me.dn, 0, 1), (3, me.up, 1, 1)):
            r = region(row, j, m, n0, cnt)
            me.copy(r, r, ass.at[i, k], ars.at[i, k], me.up, me.c).wait_send()
        for k, n0 in ((HALVES, 0), (3, 1)):
            r = region(me.dg, j, m, n0, 1)
            me.copy(r, r, ass.at[i, k], ars.at[i, k], me.up, me.c).wait_recv()

    for s in last_sends + prev_fwd + last_fwd + w_sends + rest_fwd + far_fwd:
        s.wait_send()


def out_product(mesh, x, w_o, wf, wx, ost_own, ost_par, obuf):
    n_tp, n_cp = mesh.shape["tp"], mesh.shape["cp"]
    n_seq, seq, width = x.shape
    bl = seq // HALVES
    cols = HALVES * wf.shape[-1]
    krows = w_o.shape[0]
    hbm = pl.BlockSpec(memory_space=pltpu.HBM)
    dma = pltpu.SemaphoreType.DMA
    sds = jax.ShapeDtypeStruct
    tiles = HALVES * n_seq
    return pl.pallas_call(
        functools.partial(out_kernel, (n_tp, n_cp, n_seq, bl, width // HALVES)),
        in_specs=[hbm] * 7, out_specs=[hbm] * 3,
        out_shape=[sds(x.shape, BF16), sds(wx.shape, BF16), sds((4, 2, HALVES) + obuf.shape[3:], BF16)],
        scratch_shapes=[
            pltpu.VMEM((HALVES, 4, krows, cols), BF16), pltpu.VMEM((n_seq, bl, 4 * krows), BF16), pltpu.VMEM((HALVES, n_seq, bl, cols), BF16),
            pltpu.VMEM((HALVES, bl, cols), BF16), dma((HALVES, 16)), dma((n_seq, 8)), dma((HALVES,)), dma, dma((HALVES, 7)), dma((HALVES, 7)),
            dma((10,)), dma((10,)), dma((tiles, 4)), dma((tiles, 4))],
        compiler_params=pltpu.CompilerParams(collective_id=2, has_side_effects=True, vmem_limit_bytes=63 * MIB),
        cost_estimate=pl.CostEstimate(flops=n_seq * seq * cols * 16 * krows, bytes_accessed=10**8, transcendentals=0),
        name="outp",
    )(x, w_o, wf, wx, ost_own, ost_par, obuf)[0]


def settle_kernel(src, lat, kr, dst, lat_out, kr_out, buf, lbuf, kbuf, tbuf, rsem, wsem, lsem, ksem):
    n = buf.shape[0]
    reads = [pltpu.make_async_copy(src.at[i], buf.at[i], rsem.at[i]) for i in range(n)]
    writes = [pltpu.make_async_copy(buf.at[i], dst.at[i], wsem.at[i]) for i in range(n)]
    small = [pltpu.make_async_copy(*p) for p in ((kr, kbuf, ksem.at[0]), (lat, lbuf, lsem.at[0]))]
    small_out = [pltpu.make_async_copy(*p) for p in ((tbuf, kr_out, ksem.at[1]), (lbuf, lat_out, lsem.at[1]))]
    for d in small + reads:
        d.start()
    for d in small:
        d.wait()
    for i in range(tbuf.shape[0]):
        tbuf[i] = kbuf[i].astype(F32).T.astype(BF16)
    for d in small_out:
        d.start()
    for a, b in zip(reads, writes):
        a.wait()
        b.start()
    for d in writes + small_out:
        d.wait()


def settle(out, lat, kr):
    n_seq, seq, width = out.shape
    parts = 4 * n_seq
    shape = (parts, n_seq * seq // parts, width)
    lat_shape, kr_shape = (n_seq, seq, lat.shape[-1]), (n_seq, seq, kr.shape[-1])
    turned = (n_seq, kr.shape[-1], seq)
    hbm = pl.BlockSpec(memory_space=pltpu.HBM)
    sds = jax.ShapeDtypeStruct
    dma = pltpu.SemaphoreType.DMA
    a, b, c = pl.pallas_call(
        settle_kernel, in_specs=[hbm] * 3, out_specs=[hbm] * 3,
        out_shape=[sds(shape, BF16), sds(lat_shape, BF16), sds(turned, BF16)],
        scratch_shapes=[pltpu.VMEM(shape, BF16), pltpu.VMEM(lat_shape, BF16), pltpu.VMEM(kr_shape, BF16), pltpu.VMEM(turned, BF16),
                        dma((parts,)), dma((parts,)), dma((HALVES,)), dma((HALVES,))],
        compiler_params=pltpu.CompilerParams(vmem_limit_bytes=63 * MIB), name="settle",
    )(out.reshape(shape), lat.reshape(lat_shape), kr.reshape(kr_shape))
    return a.reshape(out.shape), b, jnp.swapaxes(c, 1, HALVES)


ROPE_BASE = 10000.0


def solution(mesh):
    def local_step(x, pos, w_dq, g_q, w_uq, w_dkv, g_kv, w_uk, w_uv, w_o):
        n_seq, seq, _ = x.shape
        n_cp = mesh.shape["cp"]
        bl = seq // HALVES
        nb = HALVES * n_cp
        kv_rank = g_kv.shape[0]
        rope = w_dkv.shape[1] - kv_rank
        heads = (w_uq.shape[1] - w_uk.shape[1]) // rope
        nope = w_uk.shape[1] // heads
        c = lax.axis_index("cp")
        core = c % HALVES

        freq = np.tile(ROPE_BASE ** (-2.0 * np.arange(rope // HALVES) / rope), LANES // (rope // HALVES))[None].astype(np.float32)
        lat_all, latent, k_rope, q_own, q_par, wf, cs_own, cs_par, _, _ = project_all(
            mesh, pos, x, w_dq, w_dkv, w_uq, g_q, g_kv, freq, w_o, bl)
        q_own, q_par = (a.reshape(n_seq, seq, -1) for a in (q_own, q_par))
        ids = lat_all[:, :, 0, 0, kv_rank + rope].astype(jnp.int32)
        blocks = jnp.arange(nb)
        first = ids[:, :, None] == blocks
        second = nb - 1 - ids[:, :, None] == blocks
        dev = jnp.arange(n_cp)[:, None, None]
        slots = jnp.sum(jnp.where(first, HALVES * dev, 0) + jnp.where(second, HALVES * dev + 1, 0), axis=0)
        mine = [jnp.sum(jnp.where(jnp.arange(n_cp)[:, None] == k, ids, 0), axis=0) for k in (c, c ^ 1)]
        last = nb // 4 - 1
        extra = []
        for i, b in enumerate(mine):
            is_first = b > last
            chunk = jnp.where(is_first, 1, last)
            extra += [jnp.where(is_first, i, 2 + i), chunk, jnp.where(is_first, b, nb - 1 - b) * bl - chunk * 4 * bl, is_first]
        tab = jnp.concatenate([slots, jnp.stack(mine + extra, axis=1).astype(jnp.int32)], axis=1).astype(jnp.int32)

        ost_own, ost_par, obuf, wx = attention(mesh, tab, q_own, q_par, cs_own, cs_par, w_uk, w_uv, lat_all, wf, (nope + rope) ** -0.5)
        return settle(out_product(mesh, x, w_o, wf, wx, ost_own, ost_par, obuf), latent, k_rope)

    seq_spec = P("dp", "cp", None)
    whole = P(None, None)
    in_specs = (seq_spec, P("dp", "cp"), whole, P(None), P(None, "tp"), whole, P(None), P(None, "tp"), P(None, "tp"), P("tp", None))
    return jax.shard_map(local_step, mesh=mesh, in_specs=in_specs, out_specs=(seq_spec,) * 3, check_vma=False)
```

```python
import functools
import numpy as np
import jax, jax.numpy as jnp
from jax import lax
from jax.experimental import pallas as pl
from jax.experimental.pallas import tpu as pltpu
from jax.sharding import PartitionSpec as P

F32, BF16 = jnp.float32, jnp.bfloat16
NEG = float("-inf")
LOG2E = 1.4426950408889634
LANES, HALF, QUARTER, MXU, WIDE, PAIR = 128, 64, 32, 256, 512, 384
HALVES = 2
SOURCES = 4
MIB = 2**20
SPARE = 7


MESH = pl.DeviceIdType.MESH
NORM_EPS = 1e-6


class Place:
    def __init__(self, n_tp, n_cp):
        self.dp, self.y, self.c = (lax.axis_index(a) for a in ("dp", "tp", "cp"))
        y, c = self.y, self.c
        self.n_tp = n_tp
        self.core = lax.rem(c, HALVES)
        self.partner = c + 1 - HALVES * self.core
        self.right, self.left, self.far = (lax.rem(c + k, n_cp) for k in (HALVES, n_cp - 2, n_cp // HALVES))
        self.up, self.dn, self.dg = (lax.rem(y + k, n_tp) for k in (1, n_tp - 1, n_tp // HALVES))
        self.flip = lax.rem(y + self.core, HALVES)
        self.mate = lax.rem(y + 1 + HALVES * self.flip, n_tp)
        self.other = lax.rem(y + 3 - HALVES * self.flip, n_tp)

    def block(self, row, core):
        return lax.div(lax.rem(row + (self.n_tp - 1) * core, self.n_tp), HALVES)

    def greet(self, peers):
        barrier = pltpu.get_barrier_semaphore()
        for yy, cc in peers:
            pl.semaphore_signal(barrier, inc=1, device_id=(self.dp, yy, cc), device_id_type=MESH)
        pl.semaphore_wait(barrier, len(peers))

    def copy(self, src, dst, ss, rs, yy, cc):
        return pltpu.make_async_remote_copy(src_ref=src, dst_ref=dst, send_sem=ss, recv_sem=rs,
                                            device_id=(self.dp, yy, cc), device_id_type=MESH)

    def o_sends(self, own, par, dst, ss, rs):
        tb, tp = self.block(self.y, self.core), self.block(self.y, 1 - self.core)
        ways = [(own, tb, 1, 0, self.mate, self.c), (own, 1 - tb, 2, 0, self.other, self.c), (par, tp, 0, 1, self.y, self.partner),
                (par, tp, 1, 1, self.other, self.partner), (par, 1 - tp, 2, 1, self.mate, self.partner)]
        return [self.copy(a.at[blk], dst(src, part), ss.at[k], rs.at[k], yy, cc)
                for k, (a, blk, src, part, yy, cc) in enumerate(ways)]

    def o_forwards(self, src, dst, ss, rs):
        return [self.copy(src(2, part), dst(3, part), ss.at[5 + part], rs.at[5 + part], self.mate, self.c) for part in range(HALVES)]


def w_parts(rows):
    cut = rows // 8
    return (pl.ds(0, rows - cut), pl.ds(cut, rows - cut)), (pl.ds(rows - cut, cut), pl.ds(0, cut))


def attn_kernel(dims, tab, *refs):
    G, NB, BL, HP, scale2, n_tp, n_cp = dims
    CK = HALVES * BL
    H, HG = HALVES * HP, HP
    q_own, q_par, cs_own, cs_par, w_uk, w_uv, lat, wf = refs[:8]
    ost_own, ost_par, obuf, wx = refs[8:12]
    latbuf, KT, V, Q, sF, sS, sX, mx, lsum, acc, ob, wk, wkT, wv, sem, ksem, osem, oss, ors, wss, wrs = refs[12:]
    n, g = pl.program_id(0), pl.program_id(1)
    u, U = HALVES * n + g, HALVES * G
    me = Place(n_tp, n_cp)
    rows_ = ((me.up, me.c), (me.dn, me.c), (me.up, me.partner), (me.dn, me.partner))
    w_to = ((me.y, me.partner), (me.y, me.right), (me.y, me.left))

    krows = wf.shape[1]
    w_rows = (pl.ds(0, krows),) + w_parts(krows)[0]

    def w_send(k, slot):
        return me.copy(wf.at[:, w_rows[k]], wx.at[slot, :, w_rows[k]], wss.at[k], wrs.at[k], *w_to[k])

    def copies(i):
        return [pltpu.make_async_copy(lat.at[p, i], latbuf.at[pl.ds(HALVES * p, HALVES)], sem.at[p]) for p in range(n_cp)]

    def unit(ref, i):
        w = ob.shape[-1]
        return ref.at[lax.div(i, HALVES), :, :, pl.ds(pl.multiple_of(lax.rem(i, HALVES) * w, LANES), w)]

    def landing(i):
        w = ob.shape[-1]
        return lambda s, p: obuf.at[s, p, lax.div(i, HALVES), :, pl.ds(pl.multiple_of(lax.rem(i, HALVES) * w, LANES), w)]

    def o_store(i):
        return [pltpu.make_async_copy(ob.at[k], unit(dst, i), osem.at[k]) for k, dst in enumerate((ost_own, ost_par))]

    def o_sends(i):
        return me.o_sends(unit(ost_own, i), unit(ost_par, i), landing(i), oss.at[i], ors.at[i])

    def o_forwards(i):
        return me.o_forwards(landing(i), landing(i), oss.at[i], ors.at[i])

    hw = wv.shape[1]
    kv_loads = [pltpu.make_async_copy(a.at[:, pl.ds(pl.multiple_of(me.core * hw, LANES), hw)], b, ksem.at[k])
                for k, (a, b) in enumerate(((w_uk, wk), (w_uv, wv)))]

    @pl.when(u == 0)
    def _():
        for c in copies(0) + kv_loads:
            c.start()
        me.greet(rows_ + w_to)
        for k in range(3):
            w_send(k, me.c).start()
        for c in kv_loads:
            c.wait()
        wkT[...] = wk[...].T

    @pl.when(g == 0)
    def _():
        lane = lax.broadcasted_iota(jnp.int32, (BL, LANES), 1)
        low64 = lane < HALF
        low32 = lax.rem(lane, HALF) < QUARTER
        for src_i, (q, cs) in enumerate(((q_own, cs_own), (q_par, cs_par))):
            @pl.loop(0, HALVES)
            def _(half, src_i=src_i, q=q, cs=cs):
                r0 = half * 2 + src_i
                rows = pl.ds(pl.multiple_of(half * BL, BL), BL)
                ct = cs[rows, :LANES]
                st = cs[rows, LANES:]
                for p in range(HP):
                    a = q[0, rows, p * PAIR:p * PAIR + LANES]
                    b = q[0, rows, p * PAIR + LANES:p * PAIR + MXU].astype(F32)
                    c = q[0, rows, p * PAIR + MXU:p * PAIR + PAIR].astype(F32)
                    u = jnp.where(low64, b, c)
                    no = jnp.where(low64, c, b).astype(BF16)
                    w = jnp.where(low32, pltpu.roll(u, 96, 1), pltpu.roll(u, QUARTER, 1))
                    rot = (u * ct + w * st).astype(BF16)
                    Q[HALVES * p, r0, :, :LANES] = a
                    Q[HALVES * p, r0, :, LANES:MXU] = rot
                    Q[HALVES * p + 1, r0, :, :LANES] = no
                    Q[HALVES * p + 1, r0, :, LANES:MXU] = rot

        for c in copies(n):
            c.wait()

    @pl.when(u > 0)
    def _():
        for c in o_store(u - 1):
            c.wait()
        for s in o_sends(u - 1):
            s.start()

    WB = 4 * BL
    lane_k = lax.broadcasted_iota(jnp.int32, (WB, LANES), 1)
    KR = wkT.shape[1]
    heads = pl.ds(pl.multiple_of(g * HG * LANES, LANES), HG * LANES)

    b0, b1 = tab[n, NB], tab[n, NB + 1]

    @pl.loop(0, NB // 4)
    def _(kc):
        blocks = jnp.concatenate([latbuf[tab[n, kc * 4 + j]] for j in range(SOURCES)], axis=0)
        lt = blocks[:, :KR]
        kr = jnp.where(lane_k < HALF, blocks[:, KR:].astype(F32), 0.0)
        krT = kr.T.astype(BF16)
        krO = jnp.concatenate([krT[HALF:], krT[:HALF]], axis=0)
        kt = lax.dot_general(wkT[heads, :], lt, (((1,), (1,)), ((), ())), preferred_element_type=F32).astype(BF16)
        V[kc] = jnp.dot(lt, wv[:, heads], preferred_element_type=F32).astype(BF16)
        for h in range(HG):
            k = kt[h * LANES:h * LANES + LANES]
            KT[kc, h, :LANES] = k if h % HALVES == 0 else jnp.concatenate([k[HALF:], k[:HALF]], axis=0)
            KT[kc, h, LANES:] = krT if h % HALVES == 0 else krO

    @pl.when(jnp.logical_and(g == 1, n + 1 < G))
    def _():
        for c in copies(n + 1):
            c.start()

    HR = HALVES * BL
    R = HALVES * HR
    WK = 4 * BL
    nS = NB // 4 - 1
    row = lax.broadcasted_iota(jnp.int32, (HR, WK), 0)
    col = lax.broadcasted_iota(jnp.int32, (HR, WK), 1)
    dF = jnp.where(row < BL, b0 * BL + row, (b1 - 1) * BL + row) - col
    dS = jnp.where(row < BL, (NB - 1 - b0) * BL + row, (NB - 2 - b1) * BL + row) - col
    rF, rS = slice(HR), slice(HR, R)
    extra = []
    for i in range(HALVES):
        at = [tab[n, NB + 2 + 4 * i + k] for k in range(SOURCES)]
        is_first = row[:BL, :LANES] * 0 + at[3] > 0
        extra.append((at[0], at[1], row[:BL] + at[2] - col[:BL], is_first, pl.ds(i * BL, BL), pl.ds((2 + i) * BL, BL)))

    def fold(t):
        w = t.shape[1] // HALVES
        t = jnp.maximum(t[:, :w], t[:, w:])
        return t if w == LANES else fold(t)

    def p1(c):
        for h in range(HG):
            q = Q[g * HG + h, 2:].reshape(HR, MXU) if c else Q[g * HG + h].reshape(R, MXU)
            s = jnp.dot(q, KT[c, h], preferred_element_type=F32) * scale2
            if c == 0:
                f = jnp.where(dF >= 0, s[:HR], NEG)
                sF[h] = f
                mx[h, rF] = fold(f)
                s = s[HR:]
            elif c == nS - 1:
                s = jnp.where(dS >= c * WK, s, NEG)
            sS[h, c] = s
            mx[h, rS] = jnp.maximum(mx[h, rS], fold(s)) if c else fold(s)

    def p1x():
        for h in range(HG):
            for i, (block, chunk, d, is_first, r_f, r_s) in enumerate(extra):
                s = jnp.dot(Q[g * HG + h, block], KT[chunk, h], preferred_element_type=F32) * scale2
                s = jnp.where(d >= 0, s, NEG)
                sX[h, i] = s
                m = fold(s)
                for r, t in ((r_f, jnp.where(is_first, m, NEG)), (r_s, jnp.where(is_first, NEG, m))):
                    t = jnp.maximum(mx[h, r], t)
                    mx[h, r] = jnp.broadcast_to(jnp.max(t, axis=1, keepdims=True), (BL, LANES))

    def weigh(load, chunk, h):
        es, ls = [], None
        for j in range(WK // LANES):
            e = jnp.exp2(load(slice(j * LANES, j * LANES + LANES)))
            ls = e if ls is None else ls + e
            es.append(e.astype(BF16))
        return ls, jnp.dot(jnp.concatenate(es, axis=1), V[chunk, :, h * LANES:h * LANES + LANES], preferred_element_type=F32)

    def p2(c):
        for h in range(HG):
            def load(js):
                t = sS[h, c, :, js] - mx[h, rS]
                return t if c else jnp.concatenate([sF[h, :, js] - mx[h, rF], t], axis=0)
            ls, pv = weigh(load, c, h)
            r = rS if c else slice(R)
            lsum[h, r] = lsum[h, r] + ls if c else ls
            acc[h, r] = acc[h, r] + pv if c else pv

    def p2x():
        for h in range(HG):
            for i, (_, chunk, _, is_first, r_f, r_s) in enumerate(extra):
                m = jnp.where(is_first, mx[h, r_f], mx[h, r_s])
                ls, pv = weigh(lambda js: sX[h, i, :, js] - m, chunk, h)
                for k, r in enumerate((r_f, r_s)):
                    pick = (lambda t: jnp.where(is_first, t, 0.0)) if k == 0 else (lambda t: jnp.where(is_first, 0.0, t))
                    l = lsum[h, r] + pick(ls)
                    total = acc[h, r] + pick(pv)
                    ob[i, k, :, h * LANES:h * LANES + LANES] = (total * (1.0 / jnp.sum(l, axis=1, keepdims=True))).astype(BF16)

    for c in range(nS):
        p1(c)
    p1x()

    @pl.when(u > 1)
    def _():
        for k, f in zip((1, 4), o_forwards(u - 2)):
            o_sends(u - 2)[k].wait_recv()
            f.start()

    for c in range(nS):
        p2(c)
    p2x()
    for c in o_store(u):
        c.start()

    @pl.when(u == U - 1)
    def _():
        for c in o_store(u):
            c.wait()

        def drain_forward(i, _):
            for f in o_forwards(i):
                f.wait()
            return 0

        @pl.loop(0, U - 1)
        def _(i):
            for k, s in enumerate(o_sends(i)):
                s.wait_send()
                if k in (0, 2, 3):
                    s.wait_recv()

        lax.fori_loop(0, U - 2, drain_forward, 0)
        for k in (1, 4):
            o_sends(U - 2)[k].wait_recv()
        for k, slot in enumerate((me.partner, me.left, me.right)):
            w_send(k, me.c).wait_send()
            w_send(k, slot).wait_recv()


def attention(mesh, tab, q_own, q_par, cs_own, cs_par, w_uk, w_uv, lat, wf, soft_scale):
    G, T = tab.shape[0], q_own.shape[1] * mesh.shape["cp"]
    BL = q_own.shape[1] // HALVES
    NB = T // BL
    KR, VD = w_uv.shape[0], w_uv.shape[1] // HALVES
    H = VD // LANES
    R = 4 * BL
    dims = (G, NB, BL, H // HALVES, float(soft_scale * LOG2E), mesh.shape["tp"], mesh.shape["cp"])
    blk = lambda a: pl.BlockSpec((1,) + a.shape[1:], lambda n, g, t: (n, 0, 0))
    hbm = pl.BlockSpec(memory_space=pltpu.HBM)
    dma = pltpu.SemaphoreType.DMA
    sds = jax.ShapeDtypeStruct
    ost = sds((G, 2, BL, VD), BF16)
    HG = H // HALVES
    stat = pltpu.VMEM((HG, R, LANES), F32)
    return pl.pallas_call(
        functools.partial(attn_kernel, dims),
        grid_spec=pltpu.PrefetchScalarGridSpec(
            num_scalar_prefetch=1, grid=(G, HALVES),
            in_specs=[blk(q_own), blk(q_par)] + [pl.BlockSpec((HALVES * BL, cs_own.shape[1]), lambda n, g, t: (n, 0))] * 2 + [hbm] * 4,
            out_specs=[hbm] * 4,
            scratch_shapes=[
                pltpu.VMEM((NB, BL, lat.shape[-1]), BF16), pltpu.VMEM((NB // 4, HG, MXU, R), BF16), pltpu.VMEM((NB // 4, R, VD // HALVES), BF16),
                pltpu.VMEM((H, 4, BL, MXU), BF16), pltpu.VMEM((HG, R // HALVES, R), F32),
                pltpu.VMEM((HG, NB // 4 - 1, R // HALVES, R), F32), pltpu.VMEM((HG, 2, BL, R), F32), stat, stat, stat, pltpu.VMEM((HALVES, HALVES, BL, VD // HALVES), BF16),
                pltpu.VMEM((KR, VD), BF16), pltpu.VMEM((VD, KR), BF16), pltpu.VMEM((KR, VD), BF16),
                dma((NB // HALVES,)), dma((HALVES,)), dma((HALVES,)), dma((HALVES * G, 7)), dma((HALVES * G, 7)), dma((3,)), dma((3,))],
        ),
        out_shape=[ost, ost, sds((4, 2, G, BL, VD), BF16), sds((mesh.shape["cp"],) + wf.shape, BF16)],
        compiler_params=pltpu.CompilerParams(collective_id=1, has_side_effects=True, vmem_limit_bytes=63 * MIB),
        cost_estimate=pl.CostEstimate(flops=G * H * T * R * 800, bytes_accessed=G * T * 640 * 2, transcendentals=0),
        name="attn",
    )(tab, q_own, q_par, cs_own, cs_par, w_uk, w_uv, lat, wf)


def proj_kernel(dims, pos, x, w_dq, w_dkv, w_uq, gq, gkv, fr, w_o,
                lat_all, latent, k_rope, q_own, q_par, wf, cs_own, cs_par, qn_o, qn_p,
                xbuf, wdq, wdkv, wuq, csb, pay, krb, kvb, qlat, qn, qst,
                xsem, wsem, dsem, csem, osem, wss, wrs, lss, lrs, qss, qrs, css, crs, lsem):
    n_tp, n_cp, n_t, half_cols, wc = dims
    me = Place(n_tp, n_cp)
    y, c, partner, right, left, far = me.y, me.c, me.partner, me.right, me.left, me.far

    rows = xbuf.shape[1]
    bl = pay.shape[3]
    kr_rank = gkv.shape[0]
    nj = WIDE
    last = n_t - 1
    every = HALVES * n_t

    def load_x(i):
        return pltpu.make_async_copy(x.at[pl.ds(pl.multiple_of(lax.rem(i, n_t) * rows, rows), rows), :], xbuf.at[lax.rem(i, HALVES)],
                                     xsem.at[lax.rem(i, HALVES)])

    kv_load = pltpu.make_async_copy(w_dkv, wdkv, wsem.at[0])
    kv_load.start()
    load_x(0).start()
    me.greet([(me.up, c), (me.dn, c), (me.dg, c), (y, partner), (y, right), (y, left)])
    half = lax.rem(y, HALVES)
    col_opp = pl.multiple_of((1 - half) * half_cols + c * wc, LANES)
    col_same = pl.multiple_of(half * half_cols + c * wc, LANES)
    w_sends = [me.copy(w_o.at[:, pl.ds(col, wc)], wf.at[k], wss.at[k], wrs.at[k], yy, c)
               for k, (col, yy) in enumerate(((col_opp, me.dn), (col_opp, me.up), (col_same, me.dg)))]
    for s in w_sends:
        s.start()

    def dq_load(j):
        cols = pl.ds(pl.multiple_of(j * nj, nj), nj)
        return pltpu.make_async_copy(w_dq.at[:, cols], wdq.at[:, cols], dsem.at[j])

    late = [pltpu.make_async_copy(w_uq.at[:, pl.ds(pl.multiple_of(me.core * wuq.shape[1], LANES), wuq.shape[1])], wuq, wsem.at[1])]

    def bid(n):
        return lax.div(pos[n, 0], bl)

    lane_b = lax.broadcasted_iota(jnp.int32, (bl, LANES), 1)
    row_b = lax.broadcasted_iota(jnp.int32, (bl, LANES), 0)
    sign = jnp.where(lax.rem(lane_b, HALF) < QUARTER, -1.0, 1.0)

    @pl.loop(0, every)
    def _(n):
        for k in range(HALVES):
            b = bid(n) if k == 0 else HALVES * n_cp - 1 - bid(n)
            ang = (b * bl + row_b).astype(F32) * fr[...]
            r = pl.ds(pl.multiple_of((HALVES * n + k) * bl, bl), bl)
            csb[r, :LANES] = jnp.cos(ang)
            csb[r, LANES:] = jnp.sin(ang) * sign

    cs_store = pltpu.make_async_copy(csb, cs_own, csem)
    cs_store.start()
    kv_load.wait()
    cs_store.wait()
    cs_send = me.copy(cs_own, cs_par, css, crs, y, partner)
    cs_send.start()

    lane = lax.broadcasted_iota(jnp.int32, (rows, LANES), 1)
    low32 = lax.rem(lane, HALF) < QUARTER
    upper = lax.broadcasted_iota(jnp.int32, (rows, LANES), 0) < rows // HALVES
    tile = lambda t: pl.ds(t * 2, HALVES)
    block = lambda t: pl.ds(pl.multiple_of(t * rows, rows), rows)

    def norm(t32, gain):
        return (t32 * lax.rsqrt(jnp.mean(t32 * t32, axis=-1, keepdims=True) + NORM_EPS) * gain).astype(BF16)

    def lat_copy(k, i, t, ref, yy, cc):
        return me.copy(ref, ref, lss.at[t, k], lrs.at[t, i], yy, cc)

    def own_store(t):
        return pltpu.make_async_copy(pay.at[lax.rem(t, HALVES)], lat_all.at[c, tile(t)], lsem.at[t])

    def out_stores(t):
        sl = lax.rem(t, HALVES)
        return [pltpu.make_async_copy(pay.at[sl, :, :, :, :kr_rank], latent.at[tile(t)], osem.at[0, sl]),
                pltpu.make_async_copy(krb.at[sl], k_rope.at[block(t)], osem.at[1, sl])]

    def send_own(t):
        own_store(t).wait()
        for k, cc in ((0, partner), (1, left), (2, right)):
            lat_copy(k, k, t, lat_all.at[c, tile(t)], y, cc).start()

    def settle_stores(t):
        for s in out_stores(t):
            s.wait()

    @pl.loop(0, n_t)
    def _(t):
        load_x(t).wait()

        pl.when(t == 0)(lambda: load_x(1).start())

        @pl.when(t == 1)
        def _():
            for j in range(wdq.shape[1] // nj):
                dq_load(j).start()
            for d in late:
                d.start()

        pl.when(t > 0)(lambda: send_own(t - 1))

        sl = lax.rem(t, HALVES)

        def kv_dot(wrows):
            d = lax.dot_general(xbuf[sl], wdkv[wrows, :], (((1,), (1,)), ((), ())), preferred_element_type=F32)
            return d.astype(BF16)

        @pl.loop(0, kr_rank // nj)
        def _(j):
            js = pl.ds(pl.multiple_of(j * nj, nj), nj)
            kvb[:, js] = kv_dot(js)

        u = kv_dot(pl.ds(kr_rank, wdkv.shape[0] - kr_rank)).astype(F32)
        pl.when(t + HALVES < n_t)(lambda: load_x(t + 2).start())
        lat = norm(kvb[...].astype(F32), gkv[...])
        u = jnp.concatenate([u, u], axis=1)
        w = jnp.where(low32, pltpu.roll(u, 96, 1), pltpu.roll(u, QUARTER, 1))
        rot = u * csb[block(t), :LANES] + w * csb[block(t), LANES:]
        pl.when(t >= HALVES)(lambda: settle_stores(t - 2))
        krb[sl] = rot[:, :HALF].astype(BF16)
        pay[sl, :, :, :, :kr_rank] = lat.reshape(HALVES, HALVES, bl, kr_rank)
        ids = jnp.where(upper, bid(HALVES * t), bid(HALVES * t + 1)).astype(F32)
        pay[sl, :, :, :, kr_rank:] = jnp.where(lane < HALF, rot, ids).astype(BF16).reshape(HALVES, HALVES, bl, LANES)
        for s in [own_store(t)] + out_stores(t):
            s.start()

    send_own(last)
    for d in late:
        d.wait()

    def stage1(t):
        rp, lp = lat_all.at[right, tile(t)], lat_all.at[left, tile(t)]
        lat_copy(3, 1, t, rp, y, partner).wait_recv()
        lat_copy(3, 2, t, lp, y, partner).wait_recv()
        for k, ref, cc in ((5, lat_all.at[left, tile(t), 0], right), (6, lat_all.at[right, tile(t), 1], left), (3, rp, partner), (4, lp, partner)):
            lat_copy(k, k, t, ref, y, cc).start()

    def stage2(t):
        for k in range(HALVES):
            ref = lat_all.at[far, tile(t), k]
            lat_copy(SPARE, 5 + k, t, ref, y, partner).wait_recv()
            lat_copy(7 + k, 7 + k, t, ref, y, partner).start()

    def project(src, wref, dst, width, before=None):
        @pl.loop(0, wref.shape[1] // width)
        def _(j):
            if before is not None:
                before(j)
            cols = pl.ds(pl.multiple_of(j * width, width), width)
            dst[:, cols] = jnp.dot(src[...], wref[:, cols], preferred_element_type=F32).astype(BF16)

    def q_store(u, dst, t):
        return pltpu.make_async_copy(qst.at[lax.rem(u, HALVES)], dst.at[block(t)], osem.at[3, lax.rem(u, HALVES)])

    def q_send(t):
        return me.copy(qn_o.at[block(t)], qn_p.at[block(t)], qss.at[t], qrs.at[t], y, partner)

    @pl.loop(0, n_t)
    def _(t):
        v = last - t
        pl.when(t >= HALVES)(lambda: load_x(v).wait())
        project(xbuf.at[lax.rem(v, HALVES)], wdq, qlat, nj, lambda j: pl.when(t == 0)(lambda: dq_load(j).wait()))
        pl.when(v >= HALVES)(lambda: load_x(v - 2).start())

        @pl.when(t == 0)
        def _():
            for k in (last - 1, last):
                settle_stores(k)

        stage1(t)
        sl = lax.rem(t, HALVES)
        qn[sl] = norm(qlat[...].astype(F32), gq[...])
        cp = pltpu.make_async_copy(qn.at[sl], qn_o.at[block(v)], osem.at[2, sl])
        cp.start()
        pl.when(t >= HALVES)(lambda: q_store(t, q_own, t - 2).wait())
        project(qn.at[sl], wuq, qst.at[sl], wuq.shape[1] // HALVES)
        cp.wait()
        q_send(v).start()
        q_store(t, q_own, v).start()

    def load_qp(t):
        return pltpu.make_async_copy(qn_p.at[block(last - t)], qn.at[lax.rem(t, HALVES)], osem.at[2, lax.rem(t, HALVES)])

    def take_qp(t):
        q_send(last - t).wait_recv()
        load_qp(t).start()

    take_qp(0)

    @pl.loop(0, n_t)
    def _(t):
        load_qp(t).wait()
        pl.when(t + 1 < n_t)(lambda: take_qp(t + 1))
        q_store(n_t + t, q_own, t).wait()
        project(qn.at[lax.rem(t, HALVES)], wuq, qst.at[lax.rem(n_t + t, HALVES)], wuq.shape[1] // HALVES)
        q_store(n_t + t, q_par, last - t).start()
        stage2(t)

    for k in range(HALVES):
        q_store(k, q_par, 0).wait()

    pr, pl_, pf = (lax.rem(partner + k, n_cp) for k in (HALVES, n_cp - 2, n_cp // HALVES))

    @pl.loop(0, n_t)
    def _(t):
        whole, part = lat_all.at[c, tile(t)], lat_all.at[c, tile(t), 0]
        for i, ref in ((0, lat_all.at[partner, tile(t)]), (3, lat_all.at[pr, tile(t)]), (4, lat_all.at[pl_, tile(t)]),
                       (7, lat_all.at[pf, tile(t), 0]), (8, lat_all.at[pf, tile(t), 1])):
            lat_copy(SPARE, i, t, ref, y, partner).wait_recv()
        for k in range(9):
            lat_copy(k, k, t, whole if k < 5 else part, y, partner).wait_send()
        q_send(t).wait_send()

    for s in w_sends + [cs_send]:
        s.wait()


def project_all(mesh, pos, x, w_dq, w_dkv, w_uq, g_q, g_kv, freq, w_o, bl):
    n_tp, n_cp = mesh.shape["tp"], mesh.shape["cp"]
    n_seq, seq, width = x.shape
    rows = HALVES * seq
    n_t = n_seq // HALVES
    rank, kvw = w_dq.shape[1], w_dkv.shape[1]
    kr = g_kv.shape[0]
    qw = w_uq.shape[1] // HALVES
    half_cols = width // HALVES
    wc = half_cols // n_cp
    total = n_seq * seq
    hbm = pl.BlockSpec(memory_space=pltpu.HBM)
    sds = jax.ShapeDtypeStruct
    dma = pltpu.SemaphoreType.DMA
    trig = sds((total, MXU), F32)
    return pl.pallas_call(
        functools.partial(proj_kernel, (n_tp, n_cp, n_t, half_cols, wc)),
        in_specs=[pl.BlockSpec(memory_space=pltpu.SMEM)] + [hbm] * 4 + [pl.BlockSpec(memory_space=pltpu.VMEM)] * 3 + [hbm],
        out_specs=[hbm] * 10,
        out_shape=[sds((n_cp, n_seq, 2, bl, kr + LANES), BF16), sds((n_seq, 2, bl, kr), BF16), sds((total, kvw - kr), BF16),
                   sds((total, qw), BF16), sds((total, qw), BF16), sds((3, w_o.shape[0], wc), BF16),
                   trig, trig, sds((total, rank), BF16), sds((total, rank), BF16)],
        scratch_shapes=[
            pltpu.VMEM((HALVES, rows, width), BF16), pltpu.VMEM((width, rank), BF16), pltpu.VMEM((kvw, width), BF16),
            pltpu.VMEM((rank, qw), BF16), pltpu.VMEM(trig.shape, F32), pltpu.VMEM((HALVES, HALVES, 2, bl, kr + LANES), BF16),
            pltpu.VMEM((HALVES, rows, kvw - kr), BF16), pltpu.VMEM((rows, kr), BF16), pltpu.VMEM((rows, rank), BF16),
            pltpu.VMEM((HALVES, rows, rank), BF16), pltpu.VMEM((HALVES, rows, qw), BF16),
            dma((HALVES,)), dma((HALVES,)), dma((rank // WIDE,)), dma, dma((4, HALVES)), dma((3,)), dma((3,)), dma((n_t, 9)), dma((n_t, 9)),
            dma((n_t,)), dma((n_t,)), dma, dma, dma((n_t,))],
        compiler_params=pltpu.CompilerParams(collective_id=0, has_side_effects=True, vmem_limit_bytes=63 * MIB),
        cost_estimate=pl.CostEstimate(flops=HALVES * total * (width * (rank + kvw) + HALVES * rank * qw), bytes_accessed=10**8,
                                      transcendentals=0),
        name="proj",
    )(pos, x.reshape(total, width), w_dq, w_dkv.T, w_uq, g_q, g_kv, freq, w_o)


def out_kernel(dims, x, w_o, wf, wx, ost_own, ost_par, obuf, out, wy, oy,
               wbuf, ov, xb, stage, wsem, osem, xsem, ssem, oss, ors, wss, wrs, ass, ars):
    n_tp, n_cp, n_seq, bl, half_cols = dims
    me = Place(n_tp, n_cp)
    cols, kb = xb.shape[-1], obuf.shape[-1]
    w, krows = cols // HALVES, w_o.shape[0]
    hk = krows // HALVES
    last = n_seq - 1
    half_of = lambda row: lax.rem(row, HALVES)
    tb = me.block(me.y, me.core)

    hb = kb // HALVES
    cut = [pl.ds(k * hb, hb) for k in range(HALVES)]
    to_last = lambda s, p: oy.at[s, p, 1]
    to_prev = lambda s, p: oy.at[s, p, 0]
    prev_fwd = me.o_forwards(lambda s, p: obuf.at[s, p, last, :, cut[0]], to_prev, oss.at[0], ors.at[0])
    last_sends = me.o_sends(ost_own.at[last, :, :, cut[1]], ost_par.at[last, :, :, cut[1]], to_last, oss.at[1], ors.at[1])
    last_fwd = me.o_forwards(to_last, to_last, oss.at[1], ors.at[1])
    def w_copy(k, src, dst, yy, cc):
        return me.copy(src, dst, wss.at[k], wrs.at[k], yy, cc)

    far_rows = [pl.ds(k * hk, hk) for k in range(HALVES)]
    (to_r, to_l), (rest_r, rest_l) = w_parts(krows)
    p_right, p_left, p_far = (lax.rem(me.partner + k, n_cp) for k in (HALVES, n_cp - 2, n_cp // HALVES))
    mine, side = (me.y, me.partner), ((me.y, me.right), (me.y, me.left))

    def w_move(k, buf, dev, part, to):
        return w_copy(k, buf.at[dev, :, part], wy.at[dev, :, part], *to)

    w_sends = [w_copy(0, wf.at[:, rest_r], wy.at[me.c, :, rest_r], *side[0]), w_copy(1, wf.at[:, rest_l], wy.at[me.c, :, rest_l], *side[1]),
               w_move(2, wx, me.left, to_r, mine), w_move(3, wx, me.right, to_l, mine),
               w_move(4, wx, me.left, far_rows[0], side[0]), w_move(5, wx, me.right, far_rows[1], side[1])]
    rest_fwd = [w_move(6, wy, me.left, rest_r, mine), w_move(7, wy, me.right, rest_l, mine)]
    far_fwd = [w_move(8 + k, wy, me.far, far_rows[k], mine) for k in range(HALVES)]

    def w_recv(k, dev, part):
        w_move(k, wy, dev, part, mine).wait_recv()

    n_m = n_seq // HALVES
    rows = HALVES * bl
    k_of = (None, me.flip, 1 - me.flip, HALVES)
    every = pl.ds(0, krows)
    own = ((wx, to_l), (wy, rest_l)), ((wx, to_r), (wy, rest_r))
    pieces = ((((wf, every),), ((wx.at[me.partner], every),)),) + tuple(
        (tuple((buf.at[dev], part) for buf, part in own[i]), ((wy.at[dev_p], every),))
        for i, (dev, dev_p) in enumerate(((me.right, p_right), (me.left, p_left)))) + ((((wy.at[me.far], every),), ((wy.at[p_far], every),)),)
    offs = [pl.multiple_of(v * w, LANES) for v in (me.core, 1 - me.core)]

    def col_of(j, row):
        dx = j + (j // HALVES) * (1 - HALVES * (j % HALVES))
        xq = lax.rem(lax.div(me.c, HALVES) + dx, n_cp // HALVES)
        return pl.multiple_of(half_of(row) * half_cols + xq * cols, LANES)

    def w_loads(j):
        b = j % HALVES
        out_ = [pltpu.make_async_copy(w_o.at[:, pl.ds(col_of(j, me.y), cols)], wbuf.at[b, 0], wsem.at[b, 0])]
        for r in range(1, 4):
            for part in range(HALVES):
                for i, (buf, part_rows) in enumerate(pieces[j][part]):
                    out_.append(pltpu.make_async_copy(buf.at[k_of[r], part_rows], wbuf.at[b, r, part_rows, pl.ds(offs[part], w)],
                                                      wsem.at[b, HALVES * r + part + 8 * i]))
        return out_

    def x_load(j):
        return pltpu.make_async_copy(x.at[:, pl.ds(pl.multiple_of(tb * bl, bl), bl), pl.ds(col_of(j, me.y), cols)], xb.at[j % HALVES], xsem.at[j % HALVES])

    o_offs = [pl.multiple_of(v * kb, LANES) for v in (me.core, 1 - me.core)]

    def o_place(i, r, part, half=None):
        off = r * krows + o_offs[part] + (0 if half is None else half * hb)
        return ov.at[i, :, pl.ds(pl.multiple_of(off, LANES), kb if half is None else hb)]

    def o_load(i, r, part):
        src = ost_own.at[i, tb] if (r, part) == (0, 0) else obuf.at[r, part, i]
        return pltpu.make_async_copy(src, o_place(i, r, part), osem.at[i, HALVES * r + part])

    pairs = [(r, part) for r in range(SOURCES) for part in range(HALVES)]
    early = [o_load(i, r, part) for i in range(last - 1) for r, part in pairs]
    late = [o_load(last - 1, r, part) for r, part in pairs]
    for r, part in pairs:
        for half in range(HALVES):
            if (r, part) == (0, 0):
                src = ost_own.at[last, tb, :, cut[half]]
            else:
                src = oy.at[r, part, half] if half == 1 or r == 3 else obuf.at[r, part, last, :, cut[0]]
            late.append(pltpu.make_async_copy(src, o_place(last, r, part, half), osem.at[last, HALVES * r + part + 8 * half]))
    for d in w_loads(0) + early + [x_load(0)]:
        d.start()
    me.greet(((me.up, me.c), (me.dn, me.c), (me.up, me.partner), (me.dn, me.partner),
              (me.y, me.partner), (me.y, me.right), (me.y, me.left)))
    for s in last_sends + prev_fwd + w_sends:
        s.start()

    def region(row, j, m, n0=0, cnt=2):
        return out.at[pl.ds(HALVES * m + n0, cnt), pl.ds(pl.multiple_of(me.block(row, me.core) * bl, bl), bl), pl.ds(col_of(j, row), cols)]

    def ring(k, ref, j, m, yy):
        i = j * n_m + m
        return me.copy(ref, ref, ass.at[i, k], ars.at[i, k], yy, me.c)

    def tile_sends(j, m):
        ref = region(me.y, j, m)
        return ring(0, ref, j, m, me.up), ring(1, ref, j, m, me.dn)

    def forward(j, m):
        ring(0, region(me.dn, j, m), j, m, me.up).wait_recv()
        ring(2, region(me.dn, j, m, 0, 1), j, m, me.up).start()
        ring(1, region(me.up, j, m), j, m, me.up).wait_recv()
        ring(3, region(me.up, j, m, 1, 1), j, m, me.dn).start()

    nt = MXU

    def tile(j, m):
        b = j % HALVES

        @pl.loop(0, cols // nt)
        def _(t):
            cs_ = pl.ds(pl.multiple_of(t * nt, nt), nt)
            a = ov[pl.ds(HALVES * m, HALVES)].reshape(rows, 4 * krows)
            s = None
            for r in range(SOURCES):
                d = jnp.dot(a[:, r * krows:(r + 1) * krows], wbuf[b, r, :, cs_], preferred_element_type=F32)
                s = d if s is None else s + d
            xr = xb[b, pl.ds(HALVES * m, HALVES), :, cs_].reshape(rows, nt).astype(F32)
            stage[:, :, cs_] = (xr + s).astype(BF16).reshape(2, bl, nt)

        c = pltpu.make_async_copy(stage, region(me.y, j, m), ssem)
        c.start()
        c.wait()
        for s in tile_sends(j, m):
            s.start()

    def need(j):
        if j == 0:
            w_recv(1, me.right, rest_l)
            rest_fwd[1].start()
            w_recv(3, p_right, to_l)
            w_recv(7, p_right, rest_l)
        elif j == 1:
            w_recv(0, me.left, rest_r)
            rest_fwd[0].start()
            w_recv(2, p_left, to_r)
            w_recv(6, p_left, rest_r)
        else:
            for k in range(HALVES):
                w_recv(4 + k, me.far, far_rows[k])
                far_fwd[k].start()
            for k in range(HALVES):
                w_recv(8 + k, p_far, far_rows[k])
        for d in w_loads(j + 1) + [x_load(j + 1)]:
            d.start()

    def late_o():
        for k in (0, 2, 3):
            last_sends[k].wait_recv()
        for f in prev_fwd + last_fwd:
            f.wait_recv()
        for d in late:
            d.start()
        for d in late:
            d.wait()

    for k, f in zip((1, 4), last_fwd):
        last_sends[k].wait_recv()
        f.start()
    for d in early:
        d.wait()

    @pl.loop(0, 4 * n_m)
    def _(i):
        j, m = lax.div(i, n_m), lax.rem(i, n_m)
        for jj in range(SOURCES):
            @pl.when(i == jj * n_m)
            def _(jj=jj):
                for d in w_loads(jj) + [x_load(jj)]:
                    d.wait()
                if jj == 1:
                    need(jj)
        pl.when(i == n_m - 1)(late_o)
        tile(j, m)
        pl.when(i == 0)(lambda: need(0))

        @pl.when(j > 0)
        def _():
            forward(j - 1, m)

        pl.when(i == 3 * n_m - 1)(lambda: need(2))

    @pl.loop(0, n_m)
    def _(m):
        forward(3, m)

    @pl.loop(0, 4 * n_m)
    def _(i):
        j, m = lax.div(i, n_m), lax.rem(i, n_m)
        for k, row, n0, cnt in ((0, me.y, 0, HALVES), (1, me.y, 0, HALVES), (2, me.dn, 0, 1), (3, me.up, 1, 1)):
            r = region(row, j, m, n0, cnt)
            me.copy(r, r, ass.at[i, k], ars.at[i, k], me.up, me.c).wait_send()
        for k, n0 in ((HALVES, 0), (3, 1)):
            r = region(me.dg, j, m, n0, 1)
            me.copy(r, r, ass.at[i, k], ars.at[i, k], me.up, me.c).wait_recv()

    for s in last_sends + prev_fwd + last_fwd + w_sends + rest_fwd + far_fwd:
        s.wait_send()


def out_product(mesh, x, w_o, wf, wx, ost_own, ost_par, obuf):
    n_tp, n_cp = mesh.shape["tp"], mesh.shape["cp"]
    n_seq, seq, width = x.shape
    bl = seq // HALVES
    cols = HALVES * wf.shape[-1]
    krows = w_o.shape[0]
    hbm = pl.BlockSpec(memory_space=pltpu.HBM)
    dma = pltpu.SemaphoreType.DMA
    sds = jax.ShapeDtypeStruct
    tiles = HALVES * n_seq
    return pl.pallas_call(
        functools.partial(out_kernel, (n_tp, n_cp, n_seq, bl, width // HALVES)),
        in_specs=[hbm] * 7, out_specs=[hbm] * 3,
        out_shape=[sds(x.shape, BF16), sds(wx.shape, BF16), sds((4, 2, 2, bl, obuf.shape[-1] // HALVES), BF16)],
        scratch_shapes=[
            pltpu.VMEM((HALVES, 4, krows, cols), BF16), pltpu.VMEM((n_seq, bl, 4 * krows), BF16), pltpu.VMEM((HALVES, n_seq, bl, cols), BF16),
            pltpu.VMEM((HALVES, bl, cols), BF16), dma((HALVES, 16)), dma((n_seq, 16)), dma((HALVES,)), dma, dma((HALVES, 7)), dma((HALVES, 7)),
            dma((10,)), dma((10,)), dma((tiles, 4)), dma((tiles, 4))],
        compiler_params=pltpu.CompilerParams(collective_id=2, has_side_effects=True, vmem_limit_bytes=63 * MIB),
        cost_estimate=pl.CostEstimate(flops=n_seq * seq * cols * 16 * krows, bytes_accessed=10**8, transcendentals=0),
        name="outp",
    )(x, w_o, wf, wx, ost_own, ost_par, obuf)[0]


def settle_kernel(src, lat, kr, dst, lat_out, kr_out, buf, lbuf, kbuf, tbuf, rsem, wsem, lsem, ksem):
    n = buf.shape[0]
    reads = [pltpu.make_async_copy(src.at[i], buf.at[i], rsem.at[i]) for i in range(n)]
    writes = [pltpu.make_async_copy(buf.at[i], dst.at[i], wsem.at[i]) for i in range(n)]
    small = [pltpu.make_async_copy(*p) for p in ((kr, kbuf, ksem.at[0]), (lat, lbuf, lsem.at[0]))]
    small_out = [pltpu.make_async_copy(*p) for p in ((tbuf, kr_out, ksem.at[1]), (lbuf, lat_out, lsem.at[1]))]
    for d in small + reads:
        d.start()
    for d in small:
        d.wait()
    for i in range(tbuf.shape[0]):
        tbuf[i] = kbuf[i].astype(F32).T.astype(BF16)
    for d in small_out:
        d.start()
    for a, b in zip(reads, writes):
        a.wait()
        b.start()
    for d in writes + small_out:
        d.wait()


def settle(out, lat, kr):
    n_seq, seq, width = out.shape
    parts = 4 * n_seq
    shape = (parts, n_seq * seq // parts, width)
    lat_shape, kr_shape = (n_seq, seq, lat.shape[-1]), (n_seq, seq, kr.shape[-1])
    turned = (n_seq, kr.shape[-1], seq)
    hbm = pl.BlockSpec(memory_space=pltpu.HBM)
    sds = jax.ShapeDtypeStruct
    dma = pltpu.SemaphoreType.DMA
    a, b, c = pl.pallas_call(
        settle_kernel, in_specs=[hbm] * 3, out_specs=[hbm] * 3,
        out_shape=[sds(shape, BF16), sds(lat_shape, BF16), sds(turned, BF16)],
        scratch_shapes=[pltpu.VMEM(shape, BF16), pltpu.VMEM(lat_shape, BF16), pltpu.VMEM(kr_shape, BF16), pltpu.VMEM(turned, BF16),
                        dma((parts,)), dma((parts,)), dma((HALVES,)), dma((HALVES,))],
        compiler_params=pltpu.CompilerParams(vmem_limit_bytes=63 * MIB), name="settle",
    )(out.reshape(shape), lat.reshape(lat_shape), kr.reshape(kr_shape))
    return a.reshape(out.shape), b, jnp.swapaxes(c, 1, HALVES)


ROPE_BASE = 10000.0


def solution(mesh):
    def local_step(x, pos, w_dq, g_q, w_uq, w_dkv, g_kv, w_uk, w_uv, w_o):
        n_seq, seq, _ = x.shape
        n_cp = mesh.shape["cp"]
        bl = seq // HALVES
        nb = HALVES * n_cp
        kv_rank = g_kv.shape[0]
        rope = w_dkv.shape[1] - kv_rank
        heads = (w_uq.shape[1] - w_uk.shape[1]) // rope
        nope = w_uk.shape[1] // heads
        c = lax.axis_index("cp")
        core = c % HALVES

        freq = np.tile(ROPE_BASE ** (-2.0 * np.arange(rope // HALVES) / rope), LANES // (rope // HALVES))[None].astype(np.float32)
        lat_all, latent, k_rope, q_own, q_par, wf, cs_own, cs_par, _, _ = project_all(
            mesh, pos, x, w_dq, w_dkv, w_uq, g_q, g_kv, freq, w_o, bl)
        q_own, q_par = (a.reshape(n_seq, seq, -1) for a in (q_own, q_par))
        ids = lat_all[:, :, 0, 0, kv_rank + rope].astype(jnp.int32)
        blocks = jnp.arange(nb)
        first = ids[:, :, None] == blocks
        second = nb - 1 - ids[:, :, None] == blocks
        dev = jnp.arange(n_cp)[:, None, None]
        slots = jnp.sum(jnp.where(first, HALVES * dev, 0) + jnp.where(second, HALVES * dev + 1, 0), axis=0)
        mine = [jnp.sum(jnp.where(jnp.arange(n_cp)[:, None] == k, ids, 0), axis=0) for k in (c, c ^ 1)]
        last = nb // 4 - 1
        extra = []
        for i, b in enumerate(mine):
            is_first = b > last
            chunk = jnp.where(is_first, 1, last)
            extra += [jnp.where(is_first, i, 2 + i), chunk, jnp.where(is_first, b, nb - 1 - b) * bl - chunk * 4 * bl, is_first]
        tab = jnp.concatenate([slots, jnp.stack(mine + extra, axis=1).astype(jnp.int32)], axis=1).astype(jnp.int32)

        ost_own, ost_par, obuf, wx = attention(mesh, tab, q_own, q_par, cs_own, cs_par, w_uk, w_uv, lat_all, wf, (nope + rope) ** -0.5)
        return settle(out_product(mesh, x, w_o, wf, wx, ost_own, ost_par, obuf), latent, k_rope)

    seq_spec = P("dp", "cp", None)
    whole = P(None, None)
    in_specs = (seq_spec, P("dp", "cp"), whole, P(None), P(None, "tp"), whole, P(None), P(None, "tp"), P(None, "tp"), P("tp", None))
    return jax.shard_map(local_step, mesh=mesh, in_specs=in_specs, out_specs=(seq_spec,) * 3, check_vma=False)
```

```python
import functools
import numpy as np
import jax, jax.numpy as jnp
from jax import lax
from jax.experimental import pallas as pl
from jax.experimental.pallas import tpu as pltpu
from jax.sharding import PartitionSpec as P

F32, BF16 = jnp.float32, jnp.bfloat16
NEG = float("-inf")
LOG2E = 1.4426950408889634
LANES, HALF, QUARTER, MXU, WIDE, PAIR = 128, 64, 32, 256, 512, 384
HALVES = 2
SOURCES = 4
MIB = 2**20
FORWARDED, DIRECT = (1, 4), (0, 2, 3)
SPARE = 7


MESH = pl.DeviceIdType.MESH
NORM_EPS = 1e-6


class Place:
    def __init__(self, n_tp, n_cp):
        self.dp, self.y, self.c = (lax.axis_index(a) for a in ("dp", "tp", "cp"))
        y, c = self.y, self.c
        self.n_tp = n_tp
        self.core = lax.rem(c, HALVES)
        self.partner = c + 1 - HALVES * self.core
        self.right, self.left, self.far = (lax.rem(c + k, n_cp) for k in (HALVES, n_cp - HALVES, n_cp // HALVES))
        self.up, self.dn, self.dg = (lax.rem(y + k, n_tp) for k in (1, n_tp - 1, n_tp // HALVES))
        self.flip = lax.rem(y + self.core, HALVES)
        self.mate = lax.rem(y + 1 + HALVES * self.flip, n_tp)
        self.other = lax.rem(y + 3 - HALVES * self.flip, n_tp)

    def block(self, row, core):
        return lax.div(lax.rem(row + (self.n_tp - 1) * core, self.n_tp), HALVES)

    def greet(self, peers):
        barrier = pltpu.get_barrier_semaphore()
        for yy, cc in peers:
            pl.semaphore_signal(barrier, inc=1, device_id=(self.dp, yy, cc), device_id_type=MESH)
        pl.semaphore_wait(barrier, len(peers))

    def copy(self, src, dst, ss, rs, yy, cc):
        return pltpu.make_async_remote_copy(src_ref=src, dst_ref=dst, send_sem=ss, recv_sem=rs,
                                            device_id=(self.dp, yy, cc), device_id_type=MESH)

    def o_sends(self, own, par, dst, ss, rs):
        tb, tp = self.block(self.y, self.core), self.block(self.y, 1 - self.core)
        ways = [(own, tb, 1, 0, self.mate, self.c), (own, 1 - tb, 2, 0, self.other, self.c), (par, tp, 0, 1, self.y, self.partner),
                (par, tp, 1, 1, self.other, self.partner), (par, 1 - tp, 2, 1, self.mate, self.partner)]
        return [self.copy(a.at[blk], dst(src, part), ss.at[k], rs.at[k], yy, cc)
                for k, (a, blk, src, part, yy, cc) in enumerate(ways)]

    def o_forwards(self, src, dst, ss, rs):
        return [self.copy(src(2, part), dst(3, part), ss.at[5 + part], rs.at[5 + part], self.mate, self.c) for part in range(HALVES)]


def w_parts(rows):
    cut = rows // 8
    return (pl.ds(0, rows - cut), pl.ds(cut, rows - cut)), (pl.ds(rows - cut, cut), pl.ds(0, cut))


def attn_kernel(dims, tab, *refs):
    G, NB, BL, HP, scale2, n_tp, n_cp = dims
    CK = HALVES * BL
    H, HG = HALVES * HP, HP
    q_own, q_par, cs_own, cs_par, w_uk, w_uv, lat, wf = refs[:8]
    ost_own, ost_par, obuf, wx, lf = refs[8:13]
    latbuf, KT, V, Q, sF, sS, sX, mx, lsum, acc, ob, wk, wkT, wv, sem, ksem, osem, oss, ors, wss, wrs, fss, frs = refs[13:]
    n, g = pl.program_id(0), pl.program_id(1)
    u, U = HALVES * n + g, HALVES * G
    me = Place(n_tp, n_cp)
    rows_ = ((me.up, me.c), (me.dn, me.c), (me.up, me.partner), (me.dn, me.partner))
    w_to = ((me.y, me.partner), (me.y, me.right), (me.y, me.left))

    krows = wf.shape[1]
    w_rows = (pl.ds(0, krows),) + w_parts(krows)[0]

    def w_send(k, slot):
        return me.copy(wf.at[:, w_rows[k]], wx.at[slot, :, w_rows[k]], wss.at[k], wrs.at[k], *w_to[k])

    tail = G - 2
    p_far = lax.rem(me.partner + n_cp // HALVES, n_cp)
    far_from = [lat.at[me.left, pl.ds(tail, HALVES), 0], lat.at[me.right, pl.ds(tail, HALVES), 1]] + [lf.at[0, :, k] for k in range(HALVES)]
    far_to = [lf.at[0, :, k] for k in range(HALVES)] + [lf.at[1, :, k] for k in range(HALVES)]
    far = [me.copy(a, b, fss.at[k], frs.at[k], *(w_to[1:] + w_to[:1] * HALVES)[k]) for k, (a, b) in enumerate(zip(far_from, far_to))]

    def copy_in(src, dev):
        return pltpu.make_async_copy(src, latbuf.at[pl.ds(HALVES * dev, HALVES)], sem.at[dev])

    def start_lat(i):
        for k in range(n_cp):
            dev = lax.rem(me.c + k, n_cp)
            away = jnp.logical_and(i >= tail, jnp.logical_or(dev == me.far, dev == p_far))
            which = jnp.where(dev == me.far, 0, 1)
            pl.when(jnp.logical_not(away))(lambda: copy_in(lat.at[dev, i], dev).start())
            pl.when(away)(lambda: copy_in(lf.at[which, lax.rem(i, HALVES)], dev).start())

    def copies(i):
        return [copy_in(lat.at[p, i], p) for p in range(n_cp)]

    def unit(ref, i):
        w = ob.shape[-1]
        return ref.at[lax.div(i, HALVES), :, :, pl.ds(pl.multiple_of(lax.rem(i, HALVES) * w, LANES), w)]

    def landing(i):
        w = ob.shape[-1]
        return lambda s, p: obuf.at[s, p, lax.div(i, HALVES), :, pl.ds(pl.multiple_of(lax.rem(i, HALVES) * w, LANES), w)]

    def o_store(i):
        return [pltpu.make_async_copy(ob.at[k], unit(dst, i), osem.at[k]) for k, dst in enumerate((ost_own, ost_par))]

    def o_sends(i):
        return me.o_sends(unit(ost_own, i), unit(ost_par, i), landing(i), oss.at[i], ors.at[i])

    def o_forwards(i):
        return me.o_forwards(landing(i), landing(i), oss.at[i], ors.at[i])

    hw = wv.shape[1]
    kv_loads = [pltpu.make_async_copy(a.at[:, pl.ds(pl.multiple_of(me.core * hw, LANES), hw)], b, ksem.at[k])
                for k, (a, b) in enumerate(((w_uk, wk), (w_uv, wv)))]

    @pl.when(u == 0)
    def _():
        for c in kv_loads:
            c.start()
        start_lat(n)
        me.greet(rows_ + w_to)
        for s in far[:2] + [w_send(k, me.c) for k in range(3)]:
            s.start()
        for c in kv_loads:
            c.wait()
        wkT[...] = wk[...].T

    @pl.when(g == 0)
    def _():
        lane = lax.broadcasted_iota(jnp.int32, (BL, LANES), 1)
        low64 = lane < HALF
        low32 = lax.rem(lane, HALF) < QUARTER
        for src_i, (q, cs) in enumerate(((q_own, cs_own), (q_par, cs_par))):
            @pl.loop(0, HALVES)
            def _(half, src_i=src_i, q=q, cs=cs):
                r0 = half * 2 + src_i
                rows = pl.ds(pl.multiple_of(half * BL, BL), BL)
                ct = cs[rows, :LANES]
                st = cs[rows, LANES:]
                for p in range(HP):
                    a = q[0, rows, p * PAIR:p * PAIR + LANES]
                    b = q[0, rows, p * PAIR + LANES:p * PAIR + MXU].astype(F32)
                    c = q[0, rows, p * PAIR + MXU:p * PAIR + PAIR].astype(F32)
                    u = jnp.where(low64, b, c)
                    no = jnp.where(low64, c, b).astype(BF16)
                    w = jnp.where(low32, pltpu.roll(u, 96, 1), pltpu.roll(u, QUARTER, 1))
                    rot = (u * ct + w * st).astype(BF16)
                    Q[HALVES * p, r0, :, :LANES] = a
                    Q[HALVES * p, r0, :, LANES:MXU] = rot
                    Q[HALVES * p + 1, r0, :, :LANES] = no
                    Q[HALVES * p + 1, r0, :, LANES:MXU] = rot

        for c in copies(n):
            c.wait()

    @pl.when(u > 0)
    def _():
        for c in o_store(u - 1):
            c.wait()
        for s in o_sends(u - 1):
            s.start()

    WB = 4 * BL
    lane_k = lax.broadcasted_iota(jnp.int32, (WB, LANES), 1)
    KR = wkT.shape[1]
    heads = pl.ds(pl.multiple_of(g * HG * LANES, LANES), HG * LANES)

    b0, b1 = tab[n, NB], tab[n, NB + 1]

    @pl.loop(0, NB // 4)
    def _(kc):
        blocks = jnp.concatenate([latbuf[tab[n, kc * 4 + j]] for j in range(SOURCES)], axis=0)
        lt = blocks[:, :KR]
        kr = jnp.where(lane_k < HALF, blocks[:, KR:].astype(F32), 0.0)
        krT = kr.T.astype(BF16)
        krO = jnp.concatenate([krT[HALF:], krT[:HALF]], axis=0)
        kt = lax.dot_general(wkT[heads, :], lt, (((1,), (1,)), ((), ())), preferred_element_type=F32).astype(BF16)
        V[kc] = jnp.dot(lt, wv[:, heads], preferred_element_type=F32).astype(BF16)
        for h in range(HG):
            k = kt[h * LANES:h * LANES + LANES]
            KT[kc, h, :LANES] = k if h % HALVES == 0 else jnp.concatenate([k[HALF:], k[:HALF]], axis=0)
            KT[kc, h, LANES:] = krT if h % HALVES == 0 else krO

    @pl.when(u == G - 2)
    def _():
        for k in range(HALVES):
            far[k].wait_recv()
            far[2 + k].start()

    @pl.when(u == HALVES * tail - 1)
    def _():
        for f in far[2:]:
            f.wait_recv()

    pl.when(jnp.logical_and(g == 1, n + 1 < G))(lambda: start_lat(n + 1))

    HR = HALVES * BL
    R = HALVES * HR
    WK = 4 * BL
    nS = NB // 4 - 1
    row = lax.broadcasted_iota(jnp.int32, (HR, WK), 0)
    col = lax.broadcasted_iota(jnp.int32, (HR, WK), 1)
    dF = jnp.where(row < BL, b0 * BL + row, (b1 - 1) * BL + row) - col
    dS = jnp.where(row < BL, (NB - 1 - b0) * BL + row, (NB - 2 - b1) * BL + row) - col
    rF, rS = slice(HR), slice(HR, R)
    extra = []
    for i in range(HALVES):
        at = [tab[n, NB + 2 + 4 * i + k] for k in range(SOURCES)]
        is_first = row[:BL, :LANES] * 0 + at[3] > 0
        extra.append((at[0], at[1], row[:BL] + at[2] - col[:BL], is_first, pl.ds(i * BL, BL), pl.ds((2 + i) * BL, BL)))

    def fold(t):
        w = t.shape[1] // HALVES
        t = jnp.maximum(t[:, :w], t[:, w:])
        return t if w == LANES else fold(t)

    def p1(c):
        for h in range(HG):
            q = Q[g * HG + h, 2:].reshape(HR, MXU) if c else Q[g * HG + h].reshape(R, MXU)
            s = jnp.dot(q, KT[c, h], preferred_element_type=F32) * scale2
            if c == 0:
                f = jnp.where(dF >= 0, s[:HR], NEG)
                sF[h] = f
                mx[h, rF] = fold(f)
                s = s[HR:]
            elif c == nS - 1:
                s = jnp.where(dS >= c * WK, s, NEG)
            sS[h, c] = s
            mx[h, rS] = jnp.maximum(mx[h, rS], fold(s)) if c else fold(s)

    def p1x():
        for h in range(HG):
            for i, (block, chunk, d, is_first, r_f, r_s) in enumerate(extra):
                s = jnp.dot(Q[g * HG + h, block], KT[chunk, h], preferred_element_type=F32) * scale2
                s = jnp.where(d >= 0, s, NEG)
                sX[h, i] = s
                m = fold(s)
                for r, t in ((r_f, jnp.where(is_first, m, NEG)), (r_s, jnp.where(is_first, NEG, m))):
                    t = jnp.maximum(mx[h, r], t)
                    mx[h, r] = jnp.broadcast_to(jnp.max(t, axis=1, keepdims=True), (BL, LANES))

    def weigh(load, chunk, h):
        es, ls = [], None
        for j in range(WK // LANES):
            e = jnp.exp2(load(slice(j * LANES, j * LANES + LANES)))
            ls = e if ls is None else ls + e
            es.append(e.astype(BF16))
        return ls, jnp.dot(jnp.concatenate(es, axis=1), V[chunk, :, h * LANES:h * LANES + LANES], preferred_element_type=F32)

    def p2(c):
        for h in range(HG):
            def load(js):
                t = sS[h, c, :, js] - mx[h, rS]
                return t if c else jnp.concatenate([sF[h, :, js] - mx[h, rF], t], axis=0)
            ls, pv = weigh(load, c, h)
            r = rS if c else slice(R)
            lsum[h, r] = lsum[h, r] + ls if c else ls
            acc[h, r] = acc[h, r] + pv if c else pv

    def p2x():
        for h in range(HG):
            for i, (_, chunk, _, is_first, r_f, r_s) in enumerate(extra):
                m = jnp.where(is_first, mx[h, r_f], mx[h, r_s])
                ls, pv = weigh(lambda js: sX[h, i, :, js] - m, chunk, h)
                for k, r in enumerate((r_f, r_s)):
                    pick = (lambda t: jnp.where(is_first, t, 0.0)) if k == 0 else (lambda t: jnp.where(is_first, 0.0, t))
                    l = lsum[h, r] + pick(ls)
                    total = acc[h, r] + pick(pv)
                    ob[i, k, :, h * LANES:h * LANES + LANES] = (total * (1.0 / jnp.sum(l, axis=1, keepdims=True))).astype(BF16)

    for c in range(nS):
        p1(c)
    p1x()

    @pl.when(u > 1)
    def _():
        for k, f in zip(FORWARDED, o_forwards(u - 2)):
            o_sends(u - 2)[k].wait_recv()
            f.start()

    for c in range(nS):
        p2(c)
    p2x()
    for c in o_store(u):
        c.start()

    @pl.when(u == U - 1)
    def _():
        for c in o_store(u):
            c.wait()

        def drain_forward(i, _):
            for f in o_forwards(i):
                f.wait()
            return 0

        @pl.loop(0, U - 1)
        def _(i):
            for k, s in enumerate(o_sends(i)):
                s.wait_send()
                if k in DIRECT:
                    s.wait_recv()

        lax.fori_loop(0, U - 2, drain_forward, 0)
        for k in FORWARDED:
            o_sends(U - 2)[k].wait_recv()
        for f in far:
            f.wait_send()
        for k, slot in enumerate((me.partner, me.left, me.right)):
            w_send(k, me.c).wait_send()
            w_send(k, slot).wait_recv()


def attention(mesh, tab, q_own, q_par, cs_own, cs_par, w_uk, w_uv, lat, wf, soft_scale):
    G, T = tab.shape[0], q_own.shape[1] * mesh.shape["cp"]
    BL = q_own.shape[1] // HALVES
    NB = T // BL
    KR, VD = w_uv.shape[0], w_uv.shape[1] // HALVES
    H = VD // LANES
    R = 4 * BL
    dims = (G, NB, BL, H // HALVES, float(soft_scale * LOG2E), mesh.shape["tp"], mesh.shape["cp"])
    blk = lambda a: pl.BlockSpec((1,) + a.shape[1:], lambda n, g, t: (n, 0, 0))
    hbm = pl.BlockSpec(memory_space=pltpu.HBM)
    dma = pltpu.SemaphoreType.DMA
    sds = jax.ShapeDtypeStruct
    ost = sds((G, 2, BL, VD), BF16)
    HG = H // HALVES
    stat = pltpu.VMEM((HG, R, LANES), F32)
    return pl.pallas_call(
        functools.partial(attn_kernel, dims),
        grid_spec=pltpu.PrefetchScalarGridSpec(
            num_scalar_prefetch=1, grid=(G, HALVES),
            in_specs=[blk(q_own), blk(q_par)] + [pl.BlockSpec((HALVES * BL, cs_own.shape[1]), lambda n, g, t: (n, 0))] * 2 + [hbm] * 4,
            out_specs=[hbm] * 5,
            scratch_shapes=[
                pltpu.VMEM((NB, BL, lat.shape[-1]), BF16), pltpu.VMEM((NB // 4, HG, MXU, R), BF16), pltpu.VMEM((NB // 4, R, VD // HALVES), BF16),
                pltpu.VMEM((H, 4, BL, MXU), BF16), pltpu.VMEM((HG, R // HALVES, R), F32),
                pltpu.VMEM((HG, NB // 4 - 1, R // HALVES, R), F32), pltpu.VMEM((HG, 2, BL, R), F32), stat, stat, stat, pltpu.VMEM((HALVES, HALVES, BL, VD // HALVES), BF16),
                pltpu.VMEM((KR, VD), BF16), pltpu.VMEM((VD, KR), BF16), pltpu.VMEM((KR, VD), BF16),
                dma((NB // HALVES,)), dma((HALVES,)), dma((HALVES,)), dma((HALVES * G, 7)), dma((HALVES * G, 7)), dma((3,)), dma((3,)), dma((SOURCES,)), dma((SOURCES,))],
        ),
        out_shape=[ost, ost, sds((SOURCES, HALVES, G, BL, VD), BF16), sds((mesh.shape["cp"],) + wf.shape, BF16),
                   sds((HALVES, HALVES) + lat.shape[2:], BF16)],
        compiler_params=pltpu.CompilerParams(collective_id=1, has_side_effects=True, vmem_limit_bytes=63 * MIB),
        cost_estimate=pl.CostEstimate(flops=G * H * T * R * 800, bytes_accessed=G * T * 640 * 2, transcendentals=0),
        name="attn",
    )(tab, q_own, q_par, cs_own, cs_par, w_uk, w_uv, lat, wf)


def proj_kernel(dims, pos, x, w_dq, w_dkv, w_uq, gq, gkv, fr, w_o,
                lat_all, latent, k_rope, q_own, q_par, wf, cs_own, cs_par, qn_o, qn_p,
                xbuf, wdq, wdkv, wuq, csb, pay, krb, kvb, qlat, qn, qst,
                xsem, wsem, dsem, csem, osem, wss, wrs, lss, lrs, qss, qrs, css, crs, lsem):
    n_tp, n_cp, n_t, half_cols, wc = dims
    me = Place(n_tp, n_cp)
    y, c, partner, right, left, far = me.y, me.c, me.partner, me.right, me.left, me.far

    rows = xbuf.shape[1]
    bl = pay.shape[3]
    kr_rank = gkv.shape[0]
    nj = WIDE
    last = n_t - 1
    every = HALVES * n_t

    def load_x(i):
        return pltpu.make_async_copy(x.at[pl.ds(pl.multiple_of(lax.rem(i, n_t) * rows, rows), rows), :], xbuf.at[lax.rem(i, HALVES)],
                                     xsem.at[lax.rem(i, HALVES)])

    kv_load = pltpu.make_async_copy(w_dkv, wdkv, wsem.at[0])
    kv_load.start()
    load_x(0).start()
    me.greet([(me.up, c), (me.dn, c), (me.dg, c), (y, partner), (y, right), (y, left)])
    half = lax.rem(y, HALVES)
    col_opp = pl.multiple_of((1 - half) * half_cols + c * wc, LANES)
    col_same = pl.multiple_of(half * half_cols + c * wc, LANES)
    w_sends = [me.copy(w_o.at[:, pl.ds(col, wc)], wf.at[k], wss.at[k], wrs.at[k], yy, c)
               for k, (col, yy) in enumerate(((col_opp, me.dn), (col_opp, me.up), (col_same, me.dg)))]
    for s in w_sends:
        s.start()

    def dq_load(j):
        cols = pl.ds(pl.multiple_of(j * nj, nj), nj)
        return pltpu.make_async_copy(w_dq.at[:, cols], wdq.at[:, cols], dsem.at[j])

    late = [pltpu.make_async_copy(w_uq.at[:, pl.ds(pl.multiple_of(me.core * wuq.shape[1], LANES), wuq.shape[1])], wuq, wsem.at[1])]

    def bid(n):
        return lax.div(pos[n, 0], bl)

    lane_b = lax.broadcasted_iota(jnp.int32, (bl, LANES), 1)
    row_b = lax.broadcasted_iota(jnp.int32, (bl, LANES), 0)
    sign = jnp.where(lax.rem(lane_b, HALF) < QUARTER, -1.0, 1.0)

    @pl.loop(0, every)
    def _(n):
        for k in range(HALVES):
            b = bid(n) if k == 0 else HALVES * n_cp - 1 - bid(n)
            ang = (b * bl + row_b).astype(F32) * fr[...]
            r = pl.ds(pl.multiple_of((HALVES * n + k) * bl, bl), bl)
            csb[r, :LANES] = jnp.cos(ang)
            csb[r, LANES:] = jnp.sin(ang) * sign

    cs_store = pltpu.make_async_copy(csb, cs_own, csem)
    cs_store.start()
    kv_load.wait()

    lane = lax.broadcasted_iota(jnp.int32, (rows, LANES), 1)
    low32 = lax.rem(lane, HALF) < QUARTER
    upper = lax.broadcasted_iota(jnp.int32, (rows, LANES), 0) < rows // HALVES
    tile = lambda t: pl.ds(t * HALVES, HALVES)
    block = lambda t: pl.ds(pl.multiple_of(t * rows, rows), rows)

    def norm(t32, gain):
        return (t32 * lax.rsqrt(jnp.mean(t32 * t32, axis=-1, keepdims=True) + NORM_EPS) * gain).astype(BF16)

    def lat_copy(k, i, t, ref, yy, cc):
        return me.copy(ref, ref, lss.at[t, k], lrs.at[t, i], yy, cc)

    def own_store(t):
        return pltpu.make_async_copy(pay.at[lax.rem(t, HALVES)], lat_all.at[c, tile(t)], lsem.at[t])

    def out_stores(t):
        sl = lax.rem(t, HALVES)
        return [pltpu.make_async_copy(pay.at[sl, :, :, :, :kr_rank], latent.at[tile(t)], osem.at[0, sl]),
                pltpu.make_async_copy(krb.at[sl], k_rope.at[block(t)], osem.at[1, sl])]

    def send_own(t):
        own_store(t).wait()
        for k, cc in ((0, partner), (1, left), (2, right)):
            lat_copy(k, k, t, lat_all.at[c, tile(t)], y, cc).start()

    def settle_stores(t):
        for s in out_stores(t):
            s.wait()

    @pl.loop(0, n_t)
    def _(t):
        load_x(t).wait()

        pl.when(t == 0)(lambda: load_x(1).start())

        @pl.when(t == 1)
        def _():
            for j in range(wdq.shape[1] // nj):
                dq_load(j).start()
            for d in late:
                d.start()

        pl.when(t > 0)(lambda: send_own(t - 1))

        sl = lax.rem(t, HALVES)

        def kv_dot(wrows):
            d = lax.dot_general(xbuf[sl], wdkv[wrows, :], (((1,), (1,)), ((), ())), preferred_element_type=F32)
            return d.astype(BF16)

        @pl.loop(0, kr_rank // nj)
        def _(j):
            js = pl.ds(pl.multiple_of(j * nj, nj), nj)
            kvb[:, js] = kv_dot(js)

        u = kv_dot(pl.ds(kr_rank, wdkv.shape[0] - kr_rank)).astype(F32)
        pl.when(t + HALVES < n_t)(lambda: load_x(t + 2).start())
        lat = norm(kvb[...].astype(F32), gkv[...])
        u = jnp.concatenate([u, u], axis=1)
        w = jnp.where(low32, pltpu.roll(u, 96, 1), pltpu.roll(u, QUARTER, 1))
        rot = u * csb[block(t), :LANES] + w * csb[block(t), LANES:]
        pl.when(t >= HALVES)(lambda: settle_stores(t - 2))
        krb[sl] = rot[:, :HALF].astype(BF16)
        pay[sl, :, :, :, :kr_rank] = lat.reshape(HALVES, HALVES, bl, kr_rank)
        ids = jnp.where(upper, bid(HALVES * t), bid(HALVES * t + 1)).astype(F32)
        pay[sl, :, :, :, kr_rank:] = jnp.where(lane < HALF, rot, ids).astype(BF16).reshape(HALVES, HALVES, bl, LANES)
        for s in [own_store(t)] + out_stores(t):
            s.start()

    send_own(last)
    cs_store.wait()
    cs_send = me.copy(cs_own, cs_par, css, crs, y, partner)
    cs_send.start()
    for d in late:
        d.wait()

    def stage1(t):
        rp, lp = lat_all.at[right, tile(t)], lat_all.at[left, tile(t)]
        lat_copy(3, 1, t, rp, y, partner).wait_recv()
        lat_copy(3, 2, t, lp, y, partner).wait_recv()
        for k, ref in ((3, rp), (4, lp)):
            lat_copy(k, k, t, ref, y, partner).start()

        @pl.when(t < last)
        def _():
            for k, ref, cc in ((5, lat_all.at[left, tile(t), 0], right), (6, lat_all.at[right, tile(t), 1], left)):
                lat_copy(k, k, t, ref, y, cc).start()

        pl.when(t == last)(lambda: lat_copy(5, 5, t, id_rows(left), y, right).start())

    def id_rows(dev):
        return lat_all.at[dev, tile(last), 0, pl.ds(0, 16)]

    def stage2(t):
        for k in range(HALVES):
            ref = lat_all.at[far, tile(t), k]
            lat_copy(SPARE, 5 + k, t, ref, y, partner).wait_recv()
            lat_copy(7 + k, 7 + k, t, ref, y, partner).start()

    def project(src, wref, dst, width, before=None):
        @pl.loop(0, wref.shape[1] // width)
        def _(j):
            if before is not None:
                before(j)
            cols = pl.ds(pl.multiple_of(j * width, width), width)
            dst[:, cols] = jnp.dot(src[...], wref[:, cols], preferred_element_type=F32).astype(BF16)

    def q_store(u, dst, t):
        return pltpu.make_async_copy(qst.at[lax.rem(u, HALVES)], dst.at[block(t)], osem.at[3, lax.rem(u, HALVES)])

    def q_send(t):
        return me.copy(qn_o.at[block(t)], qn_p.at[block(t)], qss.at[t], qrs.at[t], y, partner)

    @pl.loop(0, n_t)
    def _(t):
        v = last - t
        pl.when(t >= HALVES)(lambda: load_x(v).wait())
        project(xbuf.at[lax.rem(v, HALVES)], wdq, qlat, nj, lambda j: pl.when(t == 0)(lambda: dq_load(j).wait()))
        pl.when(v >= HALVES)(lambda: load_x(v - 2).start())

        @pl.when(t == 0)
        def _():
            for k in (last - 1, last):
                settle_stores(k)

        stage1(t)
        sl = lax.rem(t, HALVES)
        qn[sl] = norm(qlat[...].astype(F32), gq[...])
        cp = pltpu.make_async_copy(qn.at[sl], qn_o.at[block(v)], osem.at[2, sl])
        cp.start()
        pl.when(t >= HALVES)(lambda: q_store(t, q_own, t - 2).wait())
        project(qn.at[sl], wuq, qst.at[sl], wuq.shape[1] // HALVES)
        cp.wait()
        q_send(v).start()
        q_store(t, q_own, v).start()

    def load_qp(t):
        return pltpu.make_async_copy(qn_p.at[block(last - t)], qn.at[lax.rem(t, HALVES)], osem.at[2, lax.rem(t, HALVES)])

    def take_qp(t):
        q_send(last - t).wait_recv()
        load_qp(t).start()

    take_qp(0)

    @pl.loop(0, n_t)
    def _(t):
        load_qp(t).wait()
        pl.when(t + 1 < n_t)(lambda: take_qp(t + 1))
        q_store(n_t + t, q_own, t).wait()
        project(qn.at[lax.rem(t, HALVES)], wuq, qst.at[lax.rem(n_t + t, HALVES)], wuq.shape[1] // HALVES)
        q_store(n_t + t, q_par, last - t).start()
        pl.when(t < last)(lambda: stage2(t))

    lat_copy(SPARE, 5, last, id_rows(far), y, partner).wait_recv()
    lat_copy(SPARE, 7, last, id_rows(far), y, partner).start()
    for k in range(HALVES):
        q_store(k, q_par, 0).wait()

    pr, pl_, pf = (lax.rem(partner + k, n_cp) for k in (HALVES, n_cp - HALVES, n_cp // HALVES))

    @pl.loop(0, n_t)
    def _(t):
        for i, ref in ((0, lat_all.at[partner, tile(t)]), (3, lat_all.at[pr, tile(t)]), (4, lat_all.at[pl_, tile(t)])):
            lat_copy(SPARE, i, t, ref, y, partner).wait_recv()
        for k in range(5):
            lat_copy(k, k, t, lat_all.at[c, tile(t)], y, partner).wait_send()

        @pl.when(t < last)
        def _():
            for k in range(HALVES):
                lat_copy(SPARE, 7 + k, t, lat_all.at[pf, tile(t), k], y, partner).wait_recv()
            for k in range(5, 9):
                lat_copy(k, k, t, lat_all.at[c, tile(t), 0], y, partner).wait_send()

        q_send(t).wait_send()

    lat_copy(SPARE, 7, last, id_rows(pf), y, partner).wait_recv()
    for k in (5, 7):
        lat_copy(k, k, last, id_rows(c), y, partner).wait_send()
    for s in w_sends + [cs_send]:
        s.wait()


def project_all(mesh, pos, x, w_dq, w_dkv, w_uq, g_q, g_kv, freq, w_o, bl):
    n_tp, n_cp = mesh.shape["tp"], mesh.shape["cp"]
    n_seq, seq, width = x.shape
    rows = HALVES * seq
    n_t = n_seq // HALVES
    rank, kvw = w_dq.shape[1], w_dkv.shape[1]
    kr = g_kv.shape[0]
    qw = w_uq.shape[1] // HALVES
    half_cols = width // HALVES
    wc = half_cols // n_cp
    total = n_seq * seq
    hbm = pl.BlockSpec(memory_space=pltpu.HBM)
    sds = jax.ShapeDtypeStruct
    dma = pltpu.SemaphoreType.DMA
    trig = sds((total, MXU), F32)
    return pl.pallas_call(
        functools.partial(proj_kernel, (n_tp, n_cp, n_t, half_cols, wc)),
        in_specs=[pl.BlockSpec(memory_space=pltpu.SMEM)] + [hbm] * 4 + [pl.BlockSpec(memory_space=pltpu.VMEM)] * 3 + [hbm],
        out_specs=[hbm] * 10,
        out_shape=[sds((n_cp, n_seq, 2, bl, kr + LANES), BF16), sds((n_seq, 2, bl, kr), BF16), sds((total, kvw - kr), BF16),
                   sds((total, qw), BF16), sds((total, qw), BF16), sds((3, w_o.shape[0], wc), BF16),
                   trig, trig, sds((total, rank), BF16), sds((total, rank), BF16)],
        scratch_shapes=[
            pltpu.VMEM((HALVES, rows, width), BF16), pltpu.VMEM((width, rank), BF16), pltpu.VMEM((kvw, width), BF16),
            pltpu.VMEM((rank, qw), BF16), pltpu.VMEM(trig.shape, F32), pltpu.VMEM((HALVES, HALVES, 2, bl, kr + LANES), BF16),
            pltpu.VMEM((HALVES, rows, kvw - kr), BF16), pltpu.VMEM((rows, kr), BF16), pltpu.VMEM((rows, rank), BF16),
            pltpu.VMEM((HALVES, rows, rank), BF16), pltpu.VMEM((HALVES, rows, qw), BF16),
            dma((HALVES,)), dma((HALVES,)), dma((rank // WIDE,)), dma, dma((4, HALVES)), dma((3,)), dma((3,)), dma((n_t, 9)), dma((n_t, 9)),
            dma((n_t,)), dma((n_t,)), dma, dma, dma((n_t,))],
        compiler_params=pltpu.CompilerParams(collective_id=0, has_side_effects=True, vmem_limit_bytes=63 * MIB),
        cost_estimate=pl.CostEstimate(flops=HALVES * total * (width * (rank + kvw) + HALVES * rank * qw), bytes_accessed=10**8,
                                      transcendentals=0),
        name="proj",
    )(pos, x.reshape(total, width), w_dq, w_dkv.T, w_uq, g_q, g_kv, freq, w_o)


def out_kernel(dims, x, w_o, wf, wx, ost_own, ost_par, obuf, out, wy, oy,
               wbuf, ov, xb, stage, wsem, osem, xsem, ssem, oss, ors, wss, wrs, ass, ars):
    n_tp, n_cp, n_seq, bl, half_cols = dims
    me = Place(n_tp, n_cp)
    cols, kb = xb.shape[-1], obuf.shape[-1]
    w, krows = cols // HALVES, w_o.shape[0]
    hk = krows // HALVES
    last = n_seq - 1
    half_of = lambda row: lax.rem(row, HALVES)
    tb = me.block(me.y, me.core)

    hb = kb // HALVES
    cut = [pl.ds(k * hb, hb) for k in range(HALVES)]
    to_last = lambda s, p: oy.at[s, p, 1]
    to_prev = lambda s, p: oy.at[s, p, 0]
    prev_fwd = me.o_forwards(lambda s, p: obuf.at[s, p, last, :, cut[0]], to_prev, oss.at[0], ors.at[0])
    last_sends = me.o_sends(ost_own.at[last, :, :, cut[1]], ost_par.at[last, :, :, cut[1]], to_last, oss.at[1], ors.at[1])
    last_fwd = me.o_forwards(to_last, to_last, oss.at[1], ors.at[1])
    def w_copy(k, src, dst, yy, cc):
        return me.copy(src, dst, wss.at[k], wrs.at[k], yy, cc)

    far_rows = [pl.ds(k * hk, hk) for k in range(HALVES)]
    (to_r, to_l), (rest_r, rest_l) = w_parts(krows)
    p_right, p_left, p_far = (lax.rem(me.partner + k, n_cp) for k in (HALVES, n_cp - HALVES, n_cp // HALVES))
    mine, side = (me.y, me.partner), ((me.y, me.right), (me.y, me.left))

    def w_move(k, buf, dev, part, to):
        return w_copy(k, buf.at[dev, :, part], wy.at[dev, :, part], *to)

    w_sends = [w_copy(0, wf.at[:, rest_r], wy.at[me.c, :, rest_r], *side[0]), w_copy(1, wf.at[:, rest_l], wy.at[me.c, :, rest_l], *side[1]),
               w_move(2, wx, me.left, to_r, mine), w_move(3, wx, me.right, to_l, mine),
               w_move(4, wx, me.left, far_rows[0], side[0]), w_move(5, wx, me.right, far_rows[1], side[1])]
    rest_fwd = [w_move(6, wy, me.left, rest_r, mine), w_move(7, wy, me.right, rest_l, mine)]
    far_fwd = [w_move(8 + k, wy, me.far, far_rows[k], mine) for k in range(HALVES)]

    def w_recv(k, dev, part):
        w_move(k, wy, dev, part, mine).wait_recv()

    n_m = n_seq // HALVES
    rows = HALVES * bl
    k_of = (None, me.flip, 1 - me.flip, HALVES)
    every = pl.ds(0, krows)
    own = ((wx, to_l), (wy, rest_l)), ((wx, to_r), (wy, rest_r))
    pieces = ((((wf, every),), ((wx.at[me.partner], every),)),) + tuple(
        (tuple((buf.at[dev], part) for buf, part in own[i]), ((wy.at[dev_p], every),))
        for i, (dev, dev_p) in enumerate(((me.right, p_right), (me.left, p_left)))) + ((((wy.at[me.far], every),), ((wy.at[p_far], every),)),)
    offs = [pl.multiple_of(v * w, LANES) for v in (me.core, 1 - me.core)]

    def col_of(j, row):
        dx = j + (j // HALVES) * (1 - HALVES * (j % HALVES))
        xq = lax.rem(lax.div(me.c, HALVES) + dx, n_cp // HALVES)
        return pl.multiple_of(half_of(row) * half_cols + xq * cols, LANES)

    def w_loads(j):
        b = j % HALVES
        out_ = [pltpu.make_async_copy(w_o.at[:, pl.ds(col_of(j, me.y), cols)], wbuf.at[b, 0], wsem.at[b, 0])]
        for r in range(1, SOURCES):
            for part in range(HALVES):
                for i, (buf, part_rows) in enumerate(pieces[j][part]):
                    out_.append(pltpu.make_async_copy(buf.at[k_of[r], part_rows], wbuf.at[b, r, part_rows, pl.ds(offs[part], w)],
                                                      wsem.at[b, HALVES * r + part + 8 * i]))
        return out_

    def x_load(j):
        return pltpu.make_async_copy(x.at[:, pl.ds(pl.multiple_of(tb * bl, bl), bl), pl.ds(col_of(j, me.y), cols)], xb.at[j % HALVES], xsem.at[j % HALVES])

    o_offs = [pl.multiple_of(v * kb, LANES) for v in (me.core, 1 - me.core)]

    def o_place(i, r, part, half=None):
        off = r * krows + o_offs[part] + (0 if half is None else half * hb)
        return ov.at[i, :, pl.ds(pl.multiple_of(off, LANES), kb if half is None else hb)]

    def o_load(i, r, part):
        src = ost_own.at[i, tb] if (r, part) == (0, 0) else obuf.at[r, part, i]
        return pltpu.make_async_copy(src, o_place(i, r, part), osem.at[i, HALVES * r + part])

    pairs = [(r, part) for r in range(SOURCES) for part in range(HALVES)]
    early = [o_load(i, r, part) for i in range(last - 1) for r, part in pairs]
    late = [o_load(last - 1, r, part) for r, part in pairs]
    for r, part in pairs:
        for half in range(HALVES):
            if (r, part) == (0, 0):
                src = ost_own.at[last, tb, :, cut[half]]
            else:
                src = oy.at[r, part, half] if half == 1 or r == 3 else obuf.at[r, part, last, :, cut[0]]
            late.append(pltpu.make_async_copy(src, o_place(last, r, part, half), osem.at[last, HALVES * r + part + 8 * half]))
    for d in w_loads(0) + early + [x_load(0)]:
        d.start()
    me.greet(((me.up, me.c), (me.dn, me.c), (me.up, me.partner), (me.dn, me.partner),
              (me.y, me.partner), (me.y, me.right), (me.y, me.left)))
    for s in last_sends + prev_fwd + w_sends:
        s.start()

    def region(row, j, m, n0=0, cnt=2):
        return out.at[pl.ds(HALVES * m + n0, cnt), pl.ds(pl.multiple_of(me.block(row, me.core) * bl, bl), bl), pl.ds(col_of(j, row), cols)]

    def ring(k, ref, j, m, yy):
        i = j * n_m + m
        return me.copy(ref, ref, ass.at[i, k], ars.at[i, k], yy, me.c)

    def tile_sends(j, m):
        ref = region(me.y, j, m)
        return ring(0, ref, j, m, me.up), ring(1, ref, j, m, me.dn)

    def forward(j, m):
        ring(0, region(me.dn, j, m), j, m, me.up).wait_recv()
        ring(2, region(me.dn, j, m, 0, 1), j, m, me.up).start()
        ring(1, region(me.up, j, m), j, m, me.up).wait_recv()
        ring(3, region(me.up, j, m, 1, 1), j, m, me.dn).start()

    nt = MXU

    def tile(j, m):
        b = j % HALVES

        @pl.loop(0, cols // nt)
        def _(t):
            cs_ = pl.ds(pl.multiple_of(t * nt, nt), nt)
            a = ov[pl.ds(HALVES * m, HALVES)].reshape(rows, SOURCES * krows)
            s = None
            for r in range(SOURCES):
                d = jnp.dot(a[:, r * krows:(r + 1) * krows], wbuf[b, r, :, cs_], preferred_element_type=F32)
                s = d if s is None else s + d
            xr = xb[b, pl.ds(HALVES * m, HALVES), :, cs_].reshape(rows, nt).astype(F32)
            stage[:, :, cs_] = (xr + s).astype(BF16).reshape(2, bl, nt)

        c = pltpu.make_async_copy(stage, region(me.y, j, m), ssem)
        c.start()
        c.wait()
        for s in tile_sends(j, m):
            s.start()

    def need(j):
        if j == 0:
            w_recv(1, me.right, rest_l)
            rest_fwd[1].start()
            w_recv(3, p_right, to_l)
            w_recv(7, p_right, rest_l)
        elif j == 1:
            w_recv(0, me.left, rest_r)
            rest_fwd[0].start()
            w_recv(2, p_left, to_r)
            w_recv(6, p_left, rest_r)
        else:
            for k in range(HALVES):
                w_recv(4 + k, me.far, far_rows[k])
                far_fwd[k].start()
            for k in range(HALVES):
                w_recv(8 + k, p_far, far_rows[k])
        for d in w_loads(j + 1) + [x_load(j + 1)]:
            d.start()

    def late_o():
        for k in DIRECT:
            last_sends[k].wait_recv()
        for f in prev_fwd + last_fwd:
            f.wait_recv()
        for d in late:
            d.start()
        for d in late:
            d.wait()

    for k, f in zip(FORWARDED, last_fwd):
        last_sends[k].wait_recv()
        f.start()
    for d in early:
        d.wait()

    @pl.loop(0, SOURCES * n_m)
    def _(i):
        j, m = lax.div(i, n_m), lax.rem(i, n_m)
        for jj in range(SOURCES):
            @pl.when(i == jj * n_m)
            def _(jj=jj):
                for d in w_loads(jj) + [x_load(jj)]:
                    d.wait()
                if jj == 1:
                    need(jj)
        pl.when(i == n_m - 1)(late_o)
        tile(j, m)
        pl.when(i == 0)(lambda: need(0))

        @pl.when(j > 0)
        def _():
            forward(j - 1, m)

        pl.when(i == 3 * n_m - 1)(lambda: need(2))

    @pl.loop(0, n_m)
    def _(m):
        forward(3, m)

    @pl.loop(0, SOURCES * n_m)
    def _(i):
        j, m = lax.div(i, n_m), lax.rem(i, n_m)
        for k, row, n0, cnt in ((0, me.y, 0, HALVES), (1, me.y, 0, HALVES), (2, me.dn, 0, 1), (3, me.up, 1, 1)):
            r = region(row, j, m, n0, cnt)
            me.copy(r, r, ass.at[i, k], ars.at[i, k], me.up, me.c).wait_send()
        for k, n0 in ((HALVES, 0), (3, 1)):
            r = region(me.dg, j, m, n0, 1)
            me.copy(r, r, ass.at[i, k], ars.at[i, k], me.up, me.c).wait_recv()

    for s in last_sends + prev_fwd + last_fwd + w_sends + rest_fwd + far_fwd:
        s.wait_send()


def out_product(mesh, x, w_o, wf, wx, ost_own, ost_par, obuf):
    n_tp, n_cp = mesh.shape["tp"], mesh.shape["cp"]
    n_seq, seq, width = x.shape
    bl = seq // HALVES
    cols = HALVES * wf.shape[-1]
    krows = w_o.shape[0]
    hbm = pl.BlockSpec(memory_space=pltpu.HBM)
    dma = pltpu.SemaphoreType.DMA
    sds = jax.ShapeDtypeStruct
    tiles = HALVES * n_seq
    return pl.pallas_call(
        functools.partial(out_kernel, (n_tp, n_cp, n_seq, bl, width // HALVES)),
        in_specs=[hbm] * 7, out_specs=[hbm] * 3,
        out_shape=[sds(x.shape, BF16), sds(wx.shape, BF16), sds((SOURCES, HALVES, HALVES, bl, obuf.shape[-1] // HALVES), BF16)],
        scratch_shapes=[
            pltpu.VMEM((HALVES, SOURCES, krows, cols), BF16), pltpu.VMEM((n_seq, bl, SOURCES * krows), BF16), pltpu.VMEM((HALVES, n_seq, bl, cols), BF16),
            pltpu.VMEM((HALVES, bl, cols), BF16), dma((HALVES, 16)), dma((n_seq, 16)), dma((HALVES,)), dma, dma((HALVES, 7)), dma((HALVES, 7)),
            dma((10,)), dma((10,)), dma((tiles, 4)), dma((tiles, 4))],
        compiler_params=pltpu.CompilerParams(collective_id=2, has_side_effects=True, vmem_limit_bytes=63 * MIB),
        cost_estimate=pl.CostEstimate(flops=n_seq * seq * cols * 16 * krows, bytes_accessed=10**8, transcendentals=0),
        name="outp",
    )(x, w_o, wf, wx, ost_own, ost_par, obuf)[0]


def settle_kernel(src, lat, kr, dst, lat_out, kr_out, buf, lbuf, kbuf, tbuf, rsem, wsem, lsem, ksem):
    n = buf.shape[0]
    reads = [pltpu.make_async_copy(src.at[i], buf.at[i], rsem.at[i]) for i in range(n)]
    writes = [pltpu.make_async_copy(buf.at[i], dst.at[i], wsem.at[i]) for i in range(n)]
    small = [pltpu.make_async_copy(*p) for p in ((kr, kbuf, ksem.at[0]), (lat, lbuf, lsem.at[0]))]
    small_out = [pltpu.make_async_copy(*p) for p in ((tbuf, kr_out, ksem.at[1]), (lbuf, lat_out, lsem.at[1]))]
    for d in small + reads:
        d.start()
    for d in small:
        d.wait()
    for i in range(tbuf.shape[0]):
        tbuf[i] = kbuf[i].astype(F32).T.astype(BF16)
    for d in small_out:
        d.start()
    for a, b in zip(reads, writes):
        a.wait()
        b.start()
    for d in writes + small_out:
        d.wait()


def settle(out, lat, kr):
    n_seq, seq, width = out.shape
    parts = 4 * n_seq
    shape = (parts, n_seq * seq // parts, width)
    lat_shape, kr_shape = (n_seq, seq, lat.shape[-1]), (n_seq, seq, kr.shape[-1])
    turned = (n_seq, kr.shape[-1], seq)
    hbm = pl.BlockSpec(memory_space=pltpu.HBM)
    sds = jax.ShapeDtypeStruct
    dma = pltpu.SemaphoreType.DMA
    a, b, c = pl.pallas_call(
        settle_kernel, in_specs=[hbm] * 3, out_specs=[hbm] * 3,
        out_shape=[sds(shape, BF16), sds(lat_shape, BF16), sds(turned, BF16)],
        scratch_shapes=[pltpu.VMEM(shape, BF16), pltpu.VMEM(lat_shape, BF16), pltpu.VMEM(kr_shape, BF16), pltpu.VMEM(turned, BF16),
                        dma((parts,)), dma((parts,)), dma((HALVES,)), dma((HALVES,))],
        compiler_params=pltpu.CompilerParams(vmem_limit_bytes=63 * MIB), name="settle",
    )(out.reshape(shape), lat.reshape(lat_shape), kr.reshape(kr_shape))
    return a.reshape(out.shape), b, jnp.swapaxes(c, 1, HALVES)


ROPE_BASE = 10000.0


def solution(mesh):
    def local_step(x, pos, w_dq, g_q, w_uq, w_dkv, g_kv, w_uk, w_uv, w_o):
        n_seq, seq, _ = x.shape
        n_cp = mesh.shape["cp"]
        bl = seq // HALVES
        nb = HALVES * n_cp
        kv_rank = g_kv.shape[0]
        rope = w_dkv.shape[1] - kv_rank
        heads = (w_uq.shape[1] - w_uk.shape[1]) // rope
        nope = w_uk.shape[1] // heads
        c = lax.axis_index("cp")
        core = c % HALVES

        freq = np.tile(ROPE_BASE ** (-2.0 * np.arange(rope // HALVES) / rope), LANES // (rope // HALVES))[None].astype(np.float32)
        lat_all, latent, k_rope, q_own, q_par, wf, cs_own, cs_par, _, _ = project_all(
            mesh, pos, x, w_dq, w_dkv, w_uq, g_q, g_kv, freq, w_o, bl)
        q_own, q_par = (a.reshape(n_seq, seq, -1) for a in (q_own, q_par))
        ids = lat_all[:, :, 0, 0, kv_rank + rope].astype(jnp.int32)
        blocks = jnp.arange(nb)
        first = ids[:, :, None] == blocks
        second = nb - 1 - ids[:, :, None] == blocks
        dev = jnp.arange(n_cp)[:, None, None]
        slots = jnp.sum(jnp.where(first, HALVES * dev, 0) + jnp.where(second, HALVES * dev + 1, 0), axis=0)
        mine = [jnp.sum(jnp.where(jnp.arange(n_cp)[:, None] == k, ids, 0), axis=0) for k in (c, c ^ 1)]
        last = nb // 4 - 1
        extra = []
        for i, b in enumerate(mine):
            is_first = b > last
            chunk = jnp.where(is_first, 1, last)
            extra += [jnp.where(is_first, i, 2 + i), chunk, jnp.where(is_first, b, nb - 1 - b) * bl - chunk * 4 * bl, is_first]
        tab = jnp.concatenate([slots, jnp.stack(mine + extra, axis=1).astype(jnp.int32)], axis=1).astype(jnp.int32)

        ost_own, ost_par, obuf, wx, _ = attention(mesh, tab, q_own, q_par, cs_own, cs_par, w_uk, w_uv, lat_all, wf, (nope + rope) ** -0.5)
        return settle(out_product(mesh, x, w_o, wf, wx, ost_own, ost_par, obuf), latent, k_rope)

    seq_spec = P("dp", "cp", None)
    whole = P(None, None)
    in_specs = (seq_spec, P("dp", "cp"), whole, P(None), P(None, "tp"), whole, P(None), P(None, "tp"), P(None, "tp"), P("tp", None))
    return jax.shard_map(local_step, mesh=mesh, in_specs=in_specs, out_specs=(seq_spec,) * 3, check_vma=False)
```

```python
import functools
import numpy as np
import jax, jax.numpy as jnp
from jax import lax
from jax.experimental import pallas as pl
from jax.experimental.pallas import tpu as pltpu
from jax.sharding import PartitionSpec as P

F32, BF16 = jnp.float32, jnp.bfloat16
NEG = float("-inf")
LOG2E = 1.4426950408889634
LANES, HALF, QUARTER, MXU, WIDE, PAIR = 128, 64, 32, 256, 512, 384
HALVES = 2
SOURCES = 4
MIB = 2**20
FORWARDED, DIRECT = (1, 4), (0, 2, 3)
SPARE = 7


MESH = pl.DeviceIdType.MESH
NORM_EPS = 1e-6


class Place:
    def __init__(self, n_tp, n_cp):
        self.dp, self.y, self.c = (lax.axis_index(a) for a in ("dp", "tp", "cp"))
        y, c = self.y, self.c
        self.n_tp = n_tp
        self.core = lax.rem(c, HALVES)
        self.partner = c + 1 - HALVES * self.core
        self.right, self.left, self.far = (lax.rem(c + k, n_cp) for k in (HALVES, n_cp - HALVES, n_cp // HALVES))
        self.up, self.dn, self.dg = (lax.rem(y + k, n_tp) for k in (1, n_tp - 1, n_tp // HALVES))
        self.flip = lax.rem(y + self.core, HALVES)
        self.mate = lax.rem(y + 1 + HALVES * self.flip, n_tp)
        self.other = lax.rem(y + 3 - HALVES * self.flip, n_tp)

    def block(self, row, core):
        return lax.div(lax.rem(row + (self.n_tp - 1) * core, self.n_tp), HALVES)

    def greet(self, peers):
        barrier = pltpu.get_barrier_semaphore()
        for yy, cc in peers:
            pl.semaphore_signal(barrier, inc=1, device_id=(self.dp, yy, cc), device_id_type=MESH)
        pl.semaphore_wait(barrier, len(peers))

    def copy(self, src, dst, ss, rs, yy, cc):
        return pltpu.make_async_remote_copy(src_ref=src, dst_ref=dst, send_sem=ss, recv_sem=rs,
                                            device_id=(self.dp, yy, cc), device_id_type=MESH)

    def o_sends(self, own, par, dst, ss, rs):
        tb, tp = self.block(self.y, self.core), self.block(self.y, 1 - self.core)
        ways = [(own, tb, 1, 0, self.mate, self.c), (own, 1 - tb, 2, 0, self.other, self.c), (par, tp, 0, 1, self.y, self.partner),
                (par, tp, 1, 1, self.other, self.partner), (par, 1 - tp, 2, 1, self.mate, self.partner)]
        return [self.copy(a.at[blk], dst(src, part), ss.at[k], rs.at[k], yy, cc)
                for k, (a, blk, src, part, yy, cc) in enumerate(ways)]

    def o_forwards(self, src, dst, ss, rs):
        return [self.copy(src(2, part), dst(3, part), ss.at[5 + part], rs.at[5 + part], self.mate, self.c) for part in range(HALVES)]


def w_parts(rows):
    cut = rows // 16
    return (pl.ds(0, rows - cut), pl.ds(cut, rows - cut)), (pl.ds(rows - cut, cut), pl.ds(0, cut))


def attn_kernel(dims, tab, *refs):
    G, NB, BL, HP, scale2, n_tp, n_cp = dims
    CK = HALVES * BL
    H, HG = HALVES * HP, HP
    q_own, q_par, cs_own, cs_par, w_uk, w_uv, lat, wf = refs[:8]
    ost_own, ost_par, obuf, wx, lf = refs[8:13]
    latbuf, KT, V, Q, sF, sS, sX, mx, lsum, acc, ob, wk, wkT, wv, sem, ksem, osem, oss, ors, wss, wrs, fss, frs = refs[13:]
    n, g = pl.program_id(0), pl.program_id(1)
    u, U = HALVES * n + g, HALVES * G
    me = Place(n_tp, n_cp)
    rows_ = ((me.up, me.c), (me.dn, me.c), (me.up, me.partner), (me.dn, me.partner))
    w_to = ((me.y, me.partner), (me.y, me.right), (me.y, me.left))

    krows = wf.shape[1]
    w_rows = (pl.ds(0, krows),) + w_parts(krows)[0]

    def w_send(k, slot):
        return me.copy(wf.at[:, w_rows[k]], wx.at[slot, :, w_rows[k]], wss.at[k], wrs.at[k], *w_to[k])

    tail = G - 2
    p_far = lax.rem(me.partner + n_cp // HALVES, n_cp)
    far_from = [lat.at[me.left, pl.ds(tail, HALVES), 0], lat.at[me.right, pl.ds(tail, HALVES), 1]] + [lf.at[0, :, k] for k in range(HALVES)]
    far_to = [lf.at[0, :, k] for k in range(HALVES)] + [lf.at[1, :, k] for k in range(HALVES)]
    far = [me.copy(a, b, fss.at[k], frs.at[k], *(w_to[1:] + w_to[:1] * HALVES)[k]) for k, (a, b) in enumerate(zip(far_from, far_to))]

    def copy_in(src, dev):
        return pltpu.make_async_copy(src, latbuf.at[pl.ds(HALVES * dev, HALVES)], sem.at[dev])

    def start_lat(i):
        for k in range(n_cp):
            dev = lax.rem(me.c + k, n_cp)
            away = jnp.logical_and(i >= tail, jnp.logical_or(dev == me.far, dev == p_far))
            which = jnp.where(dev == me.far, 0, 1)
            pl.when(jnp.logical_not(away))(lambda: copy_in(lat.at[dev, i], dev).start())
            pl.when(away)(lambda: copy_in(lf.at[which, lax.rem(i, HALVES)], dev).start())

    def copies(i):
        return [copy_in(lat.at[p, i], p) for p in range(n_cp)]

    def unit(ref, i):
        w = ob.shape[-1]
        return ref.at[lax.div(i, HALVES), :, :, pl.ds(pl.multiple_of(lax.rem(i, HALVES) * w, LANES), w)]

    def landing(i):
        w = ob.shape[-1]
        return lambda s, p: obuf.at[s, p, lax.div(i, HALVES), :, pl.ds(pl.multiple_of(lax.rem(i, HALVES) * w, LANES), w)]

    def o_store(i):
        return [pltpu.make_async_copy(ob.at[k], unit(dst, i), osem.at[k]) for k, dst in enumerate((ost_own, ost_par))]

    def o_sends(i):
        return me.o_sends(unit(ost_own, i), unit(ost_par, i), landing(i), oss.at[i], ors.at[i])

    def o_forwards(i):
        return me.o_forwards(landing(i), landing(i), oss.at[i], ors.at[i])

    hw = wv.shape[1]
    kv_loads = [pltpu.make_async_copy(a.at[:, pl.ds(pl.multiple_of(me.core * hw, LANES), hw)], b, ksem.at[k])
                for k, (a, b) in enumerate(((w_uk, wk), (w_uv, wv)))]

    @pl.when(u == 0)
    def _():
        for c in kv_loads:
            c.start()
        start_lat(n)
        me.greet(rows_ + w_to)
        for s in far[:2] + [w_send(k, me.c) for k in range(3)]:
            s.start()
        for c in kv_loads:
            c.wait()
        wkT[...] = wk[...].T

    @pl.when(g == 0)
    def _():
        lane = lax.broadcasted_iota(jnp.int32, (BL, LANES), 1)
        low64 = lane < HALF
        low32 = lax.rem(lane, HALF) < QUARTER
        for src_i, (q, cs) in enumerate(((q_own, cs_own), (q_par, cs_par))):
            @pl.loop(0, HALVES)
            def _(half, src_i=src_i, q=q, cs=cs):
                r0 = half * 2 + src_i
                rows = pl.ds(pl.multiple_of(half * BL, BL), BL)
                ct = cs[rows, :LANES]
                st = cs[rows, LANES:]
                for p in range(HP):
                    a = q[0, rows, p * PAIR:p * PAIR + LANES]
                    b = q[0, rows, p * PAIR + LANES:p * PAIR + MXU].astype(F32)
                    c = q[0, rows, p * PAIR + MXU:p * PAIR + PAIR].astype(F32)
                    u = jnp.where(low64, b, c)
                    no = jnp.where(low64, c, b).astype(BF16)
                    w = jnp.where(low32, pltpu.roll(u, 96, 1), pltpu.roll(u, QUARTER, 1))
                    rot = (u * ct + w * st).astype(BF16)
                    Q[HALVES * p, r0, :, :LANES] = a
                    Q[HALVES * p, r0, :, LANES:MXU] = rot
                    Q[HALVES * p + 1, r0, :, :LANES] = no
                    Q[HALVES * p + 1, r0, :, LANES:MXU] = rot

        for c in copies(n):
            c.wait()

    @pl.when(u > 0)
    def _():
        for c in o_store(u - 1):
            c.wait()
        for s in o_sends(u - 1):
            s.start()

    WB = 4 * BL
    lane_k = lax.broadcasted_iota(jnp.int32, (WB, LANES), 1)
    KR = wkT.shape[1]
    heads = pl.ds(pl.multiple_of(g * HG * LANES, LANES), HG * LANES)

    b0, b1 = tab[n, NB], tab[n, NB + 1]

    @pl.loop(0, NB // 4)
    def _(kc):
        blocks = jnp.concatenate([latbuf[tab[n, kc * 4 + j]] for j in range(SOURCES)], axis=0)
        lt = blocks[:, :KR]
        kr = jnp.where(lane_k < HALF, blocks[:, KR:].astype(F32), 0.0)
        krT = kr.T.astype(BF16)
        krO = jnp.concatenate([krT[HALF:], krT[:HALF]], axis=0)
        kt = lax.dot_general(wkT[heads, :], lt, (((1,), (1,)), ((), ())), preferred_element_type=F32).astype(BF16)
        V[kc] = jnp.dot(lt, wv[:, heads], preferred_element_type=F32).astype(BF16)
        for h in range(HG):
            k = kt[h * LANES:h * LANES + LANES]
            KT[kc, h, :LANES] = k if h % HALVES == 0 else jnp.concatenate([k[HALF:], k[:HALF]], axis=0)
            KT[kc, h, LANES:] = krT if h % HALVES == 0 else krO

    @pl.when(u == G - 2)
    def _():
        for k in range(HALVES):
            far[k].wait_recv()
            far[2 + k].start()

    @pl.when(u == HALVES * tail - 1)
    def _():
        for f in far[2:]:
            f.wait_recv()

    pl.when(jnp.logical_and(g == 1, n + 1 < G))(lambda: start_lat(n + 1))

    HR = HALVES * BL
    R = HALVES * HR
    WK = 4 * BL
    nS = NB // 4 - 1
    row = lax.broadcasted_iota(jnp.int32, (HR, WK), 0)
    col = lax.broadcasted_iota(jnp.int32, (HR, WK), 1)
    dF = jnp.where(row < BL, b0 * BL + row, (b1 - 1) * BL + row) - col
    dS = jnp.where(row < BL, (NB - 1 - b0) * BL + row, (NB - 2 - b1) * BL + row) - col
    rF, rS = slice(HR), slice(HR, R)
    extra = []
    for i in range(HALVES):
        at = [tab[n, NB + 2 + 4 * i + k] for k in range(SOURCES)]
        is_first = row[:BL, :LANES] * 0 + at[3] > 0
        extra.append((at[0], at[1], row[:BL] + at[2] - col[:BL], is_first, pl.ds(i * BL, BL), pl.ds((2 + i) * BL, BL)))

    def fold(t):
        w = t.shape[1] // HALVES
        t = jnp.maximum(t[:, :w], t[:, w:])
        return t if w == LANES else fold(t)

    def p1(c):
        for h in range(HG):
            q = Q[g * HG + h, 2:].reshape(HR, MXU) if c else Q[g * HG + h].reshape(R, MXU)
            s = jnp.dot(q, KT[c, h], preferred_element_type=F32) * scale2
            if c == 0:
                f = jnp.where(dF >= 0, s[:HR], NEG)
                sF[h] = f
                mx[h, rF] = fold(f)
                s = s[HR:]
            elif c == nS - 1:
                s = jnp.where(dS >= c * WK, s, NEG)
            sS[h, c] = s
            mx[h, rS] = jnp.maximum(mx[h, rS], fold(s)) if c else fold(s)

    def p1x():
        for h in range(HG):
            for i, (block, chunk, d, is_first, r_f, r_s) in enumerate(extra):
                s = jnp.dot(Q[g * HG + h, block], KT[chunk, h], preferred_element_type=F32) * scale2
                s = jnp.where(d >= 0, s, NEG)
                sX[h, i] = s
                m = fold(s)
                for r, t in ((r_f, jnp.where(is_first, m, NEG)), (r_s, jnp.where(is_first, NEG, m))):
                    t = jnp.maximum(mx[h, r], t)
                    mx[h, r] = jnp.broadcast_to(jnp.max(t, axis=1, keepdims=True), (BL, LANES))

    def weigh(load, chunk, h):
        es, ls = [], None
        for j in range(WK // LANES):
            e = jnp.exp2(load(slice(j * LANES, j * LANES + LANES)))
            ls = e if ls is None else ls + e
            es.append(e.astype(BF16))
        return ls, jnp.dot(jnp.concatenate(es, axis=1), V[chunk, :, h * LANES:h * LANES + LANES], preferred_element_type=F32)

    def p2(c):
        for h in range(HG):
            def load(js):
                t = sS[h, c, :, js] - mx[h, rS]
                return t if c else jnp.concatenate([sF[h, :, js] - mx[h, rF], t], axis=0)
            ls, pv = weigh(load, c, h)
            r = rS if c else slice(R)
            lsum[h, r] = lsum[h, r] + ls if c else ls
            acc[h, r] = acc[h, r] + pv if c else pv

    def p2x():
        for h in range(HG):
            for i, (_, chunk, _, is_first, r_f, r_s) in enumerate(extra):
                m = jnp.where(is_first, mx[h, r_f], mx[h, r_s])
                ls, pv = weigh(lambda js: sX[h, i, :, js] - m, chunk, h)
                for k, r in enumerate((r_f, r_s)):
                    pick = (lambda t: jnp.where(is_first, t, 0.0)) if k == 0 else (lambda t: jnp.where(is_first, 0.0, t))
                    l = lsum[h, r] + pick(ls)
                    total = acc[h, r] + pick(pv)
                    ob[i, k, :, h * LANES:h * LANES + LANES] = (total * (1.0 / jnp.sum(l, axis=1, keepdims=True))).astype(BF16)

    for c in range(nS):
        p1(c)
    p1x()

    @pl.when(u > 1)
    def _():
        for k, f in zip(FORWARDED, o_forwards(u - 2)):
            o_sends(u - 2)[k].wait_recv()
            f.start()

    for c in range(nS):
        p2(c)
    p2x()
    for c in o_store(u):
        c.start()

    @pl.when(u == U - 1)
    def _():
        for c in o_store(u):
            c.wait()

        def drain_forward(i, _):
            for f in o_forwards(i):
                f.wait()
            return 0

        @pl.loop(0, U - 1)
        def _(i):
            for k, s in enumerate(o_sends(i)):
                s.wait_send()
                if k in DIRECT:
                    s.wait_recv()

        lax.fori_loop(0, U - 2, drain_forward, 0)
        for k in FORWARDED:
            o_sends(U - 2)[k].wait_recv()
        for f in far:
            f.wait_send()
        for k, slot in enumerate((me.partner, me.left, me.right)):
            w_send(k, me.c).wait_send()
            w_send(k, slot).wait_recv()


def attention(mesh, tab, q_own, q_par, cs_own, cs_par, w_uk, w_uv, lat, wf, soft_scale):
    G, T = tab.shape[0], q_own.shape[1] * mesh.shape["cp"]
    BL = q_own.shape[1] // HALVES
    NB = T // BL
    KR, VD = w_uv.shape[0], w_uv.shape[1] // HALVES
    H = VD // LANES
    R = 4 * BL
    dims = (G, NB, BL, H // HALVES, float(soft_scale * LOG2E), mesh.shape["tp"], mesh.shape["cp"])
    blk = lambda a: pl.BlockSpec((1,) + a.shape[1:], lambda n, g, t: (n, 0, 0))
    hbm = pl.BlockSpec(memory_space=pltpu.HBM)
    dma = pltpu.SemaphoreType.DMA
    sds = jax.ShapeDtypeStruct
    ost = sds((G, 2, BL, VD), BF16)
    HG = H // HALVES
    stat = pltpu.VMEM((HG, R, LANES), F32)
    return pl.pallas_call(
        functools.partial(attn_kernel, dims),
        grid_spec=pltpu.PrefetchScalarGridSpec(
            num_scalar_prefetch=1, grid=(G, HALVES),
            in_specs=[blk(q_own), blk(q_par)] + [pl.BlockSpec((HALVES * BL, cs_own.shape[1]), lambda n, g, t: (n, 0))] * 2 + [hbm] * 4,
            out_specs=[hbm] * 5,
            scratch_shapes=[
                pltpu.VMEM((NB, BL, lat.shape[-1]), BF16), pltpu.VMEM((NB // 4, HG, MXU, R), BF16), pltpu.VMEM((NB // 4, R, VD // HALVES), BF16),
                pltpu.VMEM((H, 4, BL, MXU), BF16), pltpu.VMEM((HG, R // HALVES, R), F32),
                pltpu.VMEM((HG, NB // 4 - 1, R // HALVES, R), F32), pltpu.VMEM((HG, 2, BL, R), F32), stat, stat, stat, pltpu.VMEM((HALVES, HALVES, BL, VD // HALVES), BF16),
                pltpu.VMEM((KR, VD), BF16), pltpu.VMEM((VD, KR), BF16), pltpu.VMEM((KR, VD), BF16),
                dma((NB // HALVES,)), dma((HALVES,)), dma((HALVES,)), dma((HALVES * G, 7)), dma((HALVES * G, 7)), dma((3,)), dma((3,)), dma((SOURCES,)), dma((SOURCES,))],
        ),
        out_shape=[ost, ost, sds((SOURCES, HALVES, G, BL, VD), BF16), sds((mesh.shape["cp"],) + wf.shape, BF16),
                   sds((HALVES, HALVES) + lat.shape[2:], BF16)],
        compiler_params=pltpu.CompilerParams(collective_id=1, has_side_effects=True, vmem_limit_bytes=63 * MIB),
        cost_estimate=pl.CostEstimate(flops=G * H * T * R * 800, bytes_accessed=G * T * 640 * 2, transcendentals=0),
        name="attn",
    )(tab, q_own, q_par, cs_own, cs_par, w_uk, w_uv, lat, wf)


def proj_kernel(dims, pos, x, w_dq, w_dkv, w_uq, gq, gkv, fr, w_o,
                lat_all, latent, k_rope, q_own, q_par, wf, cs_own, cs_par, qn_o, qn_p,
                xbuf, wdq, wdkv, wuq, csb, pay, krb, kvb, qlat, qn, qst,
                xsem, wsem, dsem, csem, osem, wss, wrs, lss, lrs, qss, qrs, css, crs, lsem):
    n_tp, n_cp, n_t, half_cols, wc = dims
    me = Place(n_tp, n_cp)
    y, c, partner, right, left, far = me.y, me.c, me.partner, me.right, me.left, me.far

    rows = xbuf.shape[1]
    bl = pay.shape[3]
    kr_rank = gkv.shape[0]
    nj = WIDE
    last = n_t - 1
    every = HALVES * n_t

    def load_x(i):
        return pltpu.make_async_copy(x.at[pl.ds(pl.multiple_of(lax.rem(i, n_t) * rows, rows), rows), :], xbuf.at[lax.rem(i, HALVES)],
                                     xsem.at[lax.rem(i, HALVES)])

    kv_load = pltpu.make_async_copy(w_dkv, wdkv, wsem.at[0])
    kv_load.start()
    load_x(0).start()
    me.greet([(me.up, c), (me.dn, c), (me.dg, c), (y, partner), (y, right), (y, left)])
    half = lax.rem(y, HALVES)
    col_opp = pl.multiple_of((1 - half) * half_cols + c * wc, LANES)
    col_same = pl.multiple_of(half * half_cols + c * wc, LANES)
    w_sends = [me.copy(w_o.at[:, pl.ds(col, wc)], wf.at[k], wss.at[k], wrs.at[k], yy, c)
               for k, (col, yy) in enumerate(((col_opp, me.dn), (col_opp, me.up), (col_same, me.dg)))]
    for s in w_sends:
        s.start()

    def dq_load(j):
        cols = pl.ds(pl.multiple_of(j * nj, nj), nj)
        return pltpu.make_async_copy(w_dq.at[:, cols], wdq.at[:, cols], dsem.at[j])

    late = [pltpu.make_async_copy(w_uq.at[:, pl.ds(pl.multiple_of(me.core * wuq.shape[1], LANES), wuq.shape[1])], wuq, wsem.at[1])]

    def bid(n):
        return lax.div(pos[n, 0], bl)

    lane_b = lax.broadcasted_iota(jnp.int32, (bl, LANES), 1)
    row_b = lax.broadcasted_iota(jnp.int32, (bl, LANES), 0)
    sign = jnp.where(lax.rem(lane_b, HALF) < QUARTER, -1.0, 1.0)

    @pl.loop(0, every)
    def _(n):
        for k in range(HALVES):
            b = bid(n) if k == 0 else HALVES * n_cp - 1 - bid(n)
            ang = (b * bl + row_b).astype(F32) * fr[...]
            r = pl.ds(pl.multiple_of((HALVES * n + k) * bl, bl), bl)
            csb[r, :LANES] = jnp.cos(ang)
            csb[r, LANES:] = jnp.sin(ang) * sign

    cs_store = pltpu.make_async_copy(csb, cs_own, csem)
    cs_store.start()
    kv_load.wait()

    lane = lax.broadcasted_iota(jnp.int32, (rows, LANES), 1)
    low32 = lax.rem(lane, HALF) < QUARTER
    upper = lax.broadcasted_iota(jnp.int32, (rows, LANES), 0) < rows // HALVES
    tile = lambda t: pl.ds(t * HALVES, HALVES)
    block = lambda t: pl.ds(pl.multiple_of(t * rows, rows), rows)

    def norm(t32, gain):
        return (t32 * lax.rsqrt(jnp.mean(t32 * t32, axis=-1, keepdims=True) + NORM_EPS) * gain).astype(BF16)

    def lat_copy(k, i, t, ref, yy, cc):
        return me.copy(ref, ref, lss.at[t, k], lrs.at[t, i], yy, cc)

    def own_store(t):
        return pltpu.make_async_copy(pay.at[lax.rem(t, HALVES)], lat_all.at[c, tile(t)], lsem.at[t])

    def out_stores(t):
        sl = lax.rem(t, HALVES)
        return [pltpu.make_async_copy(pay.at[sl, :, :, :, :kr_rank], latent.at[tile(t)], osem.at[0, sl]),
                pltpu.make_async_copy(krb.at[sl], k_rope.at[block(t)], osem.at[1, sl])]

    def send_own(t):
        own_store(t).wait()
        for k, cc in ((0, partner), (1, left), (2, right)):
            lat_copy(k, k, t, lat_all.at[c, tile(t)], y, cc).start()

    def settle_stores(t):
        for s in out_stores(t):
            s.wait()

    @pl.loop(0, n_t)
    def _(t):
        load_x(t).wait()

        pl.when(t == 0)(lambda: load_x(1).start())

        @pl.when(t == 1)
        def _():
            for j in range(wdq.shape[1] // nj):
                dq_load(j).start()
            for d in late:
                d.start()

        pl.when(t > 0)(lambda: send_own(t - 1))

        sl = lax.rem(t, HALVES)

        def kv_dot(wrows):
            d = lax.dot_general(xbuf[sl], wdkv[wrows, :], (((1,), (1,)), ((), ())), preferred_element_type=F32)
            return d.astype(BF16)

        @pl.loop(0, kr_rank // nj)
        def _(j):
            js = pl.ds(pl.multiple_of(j * nj, nj), nj)
            kvb[:, js] = kv_dot(js)

        u = kv_dot(pl.ds(kr_rank, wdkv.shape[0] - kr_rank)).astype(F32)
        pl.when(t + HALVES < n_t)(lambda: load_x(t + 2).start())
        lat = norm(kvb[...].astype(F32), gkv[...])
        u = jnp.concatenate([u, u], axis=1)
        w = jnp.where(low32, pltpu.roll(u, 96, 1), pltpu.roll(u, QUARTER, 1))
        rot = u * csb[block(t), :LANES] + w * csb[block(t), LANES:]
        pl.when(t >= HALVES)(lambda: settle_stores(t - 2))
        krb[sl] = rot[:, :HALF].astype(BF16)
        pay[sl, :, :, :, :kr_rank] = lat.reshape(HALVES, HALVES, bl, kr_rank)
        ids = jnp.where(upper, bid(HALVES * t), bid(HALVES * t + 1)).astype(F32)
        pay[sl, :, :, :, kr_rank:] = jnp.where(lane < HALF, rot, ids).astype(BF16).reshape(HALVES, HALVES, bl, LANES)
        for s in [own_store(t)] + out_stores(t):
            s.start()

    send_own(last)
    cs_store.wait()
    cs_send = me.copy(cs_own, cs_par, css, crs, y, partner)
    cs_send.start()
    for d in late:
        d.wait()

    def stage1(t):
        rp, lp = lat_all.at[right, tile(t)], lat_all.at[left, tile(t)]
        lat_copy(3, 1, t, rp, y, partner).wait_recv()
        lat_copy(3, 2, t, lp, y, partner).wait_recv()
        for k, ref in ((3, rp), (4, lp)):
            lat_copy(k, k, t, ref, y, partner).start()

        @pl.when(t < last)
        def _():
            for k, ref, cc in ((5, lat_all.at[left, tile(t), 0], right), (6, lat_all.at[right, tile(t), 1], left)):
                lat_copy(k, k, t, ref, y, cc).start()

        pl.when(t == last)(lambda: lat_copy(5, 5, t, id_rows(left), y, right).start())

    def id_rows(dev):
        return lat_all.at[dev, tile(last), 0, pl.ds(0, 16)]

    def stage2(t):
        for k in range(HALVES):
            ref = lat_all.at[far, tile(t), k]
            lat_copy(SPARE, 5 + k, t, ref, y, partner).wait_recv()
            lat_copy(7 + k, 7 + k, t, ref, y, partner).start()

    def project(src, wref, dst, width, before=None):
        @pl.loop(0, wref.shape[1] // width)
        def _(j):
            if before is not None:
                before(j)
            cols = pl.ds(pl.multiple_of(j * width, width), width)
            dst[:, cols] = jnp.dot(src[...], wref[:, cols], preferred_element_type=F32).astype(BF16)

    def q_store(u, dst, t):
        return pltpu.make_async_copy(qst.at[lax.rem(u, HALVES)], dst.at[block(t)], osem.at[3, lax.rem(u, HALVES)])

    def q_send(t):
        return me.copy(qn_o.at[block(t)], qn_p.at[block(t)], qss.at[t], qrs.at[t], y, partner)

    @pl.loop(0, n_t)
    def _(t):
        v = last - t
        pl.when(t >= HALVES)(lambda: load_x(v).wait())
        project(xbuf.at[lax.rem(v, HALVES)], wdq, qlat, nj, lambda j: pl.when(t == 0)(lambda: dq_load(j).wait()))
        pl.when(v >= HALVES)(lambda: load_x(v - 2).start())

        @pl.when(t == 0)
        def _():
            for k in (last - 1, last):
                settle_stores(k)

        stage1(t)
        sl = lax.rem(t, HALVES)
        qn[sl] = norm(qlat[...].astype(F32), gq[...])
        cp = pltpu.make_async_copy(qn.at[sl], qn_o.at[block(v)], osem.at[2, sl])
        cp.start()
        pl.when(t >= HALVES)(lambda: q_store(t, q_own, t - 2).wait())
        project(qn.at[sl], wuq, qst.at[sl], wuq.shape[1] // HALVES)
        cp.wait()
        q_send(v).start()
        q_store(t, q_own, v).start()

    def load_qp(t):
        return pltpu.make_async_copy(qn_p.at[block(last - t)], qn.at[lax.rem(t, HALVES)], osem.at[2, lax.rem(t, HALVES)])

    def take_qp(t):
        q_send(last - t).wait_recv()
        load_qp(t).start()

    take_qp(0)

    @pl.loop(0, n_t)
    def _(t):
        load_qp(t).wait()
        pl.when(t + 1 < n_t)(lambda: take_qp(t + 1))
        q_store(n_t + t, q_own, t).wait()
        project(qn.at[lax.rem(t, HALVES)], wuq, qst.at[lax.rem(n_t + t, HALVES)], wuq.shape[1] // HALVES)
        q_store(n_t + t, q_par, last - t).start()
        pl.when(t < last)(lambda: stage2(t))

    lat_copy(SPARE, 5, last, id_rows(far), y, partner).wait_recv()
    lat_copy(SPARE, 7, last, id_rows(far), y, partner).start()
    for k in range(HALVES):
        q_store(k, q_par, 0).wait()

    pr, pl_, pf = (lax.rem(partner + k, n_cp) for k in (HALVES, n_cp - HALVES, n_cp // HALVES))

    @pl.loop(0, n_t)
    def _(t):
        for i, ref in ((0, lat_all.at[partner, tile(t)]), (3, lat_all.at[pr, tile(t)]), (4, lat_all.at[pl_, tile(t)])):
            lat_copy(SPARE, i, t, ref, y, partner).wait_recv()
        for k in range(5):
            lat_copy(k, k, t, lat_all.at[c, tile(t)], y, partner).wait_send()

        @pl.when(t < last)
        def _():
            for k in range(HALVES):
                lat_copy(SPARE, 7 + k, t, lat_all.at[pf, tile(t), k], y, partner).wait_recv()
            for k in range(5, 9):
                lat_copy(k, k, t, lat_all.at[c, tile(t), 0], y, partner).wait_send()

        q_send(t).wait_send()

    lat_copy(SPARE, 7, last, id_rows(pf), y, partner).wait_recv()
    for k in (5, 7):
        lat_copy(k, k, last, id_rows(c), y, partner).wait_send()
    for s in w_sends + [cs_send]:
        s.wait()


def project_all(mesh, pos, x, w_dq, w_dkv, w_uq, g_q, g_kv, freq, w_o, bl):
    n_tp, n_cp = mesh.shape["tp"], mesh.shape["cp"]
    n_seq, seq, width = x.shape
    rows = HALVES * seq
    n_t = n_seq // HALVES
    rank, kvw = w_dq.shape[1], w_dkv.shape[1]
    kr = g_kv.shape[0]
    qw = w_uq.shape[1] // HALVES
    half_cols = width // HALVES
    wc = half_cols // n_cp
    total = n_seq * seq
    hbm = pl.BlockSpec(memory_space=pltpu.HBM)
    sds = jax.ShapeDtypeStruct
    dma = pltpu.SemaphoreType.DMA
    trig = sds((total, MXU), F32)
    return pl.pallas_call(
        functools.partial(proj_kernel, (n_tp, n_cp, n_t, half_cols, wc)),
        in_specs=[pl.BlockSpec(memory_space=pltpu.SMEM)] + [hbm] * 4 + [pl.BlockSpec(memory_space=pltpu.VMEM)] * 3 + [hbm],
        out_specs=[hbm] * 10,
        out_shape=[sds((n_cp, n_seq, 2, bl, kr + LANES), BF16), sds((n_seq, 2, bl, kr), BF16), sds((total, kvw - kr), BF16),
                   sds((total, qw), BF16), sds((total, qw), BF16), sds((3, w_o.shape[0], wc), BF16),
                   trig, trig, sds((total, rank), BF16), sds((total, rank), BF16)],
        scratch_shapes=[
            pltpu.VMEM((HALVES, rows, width), BF16), pltpu.VMEM((width, rank), BF16), pltpu.VMEM((kvw, width), BF16),
            pltpu.VMEM((rank, qw), BF16), pltpu.VMEM(trig.shape, F32), pltpu.VMEM((HALVES, HALVES, 2, bl, kr + LANES), BF16),
            pltpu.VMEM((HALVES, rows, kvw - kr), BF16), pltpu.VMEM((rows, kr), BF16), pltpu.VMEM((rows, rank), BF16),
            pltpu.VMEM((HALVES, rows, rank), BF16), pltpu.VMEM((HALVES, rows, qw), BF16),
            dma((HALVES,)), dma((HALVES,)), dma((rank // WIDE,)), dma, dma((4, HALVES)), dma((3,)), dma((3,)), dma((n_t, 9)), dma((n_t, 9)),
            dma((n_t,)), dma((n_t,)), dma, dma, dma((n_t,))],
        compiler_params=pltpu.CompilerParams(collective_id=0, has_side_effects=True, vmem_limit_bytes=63 * MIB),
        cost_estimate=pl.CostEstimate(flops=HALVES * total * (width * (rank + kvw) + HALVES * rank * qw), bytes_accessed=10**8,
                                      transcendentals=0),
        name="proj",
    )(pos, x.reshape(total, width), w_dq, w_dkv.T, w_uq, g_q, g_kv, freq, w_o)


def out_kernel(dims, x, w_o, wf, wx, ost_own, ost_par, obuf, out, wy, oy,
               wbuf, ov, xb, stage, wsem, osem, xsem, ssem, oss, ors, wss, wrs, ass, ars):
    n_tp, n_cp, n_seq, bl, half_cols = dims
    me = Place(n_tp, n_cp)
    cols, kb = xb.shape[-1], obuf.shape[-1]
    w, krows = cols // HALVES, w_o.shape[0]
    hk = krows // HALVES
    last = n_seq - 1
    half_of = lambda row: lax.rem(row, HALVES)
    tb = me.block(me.y, me.core)

    hb = kb // HALVES
    cut = [pl.ds(k * hb, hb) for k in range(HALVES)]
    to_last = lambda s, p: oy.at[s, p, 1]
    to_prev = lambda s, p: oy.at[s, p, 0]
    prev_fwd = me.o_forwards(lambda s, p: obuf.at[s, p, last, :, cut[0]], to_prev, oss.at[0], ors.at[0])
    last_sends = me.o_sends(ost_own.at[last, :, :, cut[1]], ost_par.at[last, :, :, cut[1]], to_last, oss.at[1], ors.at[1])
    last_fwd = me.o_forwards(to_last, to_last, oss.at[1], ors.at[1])
    def w_copy(k, src, dst, yy, cc):
        return me.copy(src, dst, wss.at[k], wrs.at[k], yy, cc)

    far_rows = [pl.ds(k * hk, hk) for k in range(HALVES)]
    (to_r, to_l), (rest_r, rest_l) = w_parts(krows)
    p_right, p_left, p_far = (lax.rem(me.partner + k, n_cp) for k in (HALVES, n_cp - HALVES, n_cp // HALVES))
    mine, side = (me.y, me.partner), ((me.y, me.right), (me.y, me.left))

    def w_move(k, buf, dev, part, to):
        return w_copy(k, buf.at[dev, :, part], wy.at[dev, :, part], *to)

    w_sends = [w_copy(0, wf.at[:, rest_r], wy.at[me.c, :, rest_r], *side[0]), w_copy(1, wf.at[:, rest_l], wy.at[me.c, :, rest_l], *side[1]),
               w_move(2, wx, me.left, to_r, mine), w_move(3, wx, me.right, to_l, mine),
               w_move(4, wx, me.left, far_rows[0], side[0]), w_move(5, wx, me.right, far_rows[1], side[1])]
    rest_fwd = [w_move(6, wy, me.left, rest_r, mine), w_move(7, wy, me.right, rest_l, mine)]
    far_fwd = [w_move(8 + k, wy, me.far, far_rows[k], mine) for k in range(HALVES)]

    def w_recv(k, dev, part):
        w_move(k, wy, dev, part, mine).wait_recv()

    n_m = n_seq // HALVES
    rows = HALVES * bl
    k_of = (None, me.flip, 1 - me.flip, HALVES)
    every = pl.ds(0, krows)
    own = ((wx, to_l), (wy, rest_l)), ((wx, to_r), (wy, rest_r))
    pieces = ((((wf, every),), ((wx.at[me.partner], every),)),) + tuple(
        (tuple((buf.at[dev], part) for buf, part in own[i]), ((wy.at[dev_p], every),))
        for i, (dev, dev_p) in enumerate(((me.right, p_right), (me.left, p_left)))) + ((((wy.at[me.far], every),), ((wy.at[p_far], every),)),)
    offs = [pl.multiple_of(v * w, LANES) for v in (me.core, 1 - me.core)]

    def col_of(j, row):
        dx = j + (j // HALVES) * (1 - HALVES * (j % HALVES))
        xq = lax.rem(lax.div(me.c, HALVES) + dx, n_cp // HALVES)
        return pl.multiple_of(half_of(row) * half_cols + xq * cols, LANES)

    def w_loads(j):
        b = j % HALVES
        out_ = [pltpu.make_async_copy(w_o.at[:, pl.ds(col_of(j, me.y), cols)], wbuf.at[b, 0], wsem.at[b, 0])]
        for r in range(1, SOURCES):
            for part in range(HALVES):
                for i, (buf, part_rows) in enumerate(pieces[j][part]):
                    out_.append(pltpu.make_async_copy(buf.at[k_of[r], part_rows], wbuf.at[b, r, part_rows, pl.ds(offs[part], w)],
                                                      wsem.at[b, HALVES * r + part + 8 * i]))
        return out_

    def x_load(j):
        return pltpu.make_async_copy(x.at[:, pl.ds(pl.multiple_of(tb * bl, bl), bl), pl.ds(col_of(j, me.y), cols)], xb.at[j % HALVES], xsem.at[j % HALVES])

    o_offs = [pl.multiple_of(v * kb, LANES) for v in (me.core, 1 - me.core)]

    def o_place(i, r, part, half=None):
        off = r * krows + o_offs[part] + (0 if half is None else half * hb)
        return ov.at[i, :, pl.ds(pl.multiple_of(off, LANES), kb if half is None else hb)]

    def o_load(i, r, part):
        src = ost_own.at[i, tb] if (r, part) == (0, 0) else obuf.at[r, part, i]
        return pltpu.make_async_copy(src, o_place(i, r, part), osem.at[i, HALVES * r + part])

    pairs = [(r, part) for r in range(SOURCES) for part in range(HALVES)]
    early = [o_load(i, r, part) for i in range(last - 1) for r, part in pairs]
    late = [o_load(last - 1, r, part) for r, part in pairs]
    for r, part in pairs:
        for half in range(HALVES):
            if (r, part) == (0, 0):
                src = ost_own.at[last, tb, :, cut[half]]
            else:
                src = oy.at[r, part, half] if half == 1 or r == 3 else obuf.at[r, part, last, :, cut[0]]
            late.append(pltpu.make_async_copy(src, o_place(last, r, part, half), osem.at[last, HALVES * r + part + 8 * half]))
    for d in w_loads(0) + early + [x_load(0)]:
        d.start()
    me.greet(((me.up, me.c), (me.dn, me.c), (me.up, me.partner), (me.dn, me.partner),
              (me.y, me.partner), (me.y, me.right), (me.y, me.left)))
    for s in last_sends + prev_fwd + w_sends:
        s.start()

    def region(row, j, m, n0=0, cnt=2):
        return out.at[pl.ds(HALVES * m + n0, cnt), pl.ds(pl.multiple_of(me.block(row, me.core) * bl, bl), bl), pl.ds(col_of(j, row), cols)]

    def ring(k, ref, j, m, yy):
        i = j * n_m + m
        return me.copy(ref, ref, ass.at[i, k], ars.at[i, k], yy, me.c)

    def tile_sends(j, m):
        ref = region(me.y, j, m)
        return ring(0, ref, j, m, me.up), ring(1, ref, j, m, me.dn)

    def forward(j, m):
        ring(0, region(me.dn, j, m), j, m, me.up).wait_recv()
        ring(2, region(me.dn, j, m, 0, 1), j, m, me.up).start()
        ring(1, region(me.up, j, m), j, m, me.up).wait_recv()
        ring(3, region(me.up, j, m, 1, 1), j, m, me.dn).start()

    nt = MXU

    def tile(j, m):
        b = j % HALVES

        @pl.loop(0, cols // nt)
        def _(t):
            cs_ = pl.ds(pl.multiple_of(t * nt, nt), nt)
            a = ov[pl.ds(HALVES * m, HALVES)].reshape(rows, SOURCES * krows)
            s = None
            for r in range(SOURCES):
                d = jnp.dot(a[:, r * krows:(r + 1) * krows], wbuf[b, r, :, cs_], preferred_element_type=F32)
                s = d if s is None else s + d
            xr = xb[b, pl.ds(HALVES * m, HALVES), :, cs_].reshape(rows, nt).astype(F32)
            stage[:, :, cs_] = (xr + s).astype(BF16).reshape(2, bl, nt)

        c = pltpu.make_async_copy(stage, region(me.y, j, m), ssem)
        c.start()
        c.wait()
        for s in tile_sends(j, m):
            s.start()

    def need(j):
        if j == 0:
            w_recv(1, me.right, rest_l)
            rest_fwd[1].start()
            w_recv(3, p_right, to_l)
            w_recv(7, p_right, rest_l)
        elif j == 1:
            w_recv(0, me.left, rest_r)
            rest_fwd[0].start()
            w_recv(2, p_left, to_r)
            w_recv(6, p_left, rest_r)
        else:
            for k in range(HALVES):
                w_recv(4 + k, me.far, far_rows[k])
                far_fwd[k].start()
            for k in range(HALVES):
                w_recv(8 + k, p_far, far_rows[k])
        for d in w_loads(j + 1) + [x_load(j + 1)]:
            d.start()

    def late_o():
        for k in DIRECT:
            last_sends[k].wait_recv()
        for f in prev_fwd + last_fwd:
            f.wait_recv()
        for d in late:
            d.start()
        for d in late:
            d.wait()

    for k, f in zip(FORWARDED, last_fwd):
        last_sends[k].wait_recv()
        f.start()
    for d in early:
        d.wait()

    @pl.loop(0, SOURCES * n_m)
    def _(i):
        j, m = lax.div(i, n_m), lax.rem(i, n_m)
        for jj in range(SOURCES):
            @pl.when(i == jj * n_m)
            def _(jj=jj):
                for d in w_loads(jj) + [x_load(jj)]:
                    d.wait()
                if jj == 1:
                    need(jj)
        pl.when(i == n_m - 1)(late_o)
        tile(j, m)
        pl.when(i == 0)(lambda: need(0))

        @pl.when(j > 0)
        def _():
            forward(j - 1, m)

        pl.when(i == 3 * n_m - 1)(lambda: need(2))

    @pl.loop(0, n_m)
    def _(m):
        forward(3, m)

    @pl.loop(0, SOURCES * n_m)
    def _(i):
        j, m = lax.div(i, n_m), lax.rem(i, n_m)
        for k, row, n0, cnt in ((0, me.y, 0, HALVES), (1, me.y, 0, HALVES), (2, me.dn, 0, 1), (3, me.up, 1, 1)):
            r = region(row, j, m, n0, cnt)
            me.copy(r, r, ass.at[i, k], ars.at[i, k], me.up, me.c).wait_send()
        for k, n0 in ((HALVES, 0), (3, 1)):
            r = region(me.dg, j, m, n0, 1)
            me.copy(r, r, ass.at[i, k], ars.at[i, k], me.up, me.c).wait_recv()

    for s in last_sends + prev_fwd + last_fwd + w_sends + rest_fwd + far_fwd:
        s.wait_send()


def out_product(mesh, x, w_o, wf, wx, ost_own, ost_par, obuf):
    n_tp, n_cp = mesh.shape["tp"], mesh.shape["cp"]
    n_seq, seq, width = x.shape
    bl = seq // HALVES
    cols = HALVES * wf.shape[-1]
    krows = w_o.shape[0]
    hbm = pl.BlockSpec(memory_space=pltpu.HBM)
    dma = pltpu.SemaphoreType.DMA
    sds = jax.ShapeDtypeStruct
    tiles = HALVES * n_seq
    return pl.pallas_call(
        functools.partial(out_kernel, (n_tp, n_cp, n_seq, bl, width // HALVES)),
        in_specs=[hbm] * 7, out_specs=[hbm] * 3,
        out_shape=[sds(x.shape, BF16), sds(wx.shape, BF16), sds((SOURCES, HALVES, HALVES, bl, obuf.shape[-1] // HALVES), BF16)],
        scratch_shapes=[
            pltpu.VMEM((HALVES, SOURCES, krows, cols), BF16), pltpu.VMEM((n_seq, bl, SOURCES * krows), BF16), pltpu.VMEM((HALVES, n_seq, bl, cols), BF16),
            pltpu.VMEM((HALVES, bl, cols), BF16), dma((HALVES, 16)), dma((n_seq, 16)), dma((HALVES,)), dma, dma((HALVES, 7)), dma((HALVES, 7)),
            dma((10,)), dma((10,)), dma((tiles, 4)), dma((tiles, 4))],
        compiler_params=pltpu.CompilerParams(collective_id=2, has_side_effects=True, vmem_limit_bytes=63 * MIB),
        cost_estimate=pl.CostEstimate(flops=n_seq * seq * cols * 16 * krows, bytes_accessed=10**8, transcendentals=0),
        name="outp",
    )(x, w_o, wf, wx, ost_own, ost_par, obuf)[0]


def settle_kernel(src, lat, kr, dst, lat_out, kr_out, buf, lbuf, kbuf, tbuf, rsem, wsem, lsem, ksem):
    n = buf.shape[0]
    reads = [pltpu.make_async_copy(src.at[i], buf.at[i], rsem.at[i]) for i in range(n)]
    writes = [pltpu.make_async_copy(buf.at[i], dst.at[i], wsem.at[i]) for i in range(n)]
    small = [pltpu.make_async_copy(*p) for p in ((kr, kbuf, ksem.at[0]), (lat, lbuf, lsem.at[0]))]
    small_out = [pltpu.make_async_copy(*p) for p in ((tbuf, kr_out, ksem.at[1]), (lbuf, lat_out, lsem.at[1]))]
    for d in small + reads:
        d.start()
    for d in small:
        d.wait()
    for i in range(tbuf.shape[0]):
        tbuf[i] = kbuf[i].astype(F32).T.astype(BF16)
    for d in small_out:
        d.start()
    for a, b in zip(reads, writes):
        a.wait()
        b.start()
    for d in writes + small_out:
        d.wait()


def settle(out, lat, kr):
    n_seq, seq, width = out.shape
    parts = 4 * n_seq
    shape = (parts, n_seq * seq // parts, width)
    lat_shape, kr_shape = (n_seq, seq, lat.shape[-1]), (n_seq, seq, kr.shape[-1])
    turned = (n_seq, kr.shape[-1], seq)
    hbm = pl.BlockSpec(memory_space=pltpu.HBM)
    sds = jax.ShapeDtypeStruct
    dma = pltpu.SemaphoreType.DMA
    a, b, c = pl.pallas_call(
        settle_kernel, in_specs=[hbm] * 3, out_specs=[hbm] * 3,
        out_shape=[sds(shape, BF16), sds(lat_shape, BF16), sds(turned, BF16)],
        scratch_shapes=[pltpu.VMEM(shape, BF16), pltpu.VMEM(lat_shape, BF16), pltpu.VMEM(kr_shape, BF16), pltpu.VMEM(turned, BF16),
                        dma((parts,)), dma((parts,)), dma((HALVES,)), dma((HALVES,))],
        compiler_params=pltpu.CompilerParams(vmem_limit_bytes=63 * MIB), name="settle",
    )(out.reshape(shape), lat.reshape(lat_shape), kr.reshape(kr_shape))
    return a.reshape(out.shape), b, jnp.swapaxes(c, 1, HALVES)


ROPE_BASE = 10000.0


def solution(mesh):
    def local_step(x, pos, w_dq, g_q, w_uq, w_dkv, g_kv, w_uk, w_uv, w_o):
        n_seq, seq, _ = x.shape
        n_cp = mesh.shape["cp"]
        bl = seq // HALVES
        nb = HALVES * n_cp
        kv_rank = g_kv.shape[0]
        rope = w_dkv.shape[1] - kv_rank
        heads = (w_uq.shape[1] - w_uk.shape[1]) // rope
        nope = w_uk.shape[1] // heads
        c = lax.axis_index("cp")
        core = c % HALVES

        freq = np.tile(ROPE_BASE ** (-2.0 * np.arange(rope // HALVES) / rope), LANES // (rope // HALVES))[None].astype(np.float32)
        lat_all, latent, k_rope, q_own, q_par, wf, cs_own, cs_par, _, _ = project_all(
            mesh, pos, x, w_dq, w_dkv, w_uq, g_q, g_kv, freq, w_o, bl)
        q_own, q_par = (a.reshape(n_seq, seq, -1) for a in (q_own, q_par))
        ids = lat_all[:, :, 0, 0, kv_rank + rope].astype(jnp.int32)
        blocks = jnp.arange(nb)
        first = ids[:, :, None] == blocks
        second = nb - 1 - ids[:, :, None] == blocks
        dev = jnp.arange(n_cp)[:, None, None]
        slots = jnp.sum(jnp.where(first, HALVES * dev, 0) + jnp.where(second, HALVES * dev + 1, 0), axis=0)
        mine = [jnp.sum(jnp.where(jnp.arange(n_cp)[:, None] == k, ids, 0), axis=0) for k in (c, c ^ 1)]
        last = nb // 4 - 1
        extra = []
        for i, b in enumerate(mine):
            is_first = b > last
            chunk = jnp.where(is_first, 1, last)
            extra += [jnp.where(is_first, i, 2 + i), chunk, jnp.where(is_first, b, nb - 1 - b) * bl - chunk * 4 * bl, is_first]
        tab = jnp.concatenate([slots, jnp.stack(mine + extra, axis=1).astype(jnp.int32)], axis=1).astype(jnp.int32)

        ost_own, ost_par, obuf, wx, _ = attention(mesh, tab, q_own, q_par, cs_own, cs_par, w_uk, w_uv, lat_all, wf, (nope + rope) ** -0.5)
        return settle(out_product(mesh, x, w_o, wf, wx, ost_own, ost_par, obuf), latent, k_rope)

    seq_spec = P("dp", "cp", None)
    whole = P(None, None)
    in_specs = (seq_spec, P("dp", "cp"), whole, P(None), P(None, "tp"), whole, P(None), P(None, "tp"), P(None, "tp"), P("tp", None))
    return jax.shard_map(local_step, mesh=mesh, in_specs=in_specs, out_specs=(seq_spec,) * 3, check_vma=False)
```
